256 devices in a mesh: cp: 64 (over y, z, core), fs: 4 (over x).
Axes of the slice: x: 4, y: 4, z: 8, core: 2. Of those that a mesh axis runs over, the one named last changes fastest.
Arguments:
- embeds: bfloat16 [4, 16384, 4096], P('fs', 'cp'), may hold values from -16 to 16
- queries: bfloat16 [4, 16384, 2048], P('fs', 'cp'), may hold values from -12 to 12
- key_heads: bfloat16 [4, 16384, 512], P('fs', 'cp'), may hold values from -4 to 4
- cotangent: bfloat16 [4, 16384, 2048], P('fs', 'cp'), may hold values from -6 to 6
- doc_start: int32 [4, 16384], P('fs', 'cp'), may hold values from 0 to 16383, as said below
- need_ids: int32 [4, 64, 5], P('fs', 'cp'), may hold values from -1 to 63, as said below
- y_weight: bfloat16 [4096, 512], P(('cp', 'fs')), may hold values from -0.09375 to 0.09375
- z_weight: float32 [4096, 512], P(('cp', 'fs')), may hold values from -0.09375 to 0.09375
- x_weight: float32 [4096, 512], P(('cp', 'fs')), may hold values from -0.09375 to 0.09375
- second_moment: float32 [4096, 512], P(('cp', 'fs')), may hold values from 1e-05 to 0.001
Outputs:
- z_next: float32 [4096, 512], P(('cp', 'fs'))
- x_next: float32 [4096, 512], P(('cp', 'fs'))
- moment_next: float32 [4096, 512], P(('cp', 'fs'))
- y_next: bfloat16 [4096, 512], P(('cp', 'fs'))
The draws below stay inside these ranges and needn't reach their ends.
Inputs may be any that keep to these rules, and one draw needn't show every extreme that they name: `doc_start`: documents are contiguous and hold at most 1024 tokens, so a query block needs key-value blocks at most 4 blocks back; in every sequence some query block needs the block exactly 4 back. need_ids[f, b, j] is b - j when some query of block b is allowed a key of block b - j, else -1; need_ids[f, b, 0] is always b.
All inputs are finite; a program needn't handle non-finite values.
Results may differ from the reference program's by a relative error of at most 0.0027.
The reference program's roundings to bfloat16 on the way count: a program that leaves them out, or rounds other values in their place, can miss the bound.
Values may be sent and summed in bfloat16 or wider, within the bound.
A program may use at most 128 MiB of HBM per device.

```python
import math
import jax
import jax.numpy as jnp
from jax import lax

D = 4096
HEAD = 128
KV_HEADS = 4
TOK_DEV = 256
WIN = 4
GROUP = 4
QW = 2048
E = 512
SEQ = 16384
N_CP = 64
N_FS = 4


def query_and_key(key):
    seq_len = TOK_DEV * N_CP
    key_draw = jnp.clip(jax.random.normal(jax.random.fold_in(key, 31), (N_FS, seq_len, E), jnp.float32), -4.0, 4.0)
    query_draw = jnp.clip(jax.random.normal(jax.random.fold_in(key, 32), (N_FS, seq_len, QW), jnp.float32), -6.0, 6.0)
    return (key_draw, query_draw)


def document_starts(key):
    seq_len = TOK_DEV * N_CP
    half_block = TOK_DEV // 2
    span_len = WIN * TOK_DEV
    position = jnp.arange(seq_len, dtype=jnp.int32)
    span_index = jnp.floor_divide(position - half_block, span_len)
    span_first = jnp.maximum(half_block + span_index * span_len, 0)
    span_total = seq_len // span_len + 2
    levels = jax.random.randint(jax.random.fold_in(key, 21), (N_FS, span_total), 0, 4)
    rate_table = jnp.array([0, 2, 8, 32], jnp.int32)
    cut_rate = rate_table[levels]
    cut_rate = cut_rate.at[:, 1].set(0)
    span_rate = cut_rate[:, span_index + 1]
    coin_draw = jax.random.randint(jax.random.fold_in(key, 22), (N_FS, seq_len), 0, 1024)
    forced_off = jax.random.randint(jax.random.fold_in(key, 23), (N_FS, span_total), 1, span_len)
    span_forced = forced_off[:, span_index + 1]
    forced_cut = ((position - span_first)[None, :] == span_forced) & (span_index != 0)[None, :]
    marker = (position[None, :] == span_first[None, :]) | (coin_draw < span_rate) | forced_cut
    return lax.cummax(jnp.where(marker, position[None, :], 0), axis=1).astype(jnp.int32)


def draw_queries(key, part):
    return query_and_key(key)[1].astype(jnp.bfloat16)


def draw_key_heads(key, part):
    return query_and_key(key)[0].astype(jnp.bfloat16)


def draw_doc_start(key, part):
    return document_starts(key)


def draw_need_ids(key, part):
    starts = document_starts(key)
    first_of_block = starts[:, ::TOK_DEV]
    block_ids = jnp.arange(N_CP, dtype=jnp.int32)[:, None]
    back_steps = jnp.arange(WIN + 1, dtype=jnp.int32)[None, :]
    target = block_ids - back_steps
    needed = (first_of_block[:, :, None] < (target + 1)[None] * TOK_DEV) & (target >= 0)[None]
    return jnp.where(needed, target[None], -1).astype(jnp.int32)


def with_spikes(values, own_key, source, target, blocks, factor):
    def block_of(dim):
        return (jnp.arange(values.shape[dim]) // (values.shape[dim] // blocks)).reshape((-1,) + (1,) * (values.ndim - 1 - dim))

    near = jax.random.permutation(own_key, blocks)[block_of(target)]
    other_side = (block_of(target) + blocks // 2) % blocks
    return jnp.where((block_of(source) == near) | (block_of(source) == other_side), factor * values, values)


def block_scale(own_key, extent, cuts, smallest, high):
    gain, own = 1.0, jax.random.fold_in(own_key, 6)
    for dim, shards_of in cuts:
        steps = jnp.exp(jax.random.uniform(jax.random.fold_in(own, dim), (shards_of,), jnp.float32, smallest / len(cuts), high / len(cuts)))
        gain = gain * jnp.repeat(steps, extent[dim] // shards_of).reshape([-1 if axis == dim else 1 for axis in range(len(extent))])
    return gain


def normal_values(key, extent, width, bound, pieces=(), kind=jnp.bfloat16):
    drawn = width * jax.random.normal(key, extent, jnp.float32)
    if pieces:
        drawn = drawn * block_scale(key, extent, pieces, -0.22, 0.18)
    return jnp.clip(drawn, -bound, bound).astype(kind)


def bell_draw_with(key, dims, scale, most, shards, heavy, kind=jnp.bfloat16):
    values = scale * jax.random.normal(key, dims, jnp.float32)
    if shards:
        values = values * block_scale(key, dims, shards, -0.22, 0.18)
    return jnp.clip(with_spikes(values, jax.random.fold_in(key, 3), *heavy), -most, most).astype(kind)


def setup_inputs(seed: int = 0) -> dict:
    key_of = jax.random.split(jax.random.key(seed), 11)
    return {
        "embeds": bell_draw_with(key_of[0], (N_FS, SEQ, D), 1.0, 16.0, ((0, 4), (1, 64)), (1, 2, 64, 4.0)),
        "queries": draw_queries(jax.random.fold_in(key_of[10], 71), 0),
        "key_heads": draw_key_heads(jax.random.fold_in(key_of[10], 71), 0),
        "cotangent": normal_values(key_of[3], (N_FS, SEQ, QW), 1.0, 6.0, ((0, 4), (1, 64))),
        "doc_start": draw_doc_start(jax.random.fold_in(key_of[10], 71), 0),
        "need_ids": draw_need_ids(jax.random.fold_in(key_of[10], 71), 0),
        "y_weight": normal_values(key_of[6], (D, E), D ** -0.5, 0.09375, ((0, 256),)),
        "z_weight": normal_values(key_of[7], (D, E), D ** -0.5, 0.09375, ((0, 256),), jnp.float32),
        "x_weight": normal_values(key_of[8], (D, E), D ** -0.5, 0.09375, ((0, 256),), jnp.float32),
        "second_moment": jnp.clip(jnp.exp(math.log(0.001) - 4.6051703 * jax.random.uniform(key_of[9], (D, E), jnp.float32) ** block_scale(key_of[9], (D, E), ((0, 256),), -0.2, 0.2)), 9.999999747378752e-06, 0.001),
    }


NORM_EPS = 0.01
MOMENT_DECAY = 0.95
LEARN_RATE = 0.005
WEIGHT_DECAY = 0.1
ADAM_EPS = 1e-08
AVERAGE_MIX = 0.25
INTERP_BETA = 0.9

def visible(doc_rows, need_row, block_id, tok_rows):
    span_rows = (WIN + 1) * tok_rows
    query_pos = block_id * tok_rows + jnp.arange(tok_rows, dtype=jnp.int32)
    key_pos = (block_id - WIN) * tok_rows + jnp.arange(span_rows, dtype=jnp.int32)
    key_block = block_id - WIN + jnp.arange(span_rows, dtype=jnp.int32) // tok_rows
    listed = jnp.any(need_row[None, :] == key_block[:, None], axis=1)
    return (key_pos[None, :] >= doc_rows[:, None]) & (key_pos[None, :] <= query_pos[:, None]) & listed[None, :]

def block_attention(query_rows, key_window, value_window, allowed):
    tok_rows = query_rows.shape[0]
    scaling = 1.0 / math.sqrt(HEAD)
    query_split = query_rows.astype(jnp.float32).reshape(tok_rows, KV_HEADS, GROUP, HEAD)
    prob_list = []
    out_list = []
    for kv_head in range(KV_HEADS):
        key_part = key_window[:, kv_head * HEAD:(kv_head + 1) * HEAD].astype(jnp.float32)
        value_part = value_window[:, kv_head * HEAD:(kv_head + 1) * HEAD].astype(jnp.float32)
        scores = jnp.einsum('tgh,sh->gts', query_split[:, kv_head], key_part) * scaling
        scores = jnp.where(allowed[None], scores, -jnp.inf)
        largest = lax.optimization_barrier(jnp.max(scores, axis=-1, keepdims=True))
        weights = jnp.exp(scores - largest)
        probs_low = (weights / lax.optimization_barrier(jnp.sum(weights, axis=-1, keepdims=True))).astype(jnp.bfloat16)
        prob_list.append(probs_low)
        out_list.append(jnp.einsum('gts,sh->tgh', probs_low.astype(jnp.float32), value_part))
    attended = jnp.stack(out_list, axis=1).reshape(tok_rows, KV_HEADS * GROUP * HEAD)
    return (prob_list, attended)

def norm_backward(attended, cot_rows, token_total):
    square_mean = lax.optimization_barrier(jnp.mean(attended * attended, axis=-1, keepdims=True)) + NORM_EPS
    root_scale = jnp.sqrt(square_mean)
    normed = attended / root_scale
    upstream = cot_rows.astype(jnp.float32) / token_total
    inner = lax.optimization_barrier(jnp.mean(upstream * normed, axis=-1, keepdims=True))
    return ((upstream - normed * inner) / root_scale).astype(jnp.bfloat16)

def window_grads(prob_list, out_grad):
    tok_rows = out_grad.shape[0]
    grad_split = out_grad.astype(jnp.float32).reshape(tok_rows, KV_HEADS, GROUP, HEAD)
    head_parts = []
    for kv_head in range(KV_HEADS):
        head_parts.append(jnp.einsum('gts,tgh->sh', prob_list[kv_head].astype(jnp.float32), grad_split[:, kv_head]))
    return jnp.concatenate(head_parts, axis=1)

def reference(embeds, queries, key_heads, cotangent, doc_start, need_ids, y_weight, z_weight, x_weight, second_moment):
    seq_len = embeds.shape[1]
    tok_rows = seq_len // N_CP
    kv_width = key_heads.shape[2]
    token_total = seq_len * N_FS
    gradient = jnp.zeros((embeds.shape[2], kv_width), jnp.float32)
    for seq_index in range(N_FS):
        tokens_here = embeds[seq_index]
        values = jnp.dot(tokens_here, y_weight, preferred_element_type=jnp.float32).astype(jnp.bfloat16)
        padding = jnp.zeros((WIN * tok_rows, kv_width), jnp.bfloat16)
        keys_padded = jnp.concatenate([padding, key_heads[seq_index]], axis=0)
        values_padded = jnp.concatenate([padding, values], axis=0)
        query_seq = queries[seq_index]
        cot_seq = cotangent[seq_index]
        doc_seq = doc_start[seq_index]
        need_seq = need_ids[seq_index]

        def block_grads(block_id):
            first_row = block_id * tok_rows
            span_rows = (WIN + 1) * tok_rows
            query_rows = lax.dynamic_slice_in_dim(query_seq, first_row, tok_rows, 0)
            cot_rows = lax.dynamic_slice_in_dim(cot_seq, first_row, tok_rows, 0)
            doc_rows = lax.dynamic_slice_in_dim(doc_seq, first_row, tok_rows, 0)
            key_window = lax.dynamic_slice_in_dim(keys_padded, first_row, span_rows, 0)
            value_window = lax.dynamic_slice_in_dim(values_padded, first_row, span_rows, 0)
            allowed = visible(doc_rows, need_seq[block_id], block_id, tok_rows)
            prob_list, attended = block_attention(query_rows, key_window, value_window, allowed)
            out_grad = norm_backward(attended, cot_rows, token_total)
            return window_grads(prob_list, out_grad)
        shares = lax.map(block_grads, jnp.arange(N_CP, dtype=jnp.int32))
        shares = shares.reshape(N_CP, WIN + 1, tok_rows, kv_width)
        summed = jnp.zeros((N_CP, tok_rows, kv_width), jnp.float32)
        for slot_index in range(WIN + 1):
            lag_blocks = WIN - slot_index
            shifted = jnp.concatenate([shares[lag_blocks:, slot_index], jnp.zeros((lag_blocks, tok_rows, kv_width), jnp.float32)], axis=0)
            summed = summed + shifted
        value_grad = summed.reshape(seq_len, kv_width).astype(jnp.bfloat16)
        gradient = gradient + jnp.dot(tokens_here.T, value_grad, preferred_element_type=jnp.float32)
    moment_next = MOMENT_DECAY * second_moment + (1.0 - MOMENT_DECAY) * gradient * gradient
    z_next = z_weight - LEARN_RATE * (gradient / (jnp.sqrt(moment_next) + ADAM_EPS) + WEIGHT_DECAY * y_weight.astype(jnp.float32))
    x_next = (1.0 - AVERAGE_MIX) * x_weight + AVERAGE_MIX * z_next
    y_next = ((1.0 - INTERP_BETA) * z_next + INTERP_BETA * x_next).astype(jnp.bfloat16)
    return (z_next, x_next, moment_next, y_next)
```

```python
import math
from types import SimpleNamespace

import jax
import jax.numpy as jnp
from jax import lax
from jax.experimental import pallas as pl
from jax.experimental.pallas import tpu as pltpu
from jax.sharding import Mesh
from jax.sharding import PartitionSpec as P

HEAD = 128
KV = 4
WIN = 4
GROUP = 4
TOK = 256
SPAN = (WIN + 1) * TOK
NY, NZ, NX = 4, 8, 4
CP = ("cp_0", "cp_1", "cp_2")
CP_FS = ("cp_0", "cp_1", "cp_2", "fs")

NORM_EPS = 0.01
MOMENT_DECAY = 0.95
LEARN_RATE = 0.005
WEIGHT_DECAY = 0.1
ADAM_EPS = 1e-08
AVERAGE_MIX = 0.25
INTERP_BETA = 0.9
EXP2_SCALE = math.log2(math.e) / math.sqrt(HEAD)
MASKED = -1e30
FAR = 1 << 30

BF = jnp.bfloat16
F32 = jnp.float32
MESH = pl.DeviceIdType.MESH

BUFFERS = {
    "emb": ((8, TOK, 512), BF),
    "w": ((2, NY, NZ, 2, NX, 16, 256), BF),
    "q": ((TOK, 2048), BF),
    "kw": ((5, TOK, 512), BF),
    "vw": ((KV, 5, TOK, HEAD), BF),
    "cot": ((TOK, 2048), BF),
    "p": ((16, TOK, SPAN), BF),
    "s": ((TOK, SPAN), F32),
    "bias": ((TOK, SPAN), F32),
    "vacc": ((2, TOK, 256), F32),
    "att": ((16, TOK, HEAD), F32),
    "og": ((16, TOK, HEAD), BF),
    "dv": ((KV, 5, TOK, HEAD), F32),
    "r": ((KV, 3, TOK, HEAD), F32),
    "fo": ((KV, TOK, HEAD), BF),
    "fi": ((KV, TOK, HEAD), BF),
    "go": ((KV, TOK, HEAD), BF),
    "gi": ((KV, TOK, HEAD), BF),
    "vg": ((2, 8, TOK, 256), BF),
    "ex": ((8, TOK, 512), BF),
    "g": ((2, 4, 2, NX, 16, 256), F32),
    "x1": ((2, 2, 2, 2, 16, 256), F32),
    "tx": ((2, 2, 4, 2, 16, 256), F32),
    "x2": ((2, 2, 4, 2, 16, 256), F32),
    "t": ((2, 4, 2, 16, 256), F32),
    "rz": ((2, NZ, 16, 256), F32),
}
SEMAPHORES = {
    "ld": 16,
    "w1": 8,
    "w2": 6,
    "w3": 8,
    "wd": 10,
    "k": 4,
    "v": 16,
    "e": 8,
    "r": 8,
    "f": 4,
    "g": 4,
    "vg": 16,
    "vd": 16,
    "x": 8,
    "z": 16,
}


def kernel(need, doc, emb_h, q_h, k_h, cot_h, yw_h, out, *scratch):
    names = list(BUFFERS)
    b = SimpleNamespace(**dict(zip(names, scratch)))
    rest = scratch[len(names) :]
    snd = dict(zip(SEMAPHORES, rest[: len(SEMAPHORES)]))
    rcv = dict(zip(SEMAPHORES, rest[len(SEMAPHORES) :]))

    y, z = lax.axis_index("cp_0"), lax.axis_index("cp_1")
    c, x = lax.axis_index("cp_2"), lax.axis_index("fs")
    o = 1 - c
    zn, yn = lax.rem(z + 1, NZ), lax.rem(y + lax.div(z + 1, NZ), NY)
    zp, yp = lax.rem(z + NZ - 1, NZ), lax.rem(y + NY - 1 + lax.div(z + NZ - 1, NZ), NY)
    yup, ydn = lax.rem(y + 1, NY), lax.rem(y + NY - 1, NY)
    xup, xdn = lax.rem(x + 1, NX), lax.rem(x + NX - 1, NX)
    yop, xop = lax.rem(y + 2, NY), lax.rem(x + 2, NX)
    block = (y * NZ + z) * 2 + c

    def dev(cp_0=y, cp_1=z, cp_2=c, fs=x):
        return {"cp_0": cp_0, "cp_1": cp_1, "cp_2": cp_2, "fs": fs}

    sibling = dev(cp_2=o)
    following, preceding = dev(cp_0=yn, cp_1=zn), dev(cp_0=yp, cp_1=zp)

    started = []

    def copy(src, dst, kind, k, to):
        return pltpu.make_async_remote_copy(
            src_ref=src,
            dst_ref=dst,
            send_sem=snd[kind].at[k],
            recv_sem=rcv[kind].at[k],
            device_id=to,
            device_id_type=MESH,
        )

    def send(src, dst, kind, k, to):
        made = copy(src, dst, kind, k, to)
        made.start()
        started.append(made)

    def arrived(dst, kind, k):
        copy(dst, dst, kind, k, sibling).wait_recv()

    loads = {}

    def load(name, src, dst):
        loads[name] = pltpu.make_async_copy(src, dst, rcv["ld"].at[len(loads)])
        loads[name].start()

    mine = b.w.at[:, y, z, c, x]
    load("w0", yw_h.at[:, 0:256], b.w.at[0, y, z, c, x])
    load("w1", yw_h.at[:, 256:512], b.w.at[1, y, z, c, x])
    load("k", k_h, b.kw.at[0])
    load("q", q_h, b.q)
    for e in range(8):
        load("e%d" % e, emb_h.at[:, e * 512 : (e + 1) * 512], b.emb.at[e])
    load("cot", cot_h, b.cot)

    barrier = pltpu.get_barrier_semaphore()
    partners = [sibling, following, preceding]
    for d in range(1, NZ):
        for cc in (c, o):
            partners.append(dev(cp_1=lax.rem(z + d, NZ), cp_2=cc))
    for d in range(1, NY):
        for cc in (c, o):
            partners.append(dev(cp_0=lax.rem(y + d, NY), cp_2=cc))
        partners.append(dev(fs=lax.rem(x + d, NX)))
    for who in partners:
        pl.semaphore_signal(barrier, inc=1, device_id=who, device_id_type=MESH)
    pl.semaphore_wait(barrier, len(partners))

    loads["w0"].wait()
    loads["w1"].wait()
    for d in range(1, NZ):
        send(mine, mine, "w1", d, dev(cp_1=lax.rem(z + d, NZ)))
    loads["k"].wait()
    send(b.kw.at[0], b.kw.at[2], "k", 0, following)

    doc_t = jnp.transpose(jnp.broadcast_to(doc[...], (TOK, TOK)))
    row = lax.broadcasted_iota(jnp.int32, (TOK, TOK), 0) + block * TOK
    col = lax.broadcasted_iota(jnp.int32, (TOK, TOK), 1)
    for d in range(WIN + 1):
        listed = need[0, 0] == block - d
        for k in range(1, WIN + 1):
            listed = jnp.logical_or(listed, need[0, k] == block - d)
        shut = jnp.where(listed, 0, FAR)
        key_pos = col + (block - d) * TOK
        seen = jnp.logical_and(key_pos >= doc_t + shut, key_pos <= row)
        b.bias[:, d * TOK : (d + 1) * TOK] = jnp.where(seen, 0.0, MASKED)
    for kv in range(KV):
        b.r[kv, 2] = jnp.zeros((TOK, HEAD), F32)

    for d in range(1, NZ):
        arrived(mine, "w1", d)
    first, second = b.w.at[0, y, :, c, x], b.w.at[1, y, :, c, x]
    for d in range(1, 4):
        send(first, first, "w2", d - 1, dev(cp_0=lax.rem(y + d, NY)))
        send(second, second, "w2", d + 2, dev(fs=lax.rem(x + d, NX)))

    arrived(b.kw.at[2], "k", 0)
    send(b.kw.at[2], b.kw.at[4], "k", 1, following)
    send(b.kw.at[2 * c], b.kw.at[1], "k", 2, sibling)

    for d in range(6):
        arrived(first, "w2", d)

    def half_a(xx):
        return b.w.at[0, :, :, c, xx]

    def half_b(yy):
        return b.w.at[1, yy, :, c, :]

    def relay_a(xx, s):
        return b.w.at[0, :, 4 * s : 4 * s + 4, c, xx]

    def relay_b(yy, s):
        return b.w.at[1, yy, 4 * s : 4 * s + 4, c, :]

    send(half_a(x), half_a(x), "w3", 0, dev(fs=xup))
    send(half_a(x), half_a(x), "w3", 1, dev(fs=xdn))
    send(half_b(y), half_b(y), "w3", 2, dev(cp_0=yup))
    send(half_b(y), half_b(y), "w3", 3, dev(cp_0=ydn))
    send(half_a(x), half_a(x), "wd", 0, sibling)
    send(half_b(y), half_b(y), "wd", 1, sibling)

    arrived(b.kw.at[4], "k", 1)
    send(b.kw.at[2 + 2 * c], b.kw.at[3], "k", 3, sibling)
    arrived(b.kw.at[1], "k", 2)
    arrived(b.kw.at[3], "k", 3)
    loads["q"].wait()

    def head_probs(hd, carry):
        lanes = pl.ds(pl.multiple_of(hd * HEAD, HEAD), HEAD)
        key_lanes = pl.ds(pl.multiple_of(lax.div(hd, GROUP) * HEAD, HEAD), HEAD)
        keys = b.kw[:, :, key_lanes].reshape(SPAN, HEAD)
        b.s[...] = lax.dot_general(
            b.q[:, lanes], keys, (((1,), (1,)), ((), ())), preferred_element_type=F32
        )
        for n in range(8):
            rows = slice(n * 32, n * 32 + 32)
            score = b.s[rows, :] + b.bias[rows, :]
            largest = jnp.max(score, axis=-1, keepdims=True)
            weight = jnp.exp2((score - largest) * EXP2_SCALE)
            total = jnp.sum(weight, axis=-1, keepdims=True)
            b.p[hd, rows, :] = (weight * (1.0 / total)).astype(BF)
        return carry

    lax.fori_loop(0, 6, head_probs, 0)

    arrived(half_a(x), "w3", 0)
    send(relay_a(xdn, 0), relay_a(xdn, 0), "w3", 4, dev(fs=xup))
    send(half_a(xdn), half_a(xdn), "wd", 2, sibling)
    arrived(half_a(x), "w3", 1)
    send(relay_a(xup, 1), relay_a(xup, 1), "w3", 5, dev(fs=xdn))
    send(half_a(xup), half_a(xup), "wd", 3, sibling)
    arrived(half_b(y), "w3", 2)
    send(relay_b(ydn, 0), relay_b(ydn, 0), "w3", 6, dev(cp_0=yup))
    send(half_b(ydn), half_b(ydn), "wd", 4, sibling)
    arrived(half_b(y), "w3", 3)
    send(relay_b(yup, 1), relay_b(yup, 1), "w3", 7, dev(cp_0=ydn))
    send(half_b(yup), half_b(yup), "wd", 5, sibling)

    for e in range(8):
        loads["e%d" % e].wait()
    own = y * 2 + c
    kept = pltpu.make_async_copy(b.emb.at[own], b.ex.at[own], rcv["ld"].at[14])
    kept.start()
    send(b.emb.at[y * 2 + o], b.ex.at[own], "e", 0, sibling)
    for d in range(1, NY):
        yt = lax.rem(y + d, NY)
        for k, cc in enumerate((c, o)):
            send(b.emb.at[yt * 2 + cc], b.ex.at[own], "e", d * 2 + k, dev(cp_0=yt, cp_2=cc))

    lax.fori_loop(6, 16, head_probs, 0)

    for s in range(2):
        arrived(relay_a(x, s), "w3", 4 + s)
        send(relay_a(xop, s), relay_a(xop, s), "wd", 6 + s, sibling)
    for s in range(2):
        arrived(relay_b(y, s), "w3", 6 + s)
        send(relay_b(yop, s), relay_b(yop, s), "wd", 8 + s, sibling)
    for k in (0, 2, 3):
        arrived(half_a(x), "wd", k)
    for k in (1, 4, 5):
        arrived(half_b(y), "wd", k)
    for s in range(2):
        arrived(relay_a(x, s), "wd", 6 + s)
        arrived(relay_b(y, s), "wd", 8 + s)

    for h in range(2):
        b.vacc[h] = jnp.zeros((TOK, 256), F32)

        def add_chunk(e, carry):
            yy, low = lax.div(e, 2), 4 * lax.rem(e, 2)
            rows = b.w[h, yy, pl.ds(low, 4)].reshape(512, 256)
            b.vacc[h] += jnp.dot(b.emb[e], rows, preferred_element_type=F32)
            return carry

        lax.fori_loop(0, 8, add_chunk, 0)
        for k in range(2):
            kv = 2 * h + k
            b.vw[kv, 0] = b.vacc[h, :, k * HEAD : (k + 1) * HEAD].astype(BF)
            send(b.vw.at[kv, 0], b.vw.at[kv, 2], "v", kv, following)

    for kv in range(KV):
        arrived(b.vw.at[kv, 2], "v", kv)
        send(b.vw.at[kv, 2], b.vw.at[kv, 4], "v", 4 + kv, following)
        send(b.vw.at[kv, 2 * c], b.vw.at[kv, 1], "v", 8 + kv, sibling)

    def attend(kv):
        arrived(b.vw.at[kv, 1], "v", 8 + kv)
        arrived(b.vw.at[kv, 3], "v", 12 + kv)

        def one(k, carry):
            hd = kv * GROUP + k
            b.att[hd] = jnp.dot(
                b.p[hd], b.vw[kv].reshape(SPAN, HEAD), preferred_element_type=F32
            )
            return carry

        lax.fori_loop(0, GROUP, one, 0)

    for kv in range(KV):
        arrived(b.vw.at[kv, 4], "v", 4 + kv)
        send(b.vw.at[kv, 2 + 2 * c], b.vw.at[kv, 3], "v", 12 + kv, sibling)
        if kv:
            attend(kv - 1)
    attend(KV - 1)

    loads["cot"].wait()
    token_total = TOK * NY * NZ * 2 * NX

    def norm_rows(n, carry):
        rows = pl.ds(pl.multiple_of(n * 32, 32), 32)
        squares = jnp.zeros((32, HEAD), F32)
        crossed = jnp.zeros((32, HEAD), F32)
        for hd in range(16):
            a = b.att[hd, rows, :]
            squares += a * a
            crossed += a * b.cot[rows, hd * HEAD : (hd + 1) * HEAD].astype(F32)
        mean = jnp.sum(squares, axis=-1, keepdims=True) / 2048.0 + NORM_EPS
        inv = 1.0 / jnp.sqrt(mean)
        inner = jnp.sum(crossed, axis=-1, keepdims=True) / (2048.0 * token_total) * inv
        factor = inner * inv
        for hd in range(16):
            up = b.cot[rows, hd * HEAD : (hd + 1) * HEAD].astype(F32) / token_total
            b.og[hd, rows, :] = ((up - b.att[hd, rows, :] * factor) * inv).astype(BF)
        return carry

    lax.fori_loop(0, 8, norm_rows, 0)

    def grads(kv):
        def one(d, carry):
            lanes = pl.ds(pl.multiple_of(d * TOK, TOK), TOK)
            part = b.p[kv * GROUP : kv * GROUP + GROUP, :, lanes].reshape(GROUP * TOK, TOK)
            up = b.og[kv * GROUP : kv * GROUP + GROUP].reshape(GROUP * TOK, HEAD)
            b.dv[kv, d] = lax.dot_general(
                part, up, (((0,), (0,)), ((), ())), preferred_element_type=F32
            )
            return carry

        lax.fori_loop(0, WIN + 1, one, 0)
        send(b.dv.at[kv, 1], b.r.at[kv, 0], "r", 2 * kv, sibling)
        send(b.dv.at[kv, 3], b.r.at[kv, 1], "r", 2 * kv + 1, sibling)

    def leave_far(kv):
        arrived(b.r.at[kv, 0], "r", 2 * kv)
        arrived(b.r.at[kv, 1], "r", 2 * kv + 1)
        b.fo[kv] = (b.dv[kv, 4] + b.r[kv, 2 - c]).astype(BF)
        send(b.fo.at[kv], b.fi.at[kv], "f", kv, preceding)

    def leave_near(kv):
        arrived(b.fi.at[kv], "f", kv)
        b.go[kv] = (b.dv[kv, 2] + b.r[kv, 1 - c] + b.fi[kv].astype(F32)).astype(BF)
        send(b.go.at[kv], b.gi.at[kv], "g", kv, preceding)

    def vg_at(kv, yy, cc, rows=slice(None)):
        lanes = slice((kv % 2) * HEAD, (kv % 2) * HEAD + HEAD)
        return b.vg.at[kv // 2, yy * 2 + cc, rows, lanes]

    upper, lower = slice(0, 128), slice(128, 256)

    def settle(kv):
        arrived(b.gi.at[kv], "g", kv)
        total = b.dv[kv, 0] + b.r[kv, 2 * c] + b.gi[kv].astype(F32)
        b.vg[kv // 2, own, :, (kv % 2) * HEAD : (kv % 2) * HEAD + HEAD] = total.astype(BF)
        here = vg_at(kv, y, c)
        send(here, here, "vg", 4 * kv, dev(cp_0=yup))
        send(here, here, "vg", 4 * kv + 1, dev(cp_0=ydn))
        send(here, here, "vd", 4 * kv, sibling)

    def relay(kv):
        arrived(vg_at(kv, y, c), "vg", 4 * kv)
        part = vg_at(kv, ydn, c, upper)
        send(part, part, "vg", 4 * kv + 2, dev(cp_0=yup))
        send(vg_at(kv, ydn, c), vg_at(kv, ydn, c), "vd", 4 * kv + 1, sibling)
        arrived(vg_at(kv, y, c), "vg", 4 * kv + 1)
        part = vg_at(kv, yup, c, lower)
        send(part, part, "vg", 4 * kv + 3, dev(cp_0=ydn))
        send(vg_at(kv, yup, c), vg_at(kv, yup, c), "vd", 4 * kv + 2, sibling)

    def collect(kv):
        arrived(vg_at(kv, y, c, upper), "vg", 4 * kv + 2)
        arrived(vg_at(kv, y, c, lower), "vg", 4 * kv + 3)
        send(vg_at(kv, yop, c), vg_at(kv, yop, c), "vd", 4 * kv + 3, sibling)

    def complete(kv):
        for k in range(4):
            arrived(vg_at(kv, y, c), "vd", 4 * kv + k)

    grads(0)
    grads(1)
    leave_far(0)
    grads(2)
    leave_far(1)
    grads(3)
    leave_far(2)
    leave_far(3)
    for kv in range(KV):
        leave_near(kv)
    settle(0)
    settle(1)
    relay(0)
    settle(2)
    relay(1)
    collect(0)

    kept.wait()
    arrived(b.ex.at[0], "e", 0)
    for d in range(2, 8):
        arrived(b.ex.at[0], "e", d)

    settle(3)
    relay(2)
    collect(1)
    complete(0)
    complete(1)

    def product(h):
        grad = lax.dot_general(
            b.ex[...].reshape(8 * TOK, 512),
            b.vg[h].reshape(8 * TOK, 256),
            (((0,), (0,)), ((), ())),
            preferred_element_type=F32,
        )
        b.g[h] = grad.reshape(4, 2, NX, 16, 256)
        send(b.g.at[h, 0:2, :, xop], b.x1.at[h, 0], "x", 4 * h, dev(fs=xup))
        send(b.g.at[h, 2:4, :, xop], b.x1.at[h, 1], "x", 4 * h + 1, dev(fs=xdn))

    def across(h):
        arrived(b.x1.at[h, 0], "x", 4 * h)
        b.tx[h, 0, 0:2] = b.g[h, 0:2, :, xup] + b.x1[h, 0]
        b.tx[h, 0, 2:4] = b.g[h, 2:4, :, xup]
        send(b.tx.at[h, 0], b.x2.at[h, 0], "x", 4 * h + 2, dev(fs=xup))
        arrived(b.x1.at[h, 1], "x", 4 * h + 1)
        b.tx[h, 1, 0:2] = b.g[h, 0:2, :, xdn]
        b.tx[h, 1, 2:4] = b.g[h, 2:4, :, xdn] + b.x1[h, 1]
        send(b.tx.at[h, 1], b.x2.at[h, 1], "x", 4 * h + 3, dev(fs=xdn))

    def along(h):
        arrived(b.x2.at[h, 0], "x", 4 * h + 2)
        arrived(b.x2.at[h, 1], "x", 4 * h + 3)
        b.t[h] = b.g[h, :, :, x] + b.x2[h, 0] + b.x2[h, 1]
        for k in range(4):
            for cc in range(2):
                zt = 4 * c + k
                stays = jnp.logical_and(zt == z, c == cc)

                @pl.when(stays)
                def _():
                    b.rz[h, z] = b.t[h, k, cc]

                @pl.when(jnp.logical_not(stays))
                def _():
                    pltpu.make_async_remote_copy(
                        src_ref=b.t.at[h, k, cc],
                        dst_ref=b.rz.at[h, z],
                        send_sem=snd["z"].at[8 * h + 2 * k + cc],
                        recv_sem=rcv["z"].at[8 * h + z],
                        device_id=dev(cp_1=zt, cp_2=cc),
                        device_id_type=MESH,
                    ).start()

    def finish(h):
        for zs in range(NZ):
            stays = jnp.logical_and(zs == z, lax.div(z, 4) == c)

            @pl.when(jnp.logical_not(stays))
            def _():
                arrived(b.rz.at[h, 0], "z", 8 * h + zs)

        total = b.rz[h, 0]
        for zs in range(1, NZ):
            total = total + b.rz[h, zs]
        out[:, h * 256 : (h + 1) * 256] = total

    product(0)
    relay(3)
    collect(2)
    across(0)
    collect(3)
    complete(2)
    complete(3)
    product(1)
    along(0)
    across(1)
    along(1)
    finish(0)
    finish(1)

    for made in started:
        made.wait_send()
    for h in range(2):
        for k in range(4):
            for cc in range(2):
                stays = jnp.logical_and(4 * c + k == z, c == cc)

                @pl.when(jnp.logical_not(stays))
                def _():
                    copy(b.t.at[h, k, cc], b.rz.at[h, 0], "z", 8 * h + 2 * k + cc, sibling).wait_send()


def weight_gradient(need_ids, doc_start, embeds, queries, key_heads, cotangent, y_weight):
    any_space = pl.BlockSpec(memory_space=pl.ANY)
    vmem = pl.BlockSpec(memory_space=pltpu.VMEM)
    semaphores = [pltpu.SemaphoreType.DMA((n,)) for n in SEMAPHORES.values()]
    return pl.pallas_call(
        kernel,
        out_shape=jax.ShapeDtypeStruct((16, 512), F32),
        in_specs=[pl.BlockSpec(memory_space=pltpu.SMEM), vmem] + [any_space] * 5,
        out_specs=vmem,
        scratch_shapes=[pltpu.VMEM(shape, kind) for shape, kind in BUFFERS.values()]
        + semaphores
        + semaphores,
        compiler_params=pltpu.CompilerParams(
            collective_id=0, has_side_effects=True, vmem_limit_bytes=58 << 20
        ),
    )(need_ids, doc_start, embeds, queries, key_heads, cotangent, y_weight)


def on_device(
    embeds,
    queries,
    key_heads,
    cotangent,
    doc_start,
    need_ids,
    y_weight,
    z_weight,
    x_weight,
    second_moment,
):
    gradient = weight_gradient(
        need_ids[0], doc_start, embeds[0], queries[0], key_heads[0], cotangent[0], y_weight
    )
    moment_next = MOMENT_DECAY * second_moment + (1.0 - MOMENT_DECAY) * gradient * gradient
    z_next = z_weight - LEARN_RATE * (
        gradient / (jnp.sqrt(moment_next) + ADAM_EPS) + WEIGHT_DECAY * y_weight.astype(jnp.float32)
    )
    x_next = (1.0 - AVERAGE_MIX) * x_weight + AVERAGE_MIX * z_next
    y_next = ((1.0 - INTERP_BETA) * z_next + INTERP_BETA * x_next).astype(jnp.bfloat16)
    return (z_next, x_next, moment_next, y_next)


def solution(mesh):
    finer = Mesh(mesh.devices.reshape(NY, NZ, 2, mesh.shape["fs"]), CP_FS)
    return jax.shard_map(
        on_device,
        mesh=finer,
        in_specs=(
            P("fs", CP, None),
            P("fs", CP, None),
            P("fs", CP, None),
            P("fs", CP, None),
            P("fs", CP),
            P("fs", CP, None),
            P(CP_FS, None),
            P(CP_FS, None),
            P(CP_FS, None),
            P(CP_FS, None),
        ),
        out_specs=(P(CP_FS, None), P(CP_FS, None), P(CP_FS, None), P(CP_FS, None)),
        check_vma=False,
    )
```

```python
import math
from types import SimpleNamespace

import jax
import jax.numpy as jnp
from jax import lax
from jax.experimental import pallas as pl
from jax.experimental.pallas import tpu as pltpu
from jax.sharding import Mesh
from jax.sharding import PartitionSpec as P

HEAD = 128
KV = 4
WIN = 4
GROUP = 4
TOK = 256
SPAN = (WIN + 1) * TOK
NY, NZ, NX = 4, 8, 4
CP = ("cp_0", "cp_1", "cp_2")
CP_FS = ("cp_0", "cp_1", "cp_2", "fs")

NORM_EPS = 0.01
MOMENT_DECAY = 0.95
LEARN_RATE = 0.005
WEIGHT_DECAY = 0.1
ADAM_EPS = 1e-08
AVERAGE_MIX = 0.25
INTERP_BETA = 0.9
EXP2_SCALE = math.log2(math.e) / math.sqrt(HEAD)
MASKED = -1e30
FAR = 1 << 30

BF = jnp.bfloat16
F32 = jnp.float32
MESH = pl.DeviceIdType.MESH

BUFFERS = {
    "emb": ((TOK, 4096), BF),
    "w": ((2, NY, NZ, 2, NX, 16, 256), BF),
    "q": ((TOK, 2048), BF),
    "kw": ((5, TOK, 512), BF),
    "vw": ((KV, 5, TOK, HEAD), BF),
    "cot": ((TOK, 2048), BF),
    "p": ((16, TOK, SPAN), BF),
    "s": ((TOK, SPAN), F32),
    "bias": ((TOK, SPAN), F32),
    "att": ((16, TOK, HEAD), F32),
    "og": ((16, TOK, HEAD), BF),
    "dv": ((KV, 5, TOK, HEAD), F32),
    "r": ((KV, 3, TOK, HEAD), F32),
    "fo": ((KV, TOK, HEAD), BF),
    "fi": ((KV, TOK, HEAD), BF),
    "go": ((KV, TOK, HEAD), BF),
    "gi": ((KV, TOK, HEAD), BF),
    "vg": ((2, 8, TOK, 256), BF),
    "er": ((2, 2, 128, 512), BF),
    "ex": ((8, TOK, 512), BF),
    "g": ((2, 4, 2, NX, 16, 256), F32),
    "x1": ((2, 2, 2, 2, 16, 256), F32),
    "tx": ((2, 2, 4, 2, 16, 256), F32),
    "x2": ((2, 2, 4, 2, 16, 256), F32),
    "t": ((2, 4, 2, 16, 256), F32),
    "rz": ((2, NZ, 16, 256), F32),
}
SEMAPHORES = {
    "ld": 16,
    "w1": 8,
    "w2": 6,
    "w3": 8,
    "wd": 10,
    "k": 4,
    "v": 16,
    "e": 16,
    "r": 8,
    "f": 4,
    "g": 4,
    "vg": 16,
    "vd": 16,
    "x": 8,
    "z": 16,
}


def kernel(need, doc, emb_h, q_h, k_h, cot_h, yw_h, out, *scratch):
    names = list(BUFFERS)
    b = SimpleNamespace(**dict(zip(names, scratch)))
    rest = scratch[len(names) :]
    snd = dict(zip(SEMAPHORES, rest[: len(SEMAPHORES)]))
    rcv = dict(zip(SEMAPHORES, rest[len(SEMAPHORES) :]))

    y, z = lax.axis_index("cp_0"), lax.axis_index("cp_1")
    c, x = lax.axis_index("cp_2"), lax.axis_index("fs")
    o = 1 - c
    zn, yn = lax.rem(z + 1, NZ), lax.rem(y + lax.div(z + 1, NZ), NY)
    zp, yp = lax.rem(z + NZ - 1, NZ), lax.rem(y + NY - 1 + lax.div(z + NZ - 1, NZ), NY)
    yup, ydn = lax.rem(y + 1, NY), lax.rem(y + NY - 1, NY)
    xup, xdn = lax.rem(x + 1, NX), lax.rem(x + NX - 1, NX)
    yop, xop = lax.rem(y + 2, NY), lax.rem(x + 2, NX)
    block = (y * NZ + z) * 2 + c

    def dev(cp_0=y, cp_1=z, cp_2=c, fs=x):
        return {"cp_0": cp_0, "cp_1": cp_1, "cp_2": cp_2, "fs": fs}

    sibling = dev(cp_2=o)
    following, preceding = dev(cp_0=yn, cp_1=zn), dev(cp_0=yp, cp_1=zp)

    started = []

    def copy(src, dst, kind, k, to):
        return pltpu.make_async_remote_copy(
            src_ref=src,
            dst_ref=dst,
            send_sem=snd[kind].at[k],
            recv_sem=rcv[kind].at[k],
            device_id=to,
            device_id_type=MESH,
        )

    def send(src, dst, kind, k, to):
        made = copy(src, dst, kind, k, to)
        made.start()
        started.append(made)

    def arrived(dst, kind, k):
        copy(dst, dst, kind, k, sibling).wait_recv()

    loads = {}

    def load(name, src, dst):
        loads[name] = pltpu.make_async_copy(src, dst, rcv["ld"].at[len(loads)])
        loads[name].start()

    mine = b.w.at[:, y, z, c, x]
    load("w0", yw_h.at[:, 0:256], b.w.at[0, y, z, c, x])
    load("w1", yw_h.at[:, 256:512], b.w.at[1, y, z, c, x])
    load("k", k_h, b.kw.at[0])
    load("q", q_h, b.q)
    load("emb", emb_h, b.emb)
    load("cot", cot_h, b.cot)

    barrier = pltpu.get_barrier_semaphore()
    partners = [sibling, following, preceding]
    for d in range(1, NZ):
        for cc in (c, o):
            partners.append(dev(cp_1=lax.rem(z + d, NZ), cp_2=cc))
    for d in range(1, NY):
        for cc in (c, o):
            partners.append(dev(cp_0=lax.rem(y + d, NY), cp_2=cc))
        partners.append(dev(fs=lax.rem(x + d, NX)))
    for who in partners:
        pl.semaphore_signal(barrier, inc=1, device_id=who, device_id_type=MESH)
    pl.semaphore_wait(barrier, len(partners))

    loads["w0"].wait()
    loads["w1"].wait()
    for d in range(1, NZ):
        send(mine, mine, "w1", d, dev(cp_1=lax.rem(z + d, NZ)))
    loads["k"].wait()
    send(b.kw.at[0], b.kw.at[2], "k", 0, following)

    doc_t = jnp.transpose(jnp.broadcast_to(doc[...], (TOK, TOK)))
    row = lax.broadcasted_iota(jnp.int32, (TOK, TOK), 0) + block * TOK
    col = lax.broadcasted_iota(jnp.int32, (TOK, TOK), 1)
    for d in range(WIN + 1):
        listed = need[0, 0] == block - d
        for k in range(1, WIN + 1):
            listed = jnp.logical_or(listed, need[0, k] == block - d)
        shut = jnp.where(listed, 0, FAR)
        key_pos = col + (block - d) * TOK
        seen = jnp.logical_and(key_pos >= doc_t + shut, key_pos <= row)
        b.bias[:, d * TOK : (d + 1) * TOK] = jnp.where(seen, 0.0, MASKED)
    for kv in range(KV):
        b.r[kv, 2] = jnp.zeros((TOK, HEAD), F32)

    for d in range(1, NZ):
        arrived(mine, "w1", d)
    first, second = b.w.at[0, y, :, c, x], b.w.at[1, y, :, c, x]
    for d in range(1, 4):
        send(first, first, "w2", d - 1, dev(cp_0=lax.rem(y + d, NY)))
        send(second, second, "w2", d + 2, dev(fs=lax.rem(x + d, NX)))

    for d in range(6):
        arrived(first, "w2", d)

    def half_a(xx):
        return b.w.at[0, :, :, c, xx]

    def half_b(yy):
        return b.w.at[1, yy, :, c, :]

    def relay_a(xx, s):
        return b.w.at[0, :, 4 * s : 4 * s + 4, c, xx]

    def relay_b(yy, s):
        return b.w.at[1, yy, 4 * s : 4 * s + 4, c, :]

    send(half_a(x), half_a(x), "w3", 0, dev(fs=xup))
    send(half_a(x), half_a(x), "w3", 1, dev(fs=xdn))
    send(half_b(y), half_b(y), "w3", 2, dev(cp_0=yup))
    send(half_b(y), half_b(y), "w3", 3, dev(cp_0=ydn))

    arrived(b.kw.at[2], "k", 0)
    send(b.kw.at[2], b.kw.at[4], "k", 1, following)
    send(b.kw.at[2 * c], b.kw.at[1], "k", 2, sibling)
    send(half_a(x), half_a(x), "wd", 0, sibling)
    send(half_b(y), half_b(y), "wd", 1, sibling)

    arrived(b.kw.at[4], "k", 1)
    send(b.kw.at[2 + 2 * c], b.kw.at[3], "k", 3, sibling)

    arrived(half_a(x), "w3", 0)
    send(relay_a(xdn, 0), relay_a(xdn, 0), "w3", 4, dev(fs=xup))
    arrived(half_a(x), "w3", 1)
    send(relay_a(xup, 1), relay_a(xup, 1), "w3", 5, dev(fs=xdn))
    arrived(half_b(y), "w3", 2)
    send(relay_b(ydn, 0), relay_b(ydn, 0), "w3", 6, dev(cp_0=yup))
    arrived(half_b(y), "w3", 3)
    send(relay_b(yup, 1), relay_b(yup, 1), "w3", 7, dev(cp_0=ydn))
    send(half_a(xdn), half_a(xdn), "wd", 2, sibling)
    send(half_a(xup), half_a(xup), "wd", 3, sibling)
    send(half_b(ydn), half_b(ydn), "wd", 4, sibling)
    send(half_b(yup), half_b(yup), "wd", 5, sibling)

    arrived(b.kw.at[1], "k", 2)
    arrived(b.kw.at[3], "k", 3)
    loads["q"].wait()

    def head_probs(hd, carry):
        lanes = pl.ds(pl.multiple_of(hd * HEAD, HEAD), HEAD)
        key_lanes = pl.ds(pl.multiple_of(lax.div(hd, GROUP) * HEAD, HEAD), HEAD)
        keys = b.kw[:, :, key_lanes].reshape(SPAN, HEAD)
        b.s[...] = lax.dot_general(
            b.q[:, lanes], keys, (((1,), (1,)), ((), ())), preferred_element_type=F32
        )
        for n in range(8):
            rows = slice(n * 32, n * 32 + 32)
            score = b.s[rows, :] + b.bias[rows, :]
            largest = jnp.max(score, axis=-1, keepdims=True)
            weight = jnp.exp2((score - largest) * EXP2_SCALE)
            total = jnp.sum(weight, axis=-1, keepdims=True)
            b.p[hd, rows, :] = (weight * (1.0 / total)).astype(BF)
        return carry

    lax.fori_loop(0, 6, head_probs, 0)

    for s in range(2):
        arrived(relay_a(x, s), "w3", 4 + s)
        send(relay_a(xop, s), relay_a(xop, s), "wd", 6 + s, sibling)
    for s in range(2):
        arrived(relay_b(y, s), "w3", 6 + s)
        send(relay_b(yop, s), relay_b(yop, s), "wd", 8 + s, sibling)
    lax.fori_loop(6, 8, head_probs, 0)
    for k in (0, 2, 3):
        arrived(half_a(x), "wd", k)
    for k in (1, 4, 5):
        arrived(half_b(y), "wd", k)
    for s in range(2):
        arrived(relay_a(x, s), "wd", 6 + s)
        arrived(relay_b(y, s), "wd", 8 + s)

    loads["emb"].wait()
    for h in range(2):
        made = jnp.dot(b.emb[...], b.w[h].reshape(4096, 256), preferred_element_type=F32)
        for k in range(2):
            kv = 2 * h + k
            b.vw[kv, 0] = made[:, k * HEAD : (k + 1) * HEAD].astype(BF)
            send(b.vw.at[kv, 0], b.vw.at[kv, 2], "v", kv, following)

    def emb_at(yy, cc):
        return b.emb.at[:, pl.ds(pl.multiple_of((yy * 2 + cc) * 512, 512), 512)]

    def emb_part(yy, cc, s):
        return b.emb.at[
            128 * s : 128 * s + 128, pl.ds(pl.multiple_of((yy * 2 + cc) * 512, 512), 512)
        ]

    own = y * 2 + c
    kept = pltpu.make_async_copy(emb_at(y, c), b.ex.at[own], rcv["ld"].at[14])
    kept.start()
    send(emb_at(y, o), b.ex.at[own], "e", 0, sibling)
    for s, yt in enumerate((yup, ydn)):
        for k, cc in enumerate((c, o)):
            send(emb_part(yop, cc, s), b.er.at[s, k], "e", 8 + 2 * s + k, dev(cp_0=yt))
    for s, yt in enumerate((yup, ydn)):
        for k, cc in enumerate((c, o)):
            send(emb_at(yt, cc), b.ex.at[own], "e", 2 + 2 * s + k, dev(cp_0=yt, cp_2=cc))

    def pass_embeds():
        for s, (yt, yf) in enumerate(((yup, ydn), (ydn, yup))):
            for k, cc in enumerate((c, o)):
                arrived(b.er.at[s, k], "e", 8 + 2 * s + k)
                send(
                    b.er.at[s, k],
                    b.ex.at[yf * 2 + c, 128 * s : 128 * s + 128],
                    "e",
                    12 + 2 * s + k,
                    dev(cp_0=yt, cp_2=cc),
                )

    lax.fori_loop(8, 12, head_probs, 0)
    for kv in range(KV):
        arrived(b.vw.at[kv, 2], "v", kv)
        send(b.vw.at[kv, 2], b.vw.at[kv, 4], "v", 4 + kv, following)
        send(b.vw.at[kv, 2 * c], b.vw.at[kv, 1], "v", 8 + kv, sibling)
    lax.fori_loop(12, 16, head_probs, 0)
    near, far = 3 * TOK, 2 * TOK

    def attend_near(kv):
        arrived(b.vw.at[kv, 1], "v", 8 + kv)

        def one(k, carry):
            hd = kv * GROUP + k
            values = b.vw[kv, 0:3].reshape(near, HEAD)
            b.att[hd] = jnp.dot(b.p[hd, :, 0:near], values, preferred_element_type=F32)
            return carry

        lax.fori_loop(0, GROUP, one, 0)

    def attend_far(kv):
        arrived(b.vw.at[kv, 3], "v", 12 + kv)

        def one(k, carry):
            hd = kv * GROUP + k
            values = b.vw[kv, 3:5].reshape(far, HEAD)
            b.att[hd] += jnp.dot(b.p[hd, :, near:SPAN], values, preferred_element_type=F32)
            return carry

        lax.fori_loop(0, GROUP, one, 0)

    def pass_values(kv):
        arrived(b.vw.at[kv, 4], "v", 4 + kv)
        send(b.vw.at[kv, 2 + 2 * c], b.vw.at[kv, 3], "v", 12 + kv, sibling)

    attend_near(0)
    attend_near(1)
    pass_values(0)
    attend_near(2)
    attend_near(3)
    pass_values(1)
    attend_far(0)
    pass_values(2)
    attend_far(1)
    pass_embeds()
    pass_values(3)
    attend_far(2)
    attend_far(3)

    loads["cot"].wait()
    token_total = TOK * NY * NZ * 2 * NX

    def norm_rows(n, carry):
        rows = pl.ds(pl.multiple_of(n * 32, 32), 32)
        squares = jnp.zeros((32, HEAD), F32)
        crossed = jnp.zeros((32, HEAD), F32)
        for hd in range(16):
            a = b.att[hd, rows, :]
            squares += a * a
            crossed += a * b.cot[rows, hd * HEAD : (hd + 1) * HEAD].astype(F32)
        mean = jnp.sum(squares, axis=-1, keepdims=True) / 2048.0 + NORM_EPS
        inv = 1.0 / jnp.sqrt(mean)
        inner = jnp.sum(crossed, axis=-1, keepdims=True) / (2048.0 * token_total) * inv
        factor = inner * inv
        for hd in range(16):
            up = b.cot[rows, hd * HEAD : (hd + 1) * HEAD].astype(F32) / token_total
            b.og[hd, rows, :] = ((up - b.att[hd, rows, :] * factor) * inv).astype(BF)
        return carry

    lax.fori_loop(0, 8, norm_rows, 0)

    def grads(kv, low, high):
        def one(d, carry):
            lanes = pl.ds(pl.multiple_of(d * TOK, TOK), TOK)
            part = b.p[kv * GROUP : kv * GROUP + GROUP, :, lanes].reshape(GROUP * TOK, TOK)
            up = b.og[kv * GROUP : kv * GROUP + GROUP].reshape(GROUP * TOK, HEAD)
            b.dv[kv, d] = lax.dot_general(
                part, up, (((0,), (0,)), ((), ())), preferred_element_type=F32
            )
            return carry

        lax.fori_loop(low, high, one, 0)

    def grads_far(kv):
        grads(kv, 3, 5)
        send(b.dv.at[kv, 3], b.r.at[kv, 1], "r", 2 * kv + 1, sibling)

    def grads_near(kv):
        grads(kv, 1, 3)
        send(b.dv.at[kv, 1], b.r.at[kv, 0], "r", 2 * kv, sibling)

    def leave_far(kv):
        arrived(b.r.at[kv, 1], "r", 2 * kv + 1)
        b.fo[kv] = (b.dv[kv, 4] + b.r[kv, 2 - c]).astype(BF)
        send(b.fo.at[kv], b.fi.at[kv], "f", kv, preceding)

    def leave_near(kv):
        arrived(b.r.at[kv, 0], "r", 2 * kv)
        arrived(b.fi.at[kv], "f", kv)
        b.go[kv] = (b.dv[kv, 2] + b.r[kv, 1 - c] + b.fi[kv].astype(F32)).astype(BF)
        send(b.go.at[kv], b.gi.at[kv], "g", kv, preceding)

    def vg_at(kv, yy, cc, rows=slice(None)):
        lanes = slice((kv % 2) * HEAD, (kv % 2) * HEAD + HEAD)
        return b.vg.at[kv // 2, yy * 2 + cc, rows, lanes]

    upper, lower = slice(0, 128), slice(128, 256)

    def settle(kv):
        arrived(b.gi.at[kv], "g", kv)
        total = b.dv[kv, 0] + b.r[kv, 2 * c] + b.gi[kv].astype(F32)
        b.vg[kv // 2, own, :, (kv % 2) * HEAD : (kv % 2) * HEAD + HEAD] = total.astype(BF)
        here = vg_at(kv, y, c)
        send(here, here, "vg", 4 * kv, dev(cp_0=yup))
        send(here, here, "vg", 4 * kv + 1, dev(cp_0=ydn))
        send(here, here, "vd", 4 * kv, sibling)

    def relay(kv):
        arrived(vg_at(kv, y, c), "vg", 4 * kv)
        part = vg_at(kv, ydn, c, upper)
        send(part, part, "vg", 4 * kv + 2, dev(cp_0=yup))
        send(vg_at(kv, ydn, c), vg_at(kv, ydn, c), "vd", 4 * kv + 1, sibling)
        arrived(vg_at(kv, y, c), "vg", 4 * kv + 1)
        part = vg_at(kv, yup, c, lower)
        send(part, part, "vg", 4 * kv + 3, dev(cp_0=ydn))
        send(vg_at(kv, yup, c), vg_at(kv, yup, c), "vd", 4 * kv + 2, sibling)

    def collect(kv):
        arrived(vg_at(kv, y, c, upper), "vg", 4 * kv + 2)
        arrived(vg_at(kv, y, c, lower), "vg", 4 * kv + 3)
        send(vg_at(kv, yop, c), vg_at(kv, yop, c), "vd", 4 * kv + 3, sibling)

    def complete(kv):
        for k in range(4):
            arrived(vg_at(kv, y, c), "vd", 4 * kv + k)

    grads_far(0)
    grads_far(1)
    leave_far(0)
    grads_far(2)
    leave_far(1)
    grads_far(3)
    leave_far(2)
    grads_near(0)
    leave_far(3)
    grads_near(1)
    grads_near(2)
    leave_near(0)
    grads_near(3)
    leave_near(1)
    grads(0, 0, 1)
    grads(1, 0, 1)
    leave_near(2)
    grads(2, 0, 1)
    grads(3, 0, 1)
    leave_near(3)
    kept.wait()
    for k in (0, 2, 3, 4, 5):
        arrived(b.ex.at[0], "e", k)
    for k in range(12, 16):
        arrived(b.er.at[0, 0], "e", k)

    settle(0)
    settle(1)
    settle(2)
    relay(0)
    settle(3)
    relay(1)
    collect(0)
    relay(2)
    collect(1)
    complete(0)
    complete(1)

    def product(h):
        grad = lax.dot_general(
            b.ex[...].reshape(8 * TOK, 512),
            b.vg[h].reshape(8 * TOK, 256),
            (((0,), (0,)), ((), ())),
            preferred_element_type=F32,
        )
        b.g[h] = grad.reshape(4, 2, NX, 16, 256)
        send(b.g.at[h, 0:2, :, xop], b.x1.at[h, 0], "x", 4 * h, dev(fs=xup))
        send(b.g.at[h, 2:4, :, xop], b.x1.at[h, 1], "x", 4 * h + 1, dev(fs=xdn))

    def across(h):
        arrived(b.x1.at[h, 0], "x", 4 * h)
        b.tx[h, 0, 0:2] = b.g[h, 0:2, :, xup] + b.x1[h, 0]
        b.tx[h, 0, 2:4] = b.g[h, 2:4, :, xup]
        send(b.tx.at[h, 0], b.x2.at[h, 0], "x", 4 * h + 2, dev(fs=xup))
        arrived(b.x1.at[h, 1], "x", 4 * h + 1)
        b.tx[h, 1, 0:2] = b.g[h, 0:2, :, xdn]
        b.tx[h, 1, 2:4] = b.g[h, 2:4, :, xdn] + b.x1[h, 1]
        send(b.tx.at[h, 1], b.x2.at[h, 1], "x", 4 * h + 3, dev(fs=xdn))

    def along(h):
        arrived(b.x2.at[h, 0], "x", 4 * h + 2)
        arrived(b.x2.at[h, 1], "x", 4 * h + 3)
        b.t[h] = b.g[h, :, :, x] + b.x2[h, 0] + b.x2[h, 1]
        for k in range(4):
            for cc in range(2):
                zt = 4 * c + k
                stays = jnp.logical_and(zt == z, c == cc)

                @pl.when(stays)
                def _():
                    b.rz[h, z] = b.t[h, k, cc]

                @pl.when(jnp.logical_not(stays))
                def _():
                    pltpu.make_async_remote_copy(
                        src_ref=b.t.at[h, k, cc],
                        dst_ref=b.rz.at[h, z],
                        send_sem=snd["z"].at[8 * h + 2 * k + cc],
                        recv_sem=rcv["z"].at[8 * h + z],
                        device_id=dev(cp_1=zt, cp_2=cc),
                        device_id_type=MESH,
                    ).start()

    def finish(h):
        for zs in range(NZ):
            stays = jnp.logical_and(zs == z, lax.div(z, 4) == c)

            @pl.when(jnp.logical_not(stays))
            def _():
                arrived(b.rz.at[h, 0], "z", 8 * h + zs)

        total = b.rz[h, 0]
        for zs in range(1, NZ):
            total = total + b.rz[h, zs]
        out[:, h * 256 : (h + 1) * 256] = total

    relay(3)
    product(0)
    collect(2)
    across(0)
    collect(3)
    complete(2)
    complete(3)
    product(1)
    along(0)
    across(1)
    along(1)
    finish(0)
    finish(1)

    for made in started:
        made.wait_send()
    for h in range(2):
        for k in range(4):
            for cc in range(2):
                stays = jnp.logical_and(4 * c + k == z, c == cc)

                @pl.when(jnp.logical_not(stays))
                def _():
                    copy(b.t.at[h, k, cc], b.rz.at[h, 0], "z", 8 * h + 2 * k + cc, sibling).wait_send()


def weight_gradient(need_ids, doc_start, embeds, queries, key_heads, cotangent, y_weight):
    any_space = pl.BlockSpec(memory_space=pl.ANY)
    vmem = pl.BlockSpec(memory_space=pltpu.VMEM)
    semaphores = [pltpu.SemaphoreType.DMA((n,)) for n in SEMAPHORES.values()]
    return pl.pallas_call(
        kernel,
        out_shape=jax.ShapeDtypeStruct((16, 512), F32),
        in_specs=[pl.BlockSpec(memory_space=pltpu.SMEM), vmem] + [any_space] * 5,
        out_specs=vmem,
        scratch_shapes=[pltpu.VMEM(shape, kind) for shape, kind in BUFFERS.values()]
        + semaphores
        + semaphores,
        compiler_params=pltpu.CompilerParams(
            collective_id=0, has_side_effects=True, vmem_limit_bytes=58 << 20
        ),
    )(need_ids, doc_start, embeds, queries, key_heads, cotangent, y_weight)


def on_device(
    embeds,
    queries,
    key_heads,
    cotangent,
    doc_start,
    need_ids,
    y_weight,
    z_weight,
    x_weight,
    second_moment,
):
    gradient = weight_gradient(
        need_ids[0], doc_start, embeds[0], queries[0], key_heads[0], cotangent[0], y_weight
    )
    moment_next = MOMENT_DECAY * second_moment + (1.0 - MOMENT_DECAY) * gradient * gradient
    z_next = z_weight - LEARN_RATE * (
        gradient / (jnp.sqrt(moment_next) + ADAM_EPS) + WEIGHT_DECAY * y_weight.astype(jnp.float32)
    )
    x_next = (1.0 - AVERAGE_MIX) * x_weight + AVERAGE_MIX * z_next
    y_next = ((1.0 - INTERP_BETA) * z_next + INTERP_BETA * x_next).astype(jnp.bfloat16)
    return (z_next, x_next, moment_next, y_next)


def solution(mesh):
    finer = Mesh(mesh.devices.reshape(NY, NZ, 2, mesh.shape["fs"]), CP_FS)
    return jax.shard_map(
        on_device,
        mesh=finer,
        in_specs=(
            P("fs", CP, None),
            P("fs", CP, None),
            P("fs", CP, None),
            P("fs", CP, None),
            P("fs", CP),
            P("fs", CP, None),
            P(CP_FS, None),
            P(CP_FS, None),
            P(CP_FS, None),
            P(CP_FS, None),
        ),
        out_specs=(P(CP_FS, None), P(CP_FS, None), P(CP_FS, None), P(CP_FS, None)),
        check_vma=False,
    )
```

```python
import math
from types import SimpleNamespace

import jax
import jax.numpy as jnp
from jax import lax
from jax.experimental import pallas as pl
from jax.experimental.pallas import tpu as pltpu
from jax.sharding import Mesh
from jax.sharding import PartitionSpec as P

HEAD = 128
KV = 4
WIN = 4
GROUP = 4
TOK = 256
SPAN = (WIN + 1) * TOK
NY, NZ, NX = 4, 8, 4
CP = ("cp_0", "cp_1", "cp_2")
CP_FS = ("cp_0", "cp_1", "cp_2", "fs")

NORM_EPS = 0.01
MOMENT_DECAY = 0.95
LEARN_RATE = 0.005
WEIGHT_DECAY = 0.1
ADAM_EPS = 1e-08
AVERAGE_MIX = 0.25
INTERP_BETA = 0.9
EXP2_SCALE = math.log2(math.e) / math.sqrt(HEAD)
MASKED = -1e30
FAR = 1 << 30

BF = jnp.bfloat16
F32 = jnp.float32
MESH = pl.DeviceIdType.MESH

BUFFERS = {
    "emb": ((TOK, 4096), BF),
    "w": ((2, NY, NZ, 2, NX, 16, 256), BF),
    "q": ((TOK, 2048), BF),
    "kw": ((5, TOK, 512), BF),
    "vw": ((KV, 5, TOK, HEAD), BF),
    "cot": ((TOK, 2048), BF),
    "p": ((16, TOK, SPAN), BF),
    "s": ((TOK, SPAN), F32),
    "bias": ((TOK, SPAN), F32),
    "att": ((16, TOK, HEAD), F32),
    "og": ((16, TOK, HEAD), BF),
    "dv": ((KV, 5, TOK, HEAD), F32),
    "r": ((KV, 3, TOK, HEAD), F32),
    "fo": ((KV, TOK, HEAD), BF),
    "fi": ((KV, TOK, HEAD), BF),
    "go": ((KV, TOK, HEAD), BF),
    "gi": ((KV, TOK, HEAD), BF),
    "vg": ((2, 8, TOK, 256), BF),
    "et": ((NY, NZ, 2, NX, 16, TOK), BF),
    "er": ((2, 2, 2, NZ, 16, TOK), BF),
    "ex": ((NY, NZ, 16, 8 * TOK), BF),
    "g": ((2, NY, NZ, 16, 256), F32),
    "x1": ((2, 2, 4, 16, 256), F32),
    "tx": ((2, 2, NZ, 16, 256), F32),
    "x2": ((2, 2, NZ, 16, 256), F32),
    "t": ((2, NZ, 16, 256), F32),
    "rz": ((2, NZ, 16, 256), F32),
}
SEMAPHORES = {
    "ld": 16,
    "w1": 8,
    "w2": 6,
    "w3": 8,
    "wd": 10,
    "k": 8,
    "v": 16,
    "e": 16,
    "r": 8,
    "f": 4,
    "g": 4,
    "vg": 16,
    "vd": 16,
    "x": 8,
    "z": 16,
}


def kernel(need, doc, emb_h, q_h, k_h, cot_h, yw_h, out, *scratch):
    names = list(BUFFERS)
    b = SimpleNamespace(**dict(zip(names, scratch)))
    rest = scratch[len(names) :]
    snd = dict(zip(SEMAPHORES, rest[: len(SEMAPHORES)]))
    rcv = dict(zip(SEMAPHORES, rest[len(SEMAPHORES) :]))

    y, z = lax.axis_index("cp_0"), lax.axis_index("cp_1")
    c, x = lax.axis_index("cp_2"), lax.axis_index("fs")
    o = 1 - c
    zn, yn = lax.rem(z + 1, NZ), lax.rem(y + lax.div(z + 1, NZ), NY)
    zp, yp = lax.rem(z + NZ - 1, NZ), lax.rem(y + NY - 1 + lax.div(z + NZ - 1, NZ), NY)
    yup, ydn = lax.rem(y + 1, NY), lax.rem(y + NY - 1, NY)
    xup, xdn = lax.rem(x + 1, NX), lax.rem(x + NX - 1, NX)
    yop, xop = lax.rem(y + 2, NY), lax.rem(x + 2, NX)
    block = (y * NZ + z) * 2 + c

    def dev(cp_0=y, cp_1=z, cp_2=c, fs=x):
        return {"cp_0": cp_0, "cp_1": cp_1, "cp_2": cp_2, "fs": fs}

    sibling = dev(cp_2=o)
    following, preceding = dev(cp_0=yn, cp_1=zn), dev(cp_0=yp, cp_1=zp)

    started = []

    def copy(src, dst, kind, k, to):
        return pltpu.make_async_remote_copy(
            src_ref=src,
            dst_ref=dst,
            send_sem=snd[kind].at[k],
            recv_sem=rcv[kind].at[k],
            device_id=to,
            device_id_type=MESH,
        )

    def send(src, dst, kind, k, to):
        made = copy(src, dst, kind, k, to)
        made.start()
        started.append(made)

    def arrived(dst, kind, k):
        copy(dst, dst, kind, k, sibling).wait_recv()

    loads = {}

    def load(name, src, dst):
        loads[name] = pltpu.make_async_copy(src, dst, rcv["ld"].at[len(loads)])
        loads[name].start()

    mine = b.w.at[:, y, z, c, x]
    load("w0", yw_h.at[:, 0:256], b.w.at[0, y, z, c, x])
    load("w1", yw_h.at[:, 256:512], b.w.at[1, y, z, c, x])
    load("k", k_h, b.kw.at[0])
    load("q", q_h, b.q)
    load("emb", emb_h, b.emb)
    load("cot", cot_h, b.cot)

    barrier = pltpu.get_barrier_semaphore()
    partners = [sibling, following, preceding]
    for d in range(1, NZ):
        partners.append(dev(cp_1=lax.rem(z + d, NZ)))
    for d in range(1, NY):
        partners.append(dev(cp_0=lax.rem(y + d, NY)))
    for d in range(1, NX):
        for cc in (c, o):
            partners.append(dev(fs=lax.rem(x + d, NX), cp_2=cc))
    for who in partners:
        pl.semaphore_signal(barrier, inc=1, device_id=who, device_id_type=MESH)
    pl.semaphore_wait(barrier, len(partners))

    loads["w0"].wait()
    loads["w1"].wait()
    for d in range(1, NZ):
        send(mine, mine, "w1", d, dev(cp_1=lax.rem(z + d, NZ)))

    doc_t = jnp.transpose(jnp.broadcast_to(doc[...], (TOK, TOK)))
    row = lax.broadcasted_iota(jnp.int32, (TOK, TOK), 0) + block * TOK
    col = lax.broadcasted_iota(jnp.int32, (TOK, TOK), 1)
    for d in range(WIN + 1):
        listed = need[0, 0] == block - d
        for k in range(1, WIN + 1):
            listed = jnp.logical_or(listed, need[0, k] == block - d)
        shut = jnp.where(listed, 0, FAR)
        key_pos = col + (block - d) * TOK
        seen = jnp.logical_and(key_pos >= doc_t + shut, key_pos <= row)
        b.bias[:, d * TOK : (d + 1) * TOK] = jnp.where(seen, 0.0, MASKED)
    for kv in range(KV):
        b.r[kv, 2] = jnp.zeros((TOK, HEAD), F32)

    def turn(e, carry):
        lanes = pl.ds(pl.multiple_of(e * 512, 512), 512)
        turned = jnp.transpose(b.emb[:, lanes]).reshape(4, 2, NX, 16, TOK)
        b.et[lax.div(e, 2), pl.ds(4 * lax.rem(e, 2), 4)] = turned
        return carry

    loads["emb"].wait()

    for d in range(1, NZ):
        arrived(mine, "w1", d)
    first, second = b.w.at[0, y, :, c, x], b.w.at[1, y, :, c, x]
    for d in range(1, 4):
        send(first, first, "w2", d - 1, dev(cp_0=lax.rem(y + d, NY)))
        send(second, second, "w2", d + 2, dev(fs=lax.rem(x + d, NX)))

    lax.fori_loop(0, 8, turn, 0)

    for d in range(6):
        arrived(first, "w2", d)

    def half_a(xx):
        return b.w.at[0, :, :, c, xx]

    def half_b(yy):
        return b.w.at[1, yy, :, c, :]

    def relay_a(xx, s):
        return b.w.at[0, :, 4 * s : 4 * s + 4, c, xx]

    def relay_b(yy, s):
        return b.w.at[1, yy, 4 * s : 4 * s + 4, c, :]

    send(half_a(x), half_a(x), "w3", 0, dev(fs=xup))
    send(half_a(x), half_a(x), "w3", 1, dev(fs=xdn))
    send(half_b(y), half_b(y), "w3", 2, dev(cp_0=yup))
    send(half_b(y), half_b(y), "w3", 3, dev(cp_0=ydn))

    send(half_a(x), half_a(x), "wd", 0, sibling)
    send(half_b(y), half_b(y), "wd", 1, sibling)

    loads["k"].wait()

    def keys_at(d, s):
        return b.kw.at[d, 128 * s : 128 * s + 128]

    def pass_keys(s):
        arrived(keys_at(2, s), "k", s)
        send(keys_at(2, s), keys_at(4, s), "k", 2 + s, following)
        send(keys_at(2 * c, s), keys_at(1, s), "k", 4 + s, sibling)

    keys_out = [copy(keys_at(0, s), keys_at(2, s), "k", s, following) for s in range(2)]
    started.extend(keys_out)

    @pl.when(z != NZ - 1)
    def _():
        for made in keys_out:
            made.start()

    arrived(half_a(x), "w3", 0)
    send(relay_a(xdn, 0), relay_a(xdn, 0), "w3", 4, dev(fs=xup))
    arrived(half_a(x), "w3", 1)
    send(relay_a(xup, 1), relay_a(xup, 1), "w3", 5, dev(fs=xdn))
    arrived(half_b(y), "w3", 3)
    for s in range(2):
        send(relay_b(yup, s), relay_b(yup, s), "w3", 6 + s, dev(cp_0=ydn))
    send(half_a(xdn), half_a(xdn), "wd", 2, sibling)
    send(half_a(xup), half_a(xup), "wd", 3, sibling)
    send(half_b(yup), half_b(yup), "wd", 5, sibling)

    @pl.when(z == NZ - 1)
    def _():
        for made in keys_out:
            made.start()

    arrived(half_b(y), "w3", 2)
    send(half_b(ydn), half_b(ydn), "wd", 4, sibling)
    pass_keys(0)
    pass_keys(1)
    for s in range(2):
        arrived(keys_at(4, s), "k", 2 + s)
        send(keys_at(2 + 2 * c, s), keys_at(3, s), "k", 6 + s, sibling)
    loads["q"].wait()

    def head_probs(hd, carry):
        lanes = pl.ds(pl.multiple_of(hd * HEAD, HEAD), HEAD)
        key_lanes = pl.ds(pl.multiple_of(lax.div(hd, GROUP) * HEAD, HEAD), HEAD)
        keys = b.kw[:, :, key_lanes].reshape(SPAN, HEAD)
        b.s[...] = lax.dot_general(
            b.q[:, lanes], keys, (((1,), (1,)), ((), ())), preferred_element_type=F32
        )
        for n in range(8):
            rows = slice(n * 32, n * 32 + 32)
            score = b.s[rows, :] + b.bias[rows, :]
            largest = jnp.max(score, axis=-1, keepdims=True)
            weight = jnp.exp2((score - largest) * EXP2_SCALE)
            total = jnp.sum(weight, axis=-1, keepdims=True)
            b.p[hd, rows, :] = (weight * (1.0 / total)).astype(BF)
        return carry

    for s in range(2):
        arrived(relay_a(x, s), "w3", 4 + s)
        send(relay_a(xop, s), relay_a(xop, s), "wd", 6 + s, sibling)
    for s in range(2):
        arrived(relay_b(y, s), "w3", 6 + s)
        send(relay_b(yop, s), relay_b(yop, s), "wd", 8 + s, sibling)
    for k in (0, 2, 3):
        arrived(half_a(x), "wd", k)
    for k in (1, 4, 5):
        arrived(half_b(y), "wd", k)
    for s in range(2):
        arrived(relay_a(x, s), "wd", 6 + s)
        arrived(relay_b(y, s), "wd", 8 + s)

    def columns_of(blk):
        return pl.ds(pl.multiple_of(blk * TOK, TOK), TOK)

    own = x * 2 + c
    here = b.ex.at[:, :, :, columns_of(own)]
    kept = pltpu.make_async_copy(b.et.at[:, :, c, x], here, rcv["ld"].at[14])
    kept.start()
    send(b.et.at[:, :, o, x], here, "e", 0, sibling)
    for s, xt in enumerate((xup, xdn)):
        for k, cc in enumerate((c, o)):
            part = b.et.at[2 * s : 2 * s + 2, :, cc, xop]
            send(part, b.er.at[s, k], "e", 8 + 2 * s + k, dev(fs=xt))
    for s, xt in enumerate((xup, xdn)):
        for k, cc in enumerate((c, o)):
            send(b.et.at[:, :, cc, xt], here, "e", 2 + 2 * s + k, dev(fs=xt, cp_2=cc))

    def pass_embeds():
        for s, (xt, xf) in enumerate(((xup, xdn), (xdn, xup))):
            for k, cc in enumerate((c, o)):
                arrived(b.er.at[s, k], "e", 8 + 2 * s + k)
                there = b.ex.at[2 * s : 2 * s + 2, :, :, columns_of(xf * 2 + c)]
                send(b.er.at[s, k], there, "e", 12 + 2 * s + k, dev(fs=xt, cp_2=cc))

    for h in range(2):
        made = jnp.dot(b.emb[...], b.w[h].reshape(4096, 256), preferred_element_type=F32)
        for k in range(2):
            kv = 2 * h + k
            b.vw[kv, 0] = made[:, k * HEAD : (k + 1) * HEAD].astype(BF)
            send(b.vw.at[kv, 0], b.vw.at[kv, 2], "v", kv, following)

    def pass_near(kv):
        arrived(b.vw.at[kv, 2], "v", kv)
        send(b.vw.at[kv, 2], b.vw.at[kv, 4], "v", 4 + kv, following)
        send(b.vw.at[kv, 2 * c], b.vw.at[kv, 1], "v", 8 + kv, sibling)

    def pass_far(kv):
        arrived(b.vw.at[kv, 4], "v", 4 + kv)
        send(b.vw.at[kv, 2 + 2 * c], b.vw.at[kv, 3], "v", 12 + kv, sibling)

    def attend(kv):
        arrived(b.vw.at[kv, 1], "v", 8 + kv)
        arrived(b.vw.at[kv, 3], "v", 12 + kv)

        def one(k, carry):
            hd = kv * GROUP + k
            values = b.vw[kv].reshape(SPAN, HEAD)
            b.att[hd] = jnp.dot(b.p[hd], values, preferred_element_type=F32)
            return carry

        lax.fori_loop(0, GROUP, one, 0)

    for s in range(2):
        arrived(keys_at(1, s), "k", 4 + s)
        arrived(keys_at(3, s), "k", 6 + s)
    lax.fori_loop(0, 7, head_probs, 0)
    pass_near(0)
    pass_near(1)
    lax.fori_loop(7, 9, head_probs, 0)
    pass_near(2)
    lax.fori_loop(9, 11, head_probs, 0)
    pass_near(3)
    pass_embeds()
    lax.fori_loop(11, 16, head_probs, 0)
    pass_far(0)
    pass_far(1)
    attend(0)
    pass_far(2)
    attend(1)
    pass_far(3)
    attend(2)
    attend(3)

    loads["cot"].wait()
    token_total = TOK * NY * NZ * 2 * NX

    def norm_rows(n, carry):
        rows = pl.ds(pl.multiple_of(n * 32, 32), 32)
        squares = jnp.zeros((32, HEAD), F32)
        crossed = jnp.zeros((32, HEAD), F32)
        for hd in range(16):
            a = b.att[hd, rows, :]
            squares += a * a
            crossed += a * b.cot[rows, hd * HEAD : (hd + 1) * HEAD].astype(F32)
        mean = jnp.sum(squares, axis=-1, keepdims=True) / 2048.0 + NORM_EPS
        inv = 1.0 / jnp.sqrt(mean)
        inner = jnp.sum(crossed, axis=-1, keepdims=True) / (2048.0 * token_total) * inv
        factor = inner * inv
        for hd in range(16):
            up = b.cot[rows, hd * HEAD : (hd + 1) * HEAD].astype(F32) / token_total
            b.og[hd, rows, :] = ((up - b.att[hd, rows, :] * factor) * inv).astype(BF)
        return carry

    lax.fori_loop(0, 8, norm_rows, 0)

    def grads(kv, low, high):
        def one(d, carry):
            lanes = pl.ds(pl.multiple_of(d * TOK, TOK), TOK)
            part = b.p[kv * GROUP : kv * GROUP + GROUP, :, lanes].reshape(GROUP * TOK, TOK)
            up = b.og[kv * GROUP : kv * GROUP + GROUP].reshape(GROUP * TOK, HEAD)
            b.dv[kv, d] = lax.dot_general(
                part, up, (((0,), (0,)), ((), ())), preferred_element_type=F32
            )
            return carry

        lax.fori_loop(low, high, one, 0)

    def grads_far(kv):
        grads(kv, 3, 5)
        send(b.dv.at[kv, 3], b.r.at[kv, 1], "r", 2 * kv + 1, sibling)

    def grads_near(kv):
        grads(kv, 1, 3)
        send(b.dv.at[kv, 1], b.r.at[kv, 0], "r", 2 * kv, sibling)

    def leave_far(kv):
        arrived(b.r.at[kv, 1], "r", 2 * kv + 1)
        b.fo[kv] = (b.dv[kv, 4] + b.r[kv, 2 - c]).astype(BF)
        send(b.fo.at[kv], b.fi.at[kv], "f", kv, preceding)

    def leave_near(kv):
        arrived(b.r.at[kv, 0], "r", 2 * kv)
        arrived(b.fi.at[kv], "f", kv)
        b.go[kv] = (b.dv[kv, 2] + b.r[kv, 1 - c] + b.fi[kv].astype(F32)).astype(BF)
        send(b.go.at[kv], b.gi.at[kv], "g", kv, preceding)

    def vg_at(kv, xx, cc, rows=slice(None)):
        lanes = slice((kv % 2) * HEAD, (kv % 2) * HEAD + HEAD)
        return b.vg.at[kv // 2, xx * 2 + cc, rows, lanes]

    upper, lower = slice(0, 128), slice(128, 256)

    def settle(kv):
        arrived(b.gi.at[kv], "g", kv)
        total = b.dv[kv, 0] + b.r[kv, 2 * c] + b.gi[kv].astype(F32)
        b.vg[kv // 2, x * 2 + c, :, (kv % 2) * HEAD : (kv % 2) * HEAD + HEAD] = total.astype(BF)
        mine = vg_at(kv, x, c)
        send(mine, mine, "vg", 4 * kv, dev(fs=xup))
        send(mine, mine, "vg", 4 * kv + 1, dev(fs=xdn))
        send(mine, mine, "vd", 4 * kv, sibling)

    def relay(kv):
        arrived(vg_at(kv, x, c), "vg", 4 * kv)
        part = vg_at(kv, xdn, c, upper)
        send(part, part, "vg", 4 * kv + 2, dev(fs=xup))
        send(vg_at(kv, xdn, c), vg_at(kv, xdn, c), "vd", 4 * kv + 1, sibling)
        arrived(vg_at(kv, x, c), "vg", 4 * kv + 1)
        part = vg_at(kv, xup, c, lower)
        send(part, part, "vg", 4 * kv + 3, dev(fs=xdn))
        send(vg_at(kv, xup, c), vg_at(kv, xup, c), "vd", 4 * kv + 2, sibling)

    def collect(kv):
        arrived(vg_at(kv, x, c, upper), "vg", 4 * kv + 2)
        arrived(vg_at(kv, x, c, lower), "vg", 4 * kv + 3)
        send(vg_at(kv, xop, c), vg_at(kv, xop, c), "vd", 4 * kv + 3, sibling)

    def complete(kv):
        for k in range(4):
            arrived(vg_at(kv, x, c), "vd", 4 * kv + k)

    grads_far(0)
    grads_far(1)
    leave_far(0)
    grads_far(2)
    leave_far(1)
    grads_far(3)
    leave_far(2)
    grads_near(0)
    leave_far(3)
    grads_near(1)
    grads_near(2)
    leave_near(0)
    grads_near(3)
    leave_near(1)
    grads(0, 0, 1)
    grads(1, 0, 1)
    leave_near(2)
    grads(2, 0, 1)
    grads(3, 0, 1)
    leave_near(3)
    kept.wait()
    for k in (0, 2, 3, 4, 5):
        arrived(here, "e", k)
    for k in range(12, 16):
        arrived(b.er.at[0, 0], "e", k)

    settle(0)
    settle(1)
    settle(2)
    relay(0)
    settle(3)
    relay(1)
    collect(0)
    relay(2)
    collect(1)
    complete(0)
    complete(1)

    def product(h):
        grad = jnp.dot(
            b.ex[...].reshape(512, 8 * TOK),
            b.vg[h].reshape(8 * TOK, 256),
            preferred_element_type=F32,
        )
        b.g[h] = grad.reshape(NY, NZ, 16, 256)
        send(b.g.at[h, yop, 0:4], b.x1.at[h, 0], "x", 4 * h, dev(cp_0=yup))
        send(b.g.at[h, yop, 4:8], b.x1.at[h, 1], "x", 4 * h + 1, dev(cp_0=ydn))

    def across(h):
        arrived(b.x1.at[h, 0], "x", 4 * h)
        b.tx[h, 0, 0:4] = b.g[h, yup, 0:4] + b.x1[h, 0]
        b.tx[h, 0, 4:8] = b.g[h, yup, 4:8]
        send(b.tx.at[h, 0], b.x2.at[h, 0], "x", 4 * h + 2, dev(cp_0=yup))
        arrived(b.x1.at[h, 1], "x", 4 * h + 1)
        b.tx[h, 1, 0:4] = b.g[h, ydn, 0:4]
        b.tx[h, 1, 4:8] = b.g[h, ydn, 4:8] + b.x1[h, 1]
        send(b.tx.at[h, 1], b.x2.at[h, 1], "x", 4 * h + 3, dev(cp_0=ydn))

    def along(h):
        arrived(b.x2.at[h, 0], "x", 4 * h + 2)
        arrived(b.x2.at[h, 1], "x", 4 * h + 3)
        b.t[h] = b.g[h, y] + b.x2[h, 0] + b.x2[h, 1]
        for d in (4, 3, 5, 2, 6, 1, 7):
            zt = lax.rem(z + d, NZ)
            send(b.t.at[h, zt], b.rz.at[h, z], "z", 8 * h + d, dev(cp_1=zt))

    def finish(h):
        total = b.t[h, z]
        for d in (1, 7, 2, 6, 3, 5, 4):
            arrived(b.rz.at[h, 0], "z", 8 * h + d)
            total = total + b.rz[h, lax.rem(z + NZ - d, NZ)]
        out[:, h * 256 : (h + 1) * 256] = total

    relay(3)
    product(0)
    collect(2)
    across(0)
    collect(3)
    complete(2)
    complete(3)
    product(1)
    along(0)
    across(1)
    along(1)
    finish(0)
    finish(1)

    for made in started:
        made.wait_send()


def weight_gradient(need_ids, doc_start, embeds, queries, key_heads, cotangent, y_weight):
    any_space = pl.BlockSpec(memory_space=pl.ANY)
    vmem = pl.BlockSpec(memory_space=pltpu.VMEM)
    semaphores = [pltpu.SemaphoreType.DMA((n,)) for n in SEMAPHORES.values()]
    return pl.pallas_call(
        kernel,
        out_shape=jax.ShapeDtypeStruct((16, 512), F32),
        in_specs=[pl.BlockSpec(memory_space=pltpu.SMEM), vmem] + [any_space] * 5,
        out_specs=vmem,
        scratch_shapes=[pltpu.VMEM(shape, kind) for shape, kind in BUFFERS.values()]
        + semaphores
        + semaphores,
        compiler_params=pltpu.CompilerParams(
            collective_id=0, has_side_effects=True, vmem_limit_bytes=58 << 20
        ),
    )(need_ids, doc_start, embeds, queries, key_heads, cotangent, y_weight)


def on_device(
    embeds,
    queries,
    key_heads,
    cotangent,
    doc_start,
    need_ids,
    y_weight,
    z_weight,
    x_weight,
    second_moment,
):
    gradient = weight_gradient(
        need_ids[0], doc_start, embeds[0], queries[0], key_heads[0], cotangent[0], y_weight
    )
    moment_next = MOMENT_DECAY * second_moment + (1.0 - MOMENT_DECAY) * gradient * gradient
    z_next = z_weight - LEARN_RATE * (
        gradient / (jnp.sqrt(moment_next) + ADAM_EPS) + WEIGHT_DECAY * y_weight.astype(jnp.float32)
    )
    x_next = (1.0 - AVERAGE_MIX) * x_weight + AVERAGE_MIX * z_next
    y_next = ((1.0 - INTERP_BETA) * z_next + INTERP_BETA * x_next).astype(jnp.bfloat16)
    return (z_next, x_next, moment_next, y_next)


def solution(mesh):
    finer = Mesh(mesh.devices.reshape(NY, NZ, 2, mesh.shape["fs"]), CP_FS)
    return jax.shard_map(
        on_device,
        mesh=finer,
        in_specs=(
            P("fs", CP, None),
            P("fs", CP, None),
            P("fs", CP, None),
            P("fs", CP, None),
            P("fs", CP),
            P("fs", CP, None),
            P(CP_FS, None),
            P(CP_FS, None),
            P(CP_FS, None),
            P(CP_FS, None),
        ),
        out_specs=(P(CP_FS, None), P(CP_FS, None), P(CP_FS, None), P(CP_FS, None)),
        check_vma=False,
    )
```

```python
import math
from types import SimpleNamespace

import jax
import jax.numpy as jnp
from jax import lax
from jax.experimental import pallas as pl
from jax.experimental.pallas import tpu as pltpu
from jax.sharding import Mesh
from jax.sharding import PartitionSpec as P

HEAD = 128
KV = 4
WIN = 4
GROUP = 4
TOK = 256
SPAN = (WIN + 1) * TOK
NY, NZ, NX = 4, 8, 4
CP = ("cp_0", "cp_1", "cp_2")
CP_FS = ("cp_0", "cp_1", "cp_2", "fs")

NORM_EPS = 0.01
MOMENT_DECAY = 0.95
LEARN_RATE = 0.005
WEIGHT_DECAY = 0.1
ADAM_EPS = 1e-08
AVERAGE_MIX = 0.25
INTERP_BETA = 0.9
EXP2_SCALE = math.log2(math.e) / math.sqrt(HEAD)
MASKED = -1e30
FAR = 1 << 30

BF = jnp.bfloat16
F32 = jnp.float32
MESH = pl.DeviceIdType.MESH

BUFFERS = {
    "emb": ((TOK, 4096), BF),
    "w": ((2, NY, NZ, 2, NX, 16, 256), BF),
    "q": ((TOK, 2048), BF),
    "kw": ((5, TOK, 512), BF),
    "vw": ((KV, 5, TOK, HEAD), BF),
    "cot": ((TOK, 2048), BF),
    "p": ((16, TOK, SPAN), BF),
    "s": ((TOK, SPAN), F32),
    "bias": ((TOK, SPAN), F32),
    "att": ((16, TOK, HEAD), F32),
    "sq": ((TOK, HEAD), F32),
    "cr": ((TOK, HEAD), F32),
    "og": ((16, TOK, HEAD), BF),
    "dv": ((KV, 5, TOK, HEAD), F32),
    "r": ((KV, 3, TOK, HEAD), F32),
    "fo": ((KV, TOK, HEAD), BF),
    "fi": ((KV, TOK, HEAD), BF),
    "go": ((KV, TOK, HEAD), BF),
    "gi": ((KV, TOK, HEAD), BF),
    "vg": ((2, 8, TOK, 256), BF),
    "et": ((NY, NZ, 2, NX, 16, TOK), BF),
    "er": ((2, 2, 2, NZ, 16, TOK), BF),
    "ex": ((NY, NZ, 16, 8 * TOK), BF),
    "g": ((2, NY, NZ, 16, 256), F32),
    "g1": ((2, NZ, 16, 256), BF),
    "x1": ((2, 2, 4, 16, 256), BF),
    "tx": ((2, 2, NZ, 16, 256), BF),
    "x2": ((2, 2, NZ, 16, 256), BF),
    "t": ((2, NZ, 16, 256), F32),
    "tz": ((2, NZ, 16, 256), BF),
    "rz": ((2, NZ, 16, 256), BF),
}
SEMAPHORES = {
    "ld": 16,
    "w1": 8,
    "w2": 6,
    "w3": 8,
    "wd": 10,
    "k": 8,
    "v": 16,
    "e": 16,
    "r": 8,
    "f": 4,
    "g": 4,
    "vg": 16,
    "vd": 16,
    "x": 8,
    "z": 16,
}


def kernel(need, doc, emb_h, q_h, k_h, cot_h, yw_h, out, *scratch):
    names = list(BUFFERS)
    b = SimpleNamespace(**dict(zip(names, scratch)))
    rest = scratch[len(names) :]
    snd = dict(zip(SEMAPHORES, rest[: len(SEMAPHORES)]))
    rcv = dict(zip(SEMAPHORES, rest[len(SEMAPHORES) :]))

    y, z = lax.axis_index("cp_0"), lax.axis_index("cp_1")
    c, x = lax.axis_index("cp_2"), lax.axis_index("fs")
    o = 1 - c
    zn, yn = lax.rem(z + 1, NZ), lax.rem(y + lax.div(z + 1, NZ), NY)
    zp, yp = lax.rem(z + NZ - 1, NZ), lax.rem(y + NY - 1 + lax.div(z + NZ - 1, NZ), NY)
    yup, ydn = lax.rem(y + 1, NY), lax.rem(y + NY - 1, NY)
    xup, xdn = lax.rem(x + 1, NX), lax.rem(x + NX - 1, NX)
    yop, xop = lax.rem(y + 2, NY), lax.rem(x + 2, NX)
    block = (y * NZ + z) * 2 + c

    def dev(cp_0=y, cp_1=z, cp_2=c, fs=x):
        return {"cp_0": cp_0, "cp_1": cp_1, "cp_2": cp_2, "fs": fs}

    sibling = dev(cp_2=o)
    following, preceding = dev(cp_0=yn, cp_1=zn), dev(cp_0=yp, cp_1=zp)

    started = []

    def copy(src, dst, kind, k, to):
        return pltpu.make_async_remote_copy(
            src_ref=src,
            dst_ref=dst,
            send_sem=snd[kind].at[k],
            recv_sem=rcv[kind].at[k],
            device_id=to,
            device_id_type=MESH,
        )

    def send(src, dst, kind, k, to):
        made = copy(src, dst, kind, k, to)
        made.start()
        started.append(made)

    def arrived(dst, kind, k):
        copy(dst, dst, kind, k, sibling).wait_recv()

    loads = {}

    def load(name, src, dst):
        loads[name] = pltpu.make_async_copy(src, dst, rcv["ld"].at[len(loads)])
        loads[name].start()

    mine = b.w.at[:, y, z, c, x]
    load("w0", yw_h.at[:, 0:256], b.w.at[0, y, z, c, x])
    load("w1", yw_h.at[:, 256:512], b.w.at[1, y, z, c, x])
    load("k", k_h, b.kw.at[0])
    load("q", q_h, b.q)
    load("emb", emb_h, b.emb)
    load("cot", cot_h, b.cot)

    barrier = pltpu.get_barrier_semaphore()
    partners = [sibling, following, preceding]
    for d in range(1, NZ):
        partners.append(dev(cp_1=lax.rem(z + d, NZ)))
    for d in range(1, NY):
        partners.append(dev(cp_0=lax.rem(y + d, NY)))
    for d in range(1, NX):
        for cc in (c, o):
            partners.append(dev(fs=lax.rem(x + d, NX), cp_2=cc))
    for who in partners:
        pl.semaphore_signal(barrier, inc=1, device_id=who, device_id_type=MESH)
    pl.semaphore_wait(barrier, len(partners))

    loads["w0"].wait()
    loads["w1"].wait()
    for d in range(1, NZ):
        send(mine, mine, "w1", d, dev(cp_1=lax.rem(z + d, NZ)))

    doc_t = jnp.transpose(jnp.broadcast_to(doc[...], (TOK, TOK)))
    row = lax.broadcasted_iota(jnp.int32, (TOK, TOK), 0) + block * TOK
    col = lax.broadcasted_iota(jnp.int32, (TOK, TOK), 1)
    for d in range(WIN + 1):
        listed = need[0, 0] == block - d
        for k in range(1, WIN + 1):
            listed = jnp.logical_or(listed, need[0, k] == block - d)
        shut = jnp.where(listed, 0, FAR)
        key_pos = col + (block - d) * TOK
        seen = jnp.logical_and(key_pos >= doc_t + shut, key_pos <= row)
        b.bias[:, d * TOK : (d + 1) * TOK] = jnp.where(seen, 0.0, MASKED)
    for kv in range(KV):
        b.r[kv, 2] = jnp.zeros((TOK, HEAD), F32)
    b.sq[...] = jnp.zeros((TOK, HEAD), F32)
    b.cr[...] = jnp.zeros((TOK, HEAD), F32)

    def turn(e, carry):
        lanes = pl.ds(pl.multiple_of(e * 512, 512), 512)
        turned = jnp.transpose(b.emb[:, lanes]).reshape(4, 2, NX, 16, TOK)
        b.et[lax.div(e, 2), pl.ds(4 * lax.rem(e, 2), 4)] = turned
        return carry

    loads["emb"].wait()

    for d in range(1, NZ):
        arrived(mine, "w1", d)
    first, second = b.w.at[0, y, :, c, x], b.w.at[1, y, :, c, x]
    for d in range(1, 4):
        send(first, first, "w2", d - 1, dev(cp_0=lax.rem(y + d, NY)))
        send(second, second, "w2", d + 2, dev(fs=lax.rem(x + d, NX)))

    lax.fori_loop(0, 8, turn, 0)

    for d in range(6):
        arrived(first, "w2", d)

    def half_a(xx):
        return b.w.at[0, :, :, c, xx]

    def half_b(yy):
        return b.w.at[1, yy, :, c, :]

    def relay_a(xx, s):
        return b.w.at[0, :, 4 * s : 4 * s + 4, c, xx]

    def relay_b(yy, s):
        return b.w.at[1, yy, 4 * s : 4 * s + 4, c, :]

    send(half_a(x), half_a(x), "w3", 0, dev(fs=xup))
    send(half_a(x), half_a(x), "w3", 1, dev(fs=xdn))
    send(half_b(y), half_b(y), "w3", 2, dev(cp_0=yup))
    send(half_b(y), half_b(y), "w3", 3, dev(cp_0=ydn))

    send(half_a(x), half_a(x), "wd", 0, sibling)
    send(half_b(y), half_b(y), "wd", 1, sibling)

    loads["k"].wait()

    def keys_at(d, s):
        return b.kw.at[d, 128 * s : 128 * s + 128]

    def pass_keys(s):
        arrived(keys_at(2, s), "k", s)
        send(keys_at(2, s), keys_at(4, s), "k", 2 + s, following)
        send(keys_at(2 * c, s), keys_at(1, s), "k", 4 + s, sibling)

    keys_out = [copy(keys_at(0, s), keys_at(2, s), "k", s, following) for s in range(2)]
    started.extend(keys_out)

    @pl.when(z != NZ - 1)
    def _():
        for made in keys_out:
            made.start()

    arrived(half_a(x), "w3", 0)
    send(relay_a(xdn, 0), relay_a(xdn, 0), "w3", 4, dev(fs=xup))
    arrived(half_a(x), "w3", 1)
    send(relay_a(xup, 1), relay_a(xup, 1), "w3", 5, dev(fs=xdn))
    arrived(half_b(y), "w3", 2)
    send(relay_b(ydn, 0), relay_b(ydn, 0), "w3", 6, dev(cp_0=yup))
    arrived(half_b(y), "w3", 3)
    send(relay_b(yup, 1), relay_b(yup, 1), "w3", 7, dev(cp_0=ydn))

    @pl.when(z == NZ - 1)
    def _():
        for made in keys_out:
            made.start()

    send(half_a(xdn), half_a(xdn), "wd", 2, sibling)
    send(half_a(xup), half_a(xup), "wd", 3, sibling)
    send(half_b(ydn), half_b(ydn), "wd", 4, sibling)
    send(half_b(yup), half_b(yup), "wd", 5, sibling)
    pass_keys(0)
    pass_keys(1)
    loads["q"].wait()
    for s in range(2):
        arrived(relay_a(x, s), "w3", 4 + s)
        send(relay_a(xop, s), relay_a(xop, s), "wd", 6 + s, sibling)
    for s in range(2):
        arrived(relay_b(y, s), "w3", 6 + s)
        send(relay_b(yop, s), relay_b(yop, s), "wd", 8 + s, sibling)
    for s in range(2):
        arrived(keys_at(4, s), "k", 2 + s)
        send(keys_at(2 + 2 * c, s), keys_at(3, s), "k", 6 + s, sibling)

    def head_probs(hd, carry):
        lanes = pl.ds(pl.multiple_of(hd * HEAD, HEAD), HEAD)
        key_lanes = pl.ds(pl.multiple_of(lax.div(hd, GROUP) * HEAD, HEAD), HEAD)
        keys = b.kw[:, :, key_lanes].reshape(SPAN, HEAD)
        b.s[...] = lax.dot_general(
            b.q[:, lanes], keys, (((1,), (1,)), ((), ())), preferred_element_type=F32
        )
        for n in range(8):
            rows = slice(n * 32, n * 32 + 32)
            score = b.s[rows, :] + b.bias[rows, :]
            largest = jnp.max(score, axis=-1, keepdims=True)
            weight = jnp.exp2((score - largest) * EXP2_SCALE)
            total = jnp.sum(weight, axis=-1, keepdims=True)
            b.p[hd, rows, :] = (weight * (1.0 / total)).astype(BF)
        return carry

    for k in (0, 2, 3):
        arrived(half_a(x), "wd", k)
    for k in (1, 4, 5):
        arrived(half_b(y), "wd", k)
    for s in range(2):
        arrived(relay_a(x, s), "wd", 6 + s)
        arrived(relay_b(y, s), "wd", 8 + s)

    def columns_of(blk):
        return pl.ds(pl.multiple_of(blk * TOK, TOK), TOK)

    own = x * 2 + c
    here = b.ex.at[:, :, :, columns_of(own)]
    kept = pltpu.make_async_copy(b.et.at[:, :, c, x], here, rcv["ld"].at[14])
    kept.start()
    send(b.et.at[:, :, o, x], here, "e", 0, sibling)
    for s, xt in enumerate((xup, xdn)):
        for k, cc in enumerate((c, o)):
            part = b.et.at[2 * s : 2 * s + 2, :, cc, xop]
            send(part, b.er.at[s, k], "e", 8 + 2 * s + k, dev(fs=xt))
    for s, xt in enumerate((xup, xdn)):
        for k, cc in enumerate((c, o)):
            send(b.et.at[:, :, cc, xt], here, "e", 2 + 2 * s + k, dev(fs=xt, cp_2=cc))

    def pass_embeds():
        for s, (xt, xf) in enumerate(((xup, xdn), (xdn, xup))):
            for k, cc in enumerate((c, o)):
                arrived(b.er.at[s, k], "e", 8 + 2 * s + k)
                there = b.ex.at[2 * s : 2 * s + 2, :, :, columns_of(xf * 2 + c)]
                send(b.er.at[s, k], there, "e", 12 + 2 * s + k, dev(fs=xt, cp_2=cc))

    for h in range(2):
        made = jnp.dot(b.emb[...], b.w[h].reshape(4096, 256), preferred_element_type=F32)
        for k in range(2):
            kv = 2 * h + k
            b.vw[kv, 0] = made[:, k * HEAD : (k + 1) * HEAD].astype(BF)
            send(b.vw.at[kv, 0], b.vw.at[kv, 2], "v", kv, following)

    def pass_near(kv):
        arrived(b.vw.at[kv, 2], "v", kv)
        send(b.vw.at[kv, 2], b.vw.at[kv, 4], "v", 4 + kv, following)
        send(b.vw.at[kv, 2 * c], b.vw.at[kv, 1], "v", 8 + kv, sibling)

    def pass_far(kv):
        arrived(b.vw.at[kv, 4], "v", 4 + kv)
        send(b.vw.at[kv, 2 + 2 * c], b.vw.at[kv, 3], "v", 12 + kv, sibling)

    def attend(kv):
        arrived(b.vw.at[kv, 1], "v", 8 + kv)
        arrived(b.vw.at[kv, 3], "v", 12 + kv)

        def one(k, carry):
            hd = kv * GROUP + k
            values = b.vw[kv].reshape(SPAN, HEAD)
            made = jnp.dot(b.p[hd], values, preferred_element_type=F32)
            b.att[hd] = made
            lanes = pl.ds(pl.multiple_of(hd * HEAD, HEAD), HEAD)
            b.sq[...] += made * made
            b.cr[...] += made * b.cot[:, lanes].astype(F32)
            return carry

        lax.fori_loop(0, GROUP, one, 0)

    for s in range(2):
        arrived(keys_at(1, s), "k", 4 + s)
        arrived(keys_at(3, s), "k", 6 + s)
    loads["cot"].wait()
    lax.fori_loop(0, 8, head_probs, 0)
    pass_near(0)
    pass_near(1)
    lax.fori_loop(8, 11, head_probs, 0)
    pass_near(2)
    lax.fori_loop(11, 13, head_probs, 0)
    pass_near(3)
    pass_embeds()
    lax.fori_loop(13, 15, head_probs, 0)
    pass_far(0)
    lax.fori_loop(15, 16, head_probs, 0)
    pass_far(1)
    attend(0)
    pass_far(2)
    attend(1)
    pass_far(3)
    attend(2)
    attend(3)

    token_total = TOK * NY * NZ * 2 * NX

    def norm_rows(n, carry):
        rows = pl.ds(pl.multiple_of(n * 32, 32), 32)
        mean = jnp.sum(b.sq[rows, :], axis=-1, keepdims=True) / 2048.0 + NORM_EPS
        inv = 1.0 / jnp.sqrt(mean)
        inner = jnp.sum(b.cr[rows, :], axis=-1, keepdims=True) / (2048.0 * token_total) * inv
        factor = inner * inv
        for hd in range(16):
            up = b.cot[rows, hd * HEAD : (hd + 1) * HEAD].astype(F32) / token_total
            b.og[hd, rows, :] = ((up - b.att[hd, rows, :] * factor) * inv).astype(BF)
        return carry

    lax.fori_loop(0, 8, norm_rows, 0)

    def grads(kv, low, high):
        def one(d, carry):
            lanes = pl.ds(pl.multiple_of(d * TOK, TOK), TOK)
            part = b.p[kv * GROUP : kv * GROUP + GROUP, :, lanes].reshape(GROUP * TOK, TOK)
            up = b.og[kv * GROUP : kv * GROUP + GROUP].reshape(GROUP * TOK, HEAD)
            b.dv[kv, d] = lax.dot_general(
                part, up, (((0,), (0,)), ((), ())), preferred_element_type=F32
            )
            return carry

        lax.fori_loop(low, high, one, 0)

    def grads_far(kv):
        grads(kv, 3, 5)
        send(b.dv.at[kv, 3], b.r.at[kv, 1], "r", 2 * kv + 1, sibling)

    def grads_near(kv):
        grads(kv, 1, 3)
        send(b.dv.at[kv, 1], b.r.at[kv, 0], "r", 2 * kv, sibling)

    def leave_far(kv):
        arrived(b.r.at[kv, 1], "r", 2 * kv + 1)
        b.fo[kv] = (b.dv[kv, 4] + b.r[kv, 2 - c]).astype(BF)
        send(b.fo.at[kv], b.fi.at[kv], "f", kv, preceding)

    def leave_near(kv):
        arrived(b.r.at[kv, 0], "r", 2 * kv)
        arrived(b.fi.at[kv], "f", kv)
        b.go[kv] = (b.dv[kv, 2] + b.r[kv, 1 - c] + b.fi[kv].astype(F32)).astype(BF)
        send(b.go.at[kv], b.gi.at[kv], "g", kv, preceding)

    def vg_at(kv, xx, cc, rows=slice(None)):
        lanes = slice((kv % 2) * HEAD, (kv % 2) * HEAD + HEAD)
        return b.vg.at[kv // 2, xx * 2 + cc, rows, lanes]

    upper, lower = slice(0, 128), slice(128, 256)

    def settle(kv):
        arrived(b.gi.at[kv], "g", kv)
        total = b.dv[kv, 0] + b.r[kv, 2 * c] + b.gi[kv].astype(F32)
        b.vg[kv // 2, x * 2 + c, :, (kv % 2) * HEAD : (kv % 2) * HEAD + HEAD] = total.astype(BF)
        mine = vg_at(kv, x, c)
        send(mine, mine, "vg", 4 * kv, dev(fs=xup))
        send(mine, mine, "vg", 4 * kv + 1, dev(fs=xdn))
        send(mine, mine, "vd", 4 * kv, sibling)

    def relay(kv):
        arrived(vg_at(kv, x, c), "vg", 4 * kv)
        part = vg_at(kv, xdn, c, upper)
        send(part, part, "vg", 4 * kv + 2, dev(fs=xup))
        send(vg_at(kv, xdn, c), vg_at(kv, xdn, c), "vd", 4 * kv + 1, sibling)
        arrived(vg_at(kv, x, c), "vg", 4 * kv + 1)
        part = vg_at(kv, xup, c, lower)
        send(part, part, "vg", 4 * kv + 3, dev(fs=xdn))
        send(vg_at(kv, xup, c), vg_at(kv, xup, c), "vd", 4 * kv + 2, sibling)

    def collect(kv):
        arrived(vg_at(kv, x, c, upper), "vg", 4 * kv + 2)
        arrived(vg_at(kv, x, c, lower), "vg", 4 * kv + 3)
        send(vg_at(kv, xop, c), vg_at(kv, xop, c), "vd", 4 * kv + 3, sibling)

    def complete(kv):
        for k in range(4):
            arrived(vg_at(kv, x, c), "vd", 4 * kv + k)

    grads_far(0)
    grads_far(1)
    leave_far(0)
    grads_far(2)
    leave_far(1)
    grads_far(3)
    leave_far(2)
    grads_near(0)
    leave_far(3)
    grads_near(1)
    grads_near(2)
    leave_near(0)
    grads_near(3)
    leave_near(1)
    grads(0, 0, 1)
    grads(1, 0, 1)
    leave_near(2)
    grads(2, 0, 1)
    grads(3, 0, 1)
    leave_near(3)
    kept.wait()
    for k in (0, 2, 3, 4, 5):
        arrived(here, "e", k)
    for k in range(12, 16):
        arrived(b.er.at[0, 0], "e", k)

    settle(0)
    settle(1)
    settle(2)
    relay(0)
    settle(3)
    relay(1)
    collect(0)
    relay(2)
    collect(1)
    complete(0)
    complete(1)

    def product(h):
        grad = jnp.dot(
            b.ex[...].reshape(512, 8 * TOK),
            b.vg[h].reshape(8 * TOK, 256),
            preferred_element_type=F32,
        )
        b.g[h] = grad.reshape(NY, NZ, 16, 256)
        b.g1[h] = b.g[h, yop].astype(BF)
        send(b.g1.at[h, 0:4], b.x1.at[h, 0], "x", 4 * h, dev(cp_0=yup))
        send(b.g1.at[h, 4:8], b.x1.at[h, 1], "x", 4 * h + 1, dev(cp_0=ydn))

    def across(h):
        arrived(b.x1.at[h, 0], "x", 4 * h)
        b.tx[h, 0, 0:4] = (b.g[h, yup, 0:4] + b.x1[h, 0].astype(F32)).astype(BF)
        b.tx[h, 0, 4:8] = b.g[h, yup, 4:8].astype(BF)
        send(b.tx.at[h, 0], b.x2.at[h, 0], "x", 4 * h + 2, dev(cp_0=yup))
        arrived(b.x1.at[h, 1], "x", 4 * h + 1)
        b.tx[h, 1, 0:4] = b.g[h, ydn, 0:4].astype(BF)
        b.tx[h, 1, 4:8] = (b.g[h, ydn, 4:8] + b.x1[h, 1].astype(F32)).astype(BF)
        send(b.tx.at[h, 1], b.x2.at[h, 1], "x", 4 * h + 3, dev(cp_0=ydn))

    def along(h):
        arrived(b.x2.at[h, 0], "x", 4 * h + 2)
        arrived(b.x2.at[h, 1], "x", 4 * h + 3)
        b.t[h] = b.g[h, y] + b.x2[h, 0].astype(F32) + b.x2[h, 1].astype(F32)
        b.tz[h] = b.t[h].astype(BF)
        for d in (4, 3, 5, 2, 6, 1, 7):
            zt = lax.rem(z + d, NZ)
            send(b.tz.at[h, zt], b.rz.at[h, z], "z", 8 * h + d, dev(cp_1=zt))

    def finish(h):
        total = b.t[h, z]
        for d in (1, 7, 2, 6, 3, 5, 4):
            arrived(b.rz.at[h, 0], "z", 8 * h + d)
            total = total + b.rz[h, lax.rem(z + NZ - d, NZ)].astype(F32)
        out[:, h * 256 : (h + 1) * 256] = total

    relay(3)
    product(0)
    collect(2)
    collect(3)
    complete(2)
    complete(3)
    product(1)
    across(0)
    across(1)
    along(0)
    along(1)
    finish(0)
    finish(1)

    for made in started:
        made.wait_send()


def weight_gradient(need_ids, doc_start, embeds, queries, key_heads, cotangent, y_weight):
    any_space = pl.BlockSpec(memory_space=pl.ANY)
    vmem = pl.BlockSpec(memory_space=pltpu.VMEM)
    semaphores = [pltpu.SemaphoreType.DMA((n,)) for n in SEMAPHORES.values()]
    return pl.pallas_call(
        kernel,
        out_shape=jax.ShapeDtypeStruct((16, 512), F32),
        in_specs=[pl.BlockSpec(memory_space=pltpu.SMEM), vmem] + [any_space] * 5,
        out_specs=vmem,
        scratch_shapes=[pltpu.VMEM(shape, kind) for shape, kind in BUFFERS.values()]
        + semaphores
        + semaphores,
        compiler_params=pltpu.CompilerParams(
            collective_id=0, has_side_effects=True, vmem_limit_bytes=58 << 20
        ),
    )(need_ids, doc_start, embeds, queries, key_heads, cotangent, y_weight)


def on_device(
    embeds,
    queries,
    key_heads,
    cotangent,
    doc_start,
    need_ids,
    y_weight,
    z_weight,
    x_weight,
    second_moment,
):
    gradient = weight_gradient(
        need_ids[0], doc_start, embeds[0], queries[0], key_heads[0], cotangent[0], y_weight
    )
    moment_next = MOMENT_DECAY * second_moment + (1.0 - MOMENT_DECAY) * gradient * gradient
    z_next = z_weight - LEARN_RATE * (
        gradient / (jnp.sqrt(moment_next) + ADAM_EPS) + WEIGHT_DECAY * y_weight.astype(jnp.float32)
    )
    x_next = (1.0 - AVERAGE_MIX) * x_weight + AVERAGE_MIX * z_next
    y_next = ((1.0 - INTERP_BETA) * z_next + INTERP_BETA * x_next).astype(jnp.bfloat16)
    return (z_next, x_next, moment_next, y_next)


def solution(mesh):
    finer = Mesh(mesh.devices.reshape(NY, NZ, 2, mesh.shape["fs"]), CP_FS)
    return jax.shard_map(
        on_device,
        mesh=finer,
        in_specs=(
            P("fs", CP, None),
            P("fs", CP, None),
            P("fs", CP, None),
            P("fs", CP, None),
            P("fs", CP),
            P("fs", CP, None),
            P(CP_FS, None),
            P(CP_FS, None),
            P(CP_FS, None),
            P(CP_FS, None),
        ),
        out_specs=(P(CP_FS, None), P(CP_FS, None), P(CP_FS, None), P(CP_FS, None)),
        check_vma=False,
    )
```

```python
import math
from types import SimpleNamespace

import jax
import jax.numpy as jnp
from jax import lax
from jax.experimental import pallas as pl
from jax.experimental.pallas import tpu as pltpu
from jax.sharding import Mesh
from jax.sharding import PartitionSpec as P

HEAD = 128
KV = 4
WIN = 4
GROUP = 4
TOK = 256
SPAN = (WIN + 1) * TOK
NY, NZ, NX = 4, 8, 4
CP = ("cp_0", "cp_1", "cp_2")
CP_FS = ("cp_0", "cp_1", "cp_2", "fs")

NORM_EPS = 0.01
MOMENT_DECAY = 0.95
LEARN_RATE = 0.005
WEIGHT_DECAY = 0.1
ADAM_EPS = 1e-08
AVERAGE_MIX = 0.25
INTERP_BETA = 0.9
EXP2_SCALE = math.log2(math.e) / math.sqrt(HEAD)
MASKED = -1e30
FAR = 1 << 30

BF = jnp.bfloat16
F32 = jnp.float32
MESH = pl.DeviceIdType.MESH

BUFFERS = {
    "emb": ((TOK, 4096), BF),
    "w": ((2, NY, NZ, 2, NX, 16, 256), BF),
    "q": ((TOK, 2048), BF),
    "kw": ((5, TOK, 512), BF),
    "vw": ((KV, 5, TOK, HEAD), BF),
    "cot": ((TOK, 2048), BF),
    "p": ((16, TOK, SPAN), BF),
    "s": ((TOK, SPAN), F32),
    "bias": ((TOK, SPAN), F32),
    "att": ((16, TOK, HEAD), F32),
    "sq": ((TOK, HEAD), F32),
    "cr": ((TOK, HEAD), F32),
    "og": ((16, TOK, HEAD), BF),
    "dv": ((KV, 5, TOK, HEAD), F32),
    "r": ((KV, 3, TOK, HEAD), F32),
    "fo": ((KV, TOK, HEAD), BF),
    "fi": ((KV, TOK, HEAD), BF),
    "go": ((KV, TOK, HEAD), BF),
    "gi": ((KV, TOK, HEAD), BF),
    "vg": ((2, 8, TOK, 256), BF),
    "et": ((NY, NZ, 2, NX, 16, TOK), BF),
    "er": ((2, 2, 2, NZ, 16, TOK), BF),
    "ex": ((NY, NZ, 16, 8 * TOK), BF),
    "g": ((2, NY, NZ, 16, 256), F32),
    "g1": ((2, NZ, 16, 256), BF),
    "x1": ((2, 2, 4, 16, 256), BF),
    "tx": ((2, 2, NZ, 16, 256), BF),
    "x2": ((2, 2, NZ, 16, 256), BF),
    "t": ((2, NZ, 16, 256), F32),
    "tz": ((2, NZ, 16, 256), BF),
    "sum": ((2, 16, 256), F32),
    "rz": ((2, NZ, 16, 256), BF),
}
SEMAPHORES = {
    "ld": 8,
    "w1": 1,
    "w2": 1,
    "w3": 8,
    "wd": 1,
    "k": 5,
    "v": 12,
    "e": 2,
    "r": 8,
    "f": 4,
    "g": 4,
    "vg": 12,
    "vd": 4,
    "x": 6,
    "z": 2,
}
SENDERS = tuple(SEMAPHORES) + ("es",)


def kernel(need, doc, emb_h, q_h, k_h, cot_h, yw_h, out, *scratch):
    names = list(BUFFERS)
    b = SimpleNamespace(**dict(zip(names, scratch)))
    rest = scratch[len(names) :]
    rcv, snd = dict(zip(SEMAPHORES, rest)), rest[-1]

    y, z = lax.axis_index("cp_0"), lax.axis_index("cp_1")
    c, x = lax.axis_index("cp_2"), lax.axis_index("fs")
    o = 1 - c
    zn, yn = lax.rem(z + 1, NZ), lax.rem(y + lax.div(z + 1, NZ), NY)
    zp, yp = lax.rem(z + NZ - 1, NZ), lax.rem(y + NY - 1 + lax.div(z + NZ - 1, NZ), NY)
    yup, ydn = lax.rem(y + 1, NY), lax.rem(y + NY - 1, NY)
    xup, xdn = lax.rem(x + 1, NX), lax.rem(x + NX - 1, NX)
    yop, xop = lax.rem(y + 2, NY), lax.rem(x + 2, NX)
    block = (y * NZ + z) * 2 + c

    def dev(cp_0=y, cp_1=z, cp_2=c, fs=x):
        return {"cp_0": cp_0, "cp_1": cp_1, "cp_2": cp_2, "fs": fs}

    sibling = dev(cp_2=o)
    following, preceding = dev(cp_0=yn, cp_1=zn), dev(cp_0=yp, cp_1=zp)

    sent = dict.fromkeys(SENDERS, 0)
    results = []

    def copy(src, dst, kind, k, to, sender=None):
        return pltpu.make_async_remote_copy(
            src_ref=src,
            dst_ref=dst,
            send_sem=snd.at[SENDERS.index(sender or kind)],
            recv_sem=rcv[kind].at[k],
            device_id=to,
            device_id_type=MESH,
        )

    def prepare(src, dst, kind, k, to, sender=None):
        sent[sender or kind] += math.prod(src.shape) * jnp.dtype(src.dtype).itemsize
        return copy(src, dst, kind, k, to, sender)

    def send(*what):
        prepare(*what).start()

    def arrived(dst, kind, k):
        copy(dst, dst, kind, k, sibling).wait_recv()

    def room(size):
        n = size // (1 << 16)
        if size % (1 << 16):
            return b.w.at[0, 0, 0 : size // (1 << 14), :, 0]
        if n <= 8:
            return b.ex.at[0, 0:n]
        rows = next(a for a in (2, 3, 4) if n % a == 0 and n // a <= 8)
        return b.ex.at[0:rows, 0 : n // rows]

    loads = {}

    def load(name, src, dst):
        loads[name] = pltpu.make_async_copy(src, dst, rcv["ld"].at[len(loads)])
        loads[name].start()

    mine = b.w.at[:, y, z, c, x]
    load("w0", yw_h.at[:, 0:256], b.w.at[0, y, z, c, x])
    load("w1", yw_h.at[:, 256:512], b.w.at[1, y, z, c, x])
    load("k", k_h, b.kw.at[0])
    load("q", q_h, b.q)
    load("emb", emb_h, b.emb)
    load("cot", cot_h, b.cot)

    barrier = pltpu.get_barrier_semaphore()
    partners = [sibling, following, preceding]
    for d in range(1, NZ):
        partners.append(dev(cp_1=lax.rem(z + d, NZ)))
    for d in range(1, NY):
        partners.append(dev(cp_0=lax.rem(y + d, NY)))
    for d in range(1, NX):
        for cc in (c, o):
            partners.append(dev(fs=lax.rem(x + d, NX), cp_2=cc))
    for who in partners:
        pl.semaphore_signal(barrier, inc=1, device_id=who, device_id_type=MESH)
    pl.semaphore_wait(barrier, len(partners))

    loads["w0"].wait()
    loads["w1"].wait()
    for d in range(1, NZ):
        send(mine, mine, "w1", 0, dev(cp_1=lax.rem(z + d, NZ)))

    doc_t = jnp.transpose(jnp.broadcast_to(doc[...], (TOK, TOK)))
    row = lax.broadcasted_iota(jnp.int32, (TOK, TOK), 0) + block * TOK
    col = lax.broadcasted_iota(jnp.int32, (TOK, TOK), 1)
    for d in range(WIN + 1):
        listed = need[0, 0] == block - d
        for k in range(1, WIN + 1):
            listed = jnp.logical_or(listed, need[0, k] == block - d)
        shut = jnp.where(listed, 0, FAR)
        key_pos = col + (block - d) * TOK
        seen = jnp.logical_and(key_pos >= doc_t + shut, key_pos <= row)
        b.bias[:, d * TOK : (d + 1) * TOK] = jnp.where(seen, 0.0, MASKED)
    for kv in range(KV):
        b.r[kv, 2] = jnp.zeros((TOK, HEAD), F32)
    b.sq[...] = jnp.zeros((TOK, HEAD), F32)
    b.cr[...] = jnp.zeros((TOK, HEAD), F32)

    def turn(e, carry):
        lanes = pl.ds(pl.multiple_of(e * 512, 512), 512)
        turned = jnp.transpose(b.emb[:, lanes]).reshape(4, 2, NX, 16, TOK)
        b.et[lax.div(e, 2), pl.ds(4 * lax.rem(e, 2), 4)] = turned
        return carry

    loads["emb"].wait()

    arrived(room(7 << 14), "w1", 0)
    first, second = b.w.at[0, y, :, c, x], b.w.at[1, y, :, c, x]
    for d in range(1, 4):
        send(first, first, "w2", 0, dev(cp_0=lax.rem(y + d, NY)))
        send(second, second, "w2", 0, dev(fs=lax.rem(x + d, NX)))

    lax.fori_loop(0, 8, turn, 0)

    arrived(room(6 << 16), "w2", 0)

    def half_a(xx):
        return b.w.at[0, :, :, c, xx]

    def half_b(yy):
        return b.w.at[1, yy, :, c, :]

    def relay_a(xx, s):
        return b.w.at[0, :, 4 * s : 4 * s + 4, c, xx]

    def relay_b(yy, s):
        return b.w.at[1, yy, 4 * s : 4 * s + 4, c, :]

    send(half_a(x), half_a(x), "w3", 0, dev(fs=xup))
    send(half_a(x), half_a(x), "w3", 1, dev(fs=xdn))
    send(half_b(y), half_b(y), "w3", 2, dev(cp_0=yup))
    send(half_b(y), half_b(y), "w3", 3, dev(cp_0=ydn))

    send(half_a(x), half_a(x), "wd", 0, sibling)
    send(half_b(y), half_b(y), "wd", 0, sibling)

    loads["k"].wait()

    def keys_at(d, s):
        return b.kw.at[d, 128 * s : 128 * s + 128]

    def pass_keys(s):
        arrived(keys_at(2, s), "k", s)
        send(keys_at(2, s), keys_at(4, s), "k", 2 + s, following)
        send(keys_at(2 * c, s), keys_at(1, s), "k", 4, sibling)

    keys_out = [prepare(keys_at(0, s), keys_at(2, s), "k", s, following) for s in range(2)]

    @pl.when(z != NZ - 1)
    def _():
        for made in keys_out:
            made.start()

    arrived(half_a(x), "w3", 0)
    send(relay_a(xdn, 0), relay_a(xdn, 0), "w3", 4, dev(fs=xup))
    arrived(half_a(x), "w3", 1)
    send(relay_a(xup, 1), relay_a(xup, 1), "w3", 5, dev(fs=xdn))
    arrived(half_b(y), "w3", 3)
    for s in range(2):
        send(relay_b(yup, s), relay_b(yup, s), "w3", 6 + s, dev(cp_0=ydn))

    @pl.when(z == NZ - 1)
    def _():
        for made in keys_out:
            made.start()

    send(half_a(xdn), half_a(xdn), "wd", 0, sibling)
    send(half_a(xup), half_a(xup), "wd", 0, sibling)
    arrived(half_b(y), "w3", 2)
    send(half_b(ydn), half_b(ydn), "wd", 0, sibling)
    send(half_b(yup), half_b(yup), "wd", 0, sibling)
    pass_keys(0)
    pass_keys(1)
    loads["q"].wait()
    for s in range(2):
        arrived(relay_a(x, s), "w3", 4 + s)
        send(relay_a(xop, s), relay_a(xop, s), "wd", 0, sibling)
    for s in range(2):
        arrived(relay_b(y, s), "w3", 6 + s)
        send(relay_b(yop, s), relay_b(yop, s), "wd", 0, sibling)
    def head_probs(hd, carry):
        lanes = pl.ds(pl.multiple_of(hd * HEAD, HEAD), HEAD)
        key_lanes = pl.ds(pl.multiple_of(lax.div(hd, GROUP) * HEAD, HEAD), HEAD)
        keys = b.kw[:, :, key_lanes].reshape(SPAN, HEAD)
        b.s[...] = lax.dot_general(
            b.q[:, lanes], keys, (((1,), (1,)), ((), ())), preferred_element_type=F32
        )
        for n in range(8):
            rows = slice(n * 32, n * 32 + 32)
            score = b.s[rows, :] + b.bias[rows, :]
            largest = jnp.max(score, axis=-1, keepdims=True)
            weight = jnp.exp2((score - largest) * EXP2_SCALE)
            total = jnp.sum(weight, axis=-1, keepdims=True)
            b.p[hd, rows, :] = (weight * (1.0 / total)).astype(BF)
        return carry

    arrived(room(32 << 16), "wd", 0)

    def tokens_of(slot, ys=slice(None)):
        return b.ex.at[ys, :, :, slot * TOK : slot * TOK + TOK]

    kept = pltpu.make_async_copy(b.et.at[:, :, c, x], tokens_of(0), rcv["ld"].at[7])
    kept.start()
    send(b.et.at[:, :, o, x], tokens_of(1), "e", 0, sibling, "es")
    for s, xt in enumerate((xup, xdn)):
        for k, cc in enumerate((c, o)):
            part = b.et.at[2 * s : 2 * s + 2, :, cc, xop]
            send(part, b.er.at[s, k], "e", 1, dev(fs=xt))
    for s, xt in enumerate((xup, xdn)):
        for k, cc in enumerate((c, o)):
            there = tokens_of(2 + 2 * s + k)
            send(b.et.at[:, :, cc, xt], there, "e", 0, dev(fs=xt, cp_2=cc))

    def pass_embeds():
        arrived(b.er, "e", 1)
        for s, xt in enumerate((xup, xdn)):
            for k, cc in enumerate((c, o)):
                there = tokens_of(6 + k, slice(2 * s, 2 * s + 2))
                send(b.er.at[s, k], there, "e", 0, dev(fs=xt, cp_2=cc))

    for h in range(2):
        made = jnp.dot(b.emb[...], b.w[h].reshape(4096, 256), preferred_element_type=F32)
        for k in range(2):
            kv = 2 * h + k
            b.vw[kv, 0] = made[:, k * HEAD : (k + 1) * HEAD].astype(BF)
            send(b.vw.at[kv, 0], b.vw.at[kv, 2], "v", kv, following)

    def pass_near(kv):
        arrived(b.vw.at[kv, 2], "v", kv)
        send(b.vw.at[kv, 2], b.vw.at[kv, 4], "v", 4 + kv, following)
        send(b.vw.at[kv, 2 * c], b.vw.at[kv, 1], "v", 8 + kv, sibling)

    def pass_far(kv):
        arrived(b.vw.at[kv, 4], "v", 4 + kv)
        send(b.vw.at[kv, 2 + 2 * c], b.vw.at[kv, 3], "v", 8 + kv, sibling)

    def attend(kv):
        arrived(b.vw.at[kv, 0:2], "v", 8 + kv)

        def one(k, carry):
            hd = kv * GROUP + k
            values = b.vw[kv].reshape(SPAN, HEAD)
            made = jnp.dot(b.p[hd], values, preferred_element_type=F32)
            b.att[hd] = made
            lanes = pl.ds(pl.multiple_of(hd * HEAD, HEAD), HEAD)
            b.sq[...] += made * made
            b.cr[...] += made * b.cot[:, lanes].astype(F32)
            return carry

        lax.fori_loop(0, GROUP, one, 0)

    for s in range(2):
        arrived(keys_at(4, s), "k", 2 + s)
        send(keys_at(2 + 2 * c, s), keys_at(3, s), "k", 4, sibling)

    arrived(room(8 << 16), "k", 4)
    loads["cot"].wait()
    lax.fori_loop(0, 8, head_probs, 0)
    pass_near(0)
    pass_near(1)
    lax.fori_loop(8, 11, head_probs, 0)
    pass_near(2)
    lax.fori_loop(11, 13, head_probs, 0)
    pass_near(3)
    pass_embeds()
    lax.fori_loop(13, 15, head_probs, 0)
    pass_far(0)
    lax.fori_loop(15, 16, head_probs, 0)
    pass_far(1)
    attend(0)
    pass_far(2)
    attend(1)
    pass_far(3)
    attend(2)
    attend(3)

    token_total = TOK * NY * NZ * 2 * NX

    def norm_rows(n, carry):
        rows = pl.ds(pl.multiple_of(n * 32, 32), 32)
        mean = jnp.sum(b.sq[rows, :], axis=-1, keepdims=True) / 2048.0 + NORM_EPS
        inv = 1.0 / jnp.sqrt(mean)
        inner = jnp.sum(b.cr[rows, :], axis=-1, keepdims=True) / (2048.0 * token_total) * inv
        factor = inner * inv
        for hd in range(16):
            up = b.cot[rows, hd * HEAD : (hd + 1) * HEAD].astype(F32) / token_total
            b.og[hd, rows, :] = ((up - b.att[hd, rows, :] * factor) * inv).astype(BF)
        return carry

    lax.fori_loop(0, 8, norm_rows, 0)

    def grads(kv, low, high):
        def one(d, carry):
            lanes = pl.ds(pl.multiple_of(d * TOK, TOK), TOK)
            part = b.p[kv * GROUP : kv * GROUP + GROUP, :, lanes].reshape(GROUP * TOK, TOK)
            up = b.og[kv * GROUP : kv * GROUP + GROUP].reshape(GROUP * TOK, HEAD)
            b.dv[kv, d] = lax.dot_general(
                part, up, (((0,), (0,)), ((), ())), preferred_element_type=F32
            )
            return carry

        lax.fori_loop(low, high, one, 0)

    def grads_far(kv):
        grads(kv, 3, 5)
        send(b.dv.at[kv, 3], b.r.at[kv, 1], "r", 2 * kv + 1, sibling)

    def grads_near(kv):
        grads(kv, 1, 3)
        send(b.dv.at[kv, 1], b.r.at[kv, 0], "r", 2 * kv, sibling)

    def leave_far(kv):
        arrived(b.r.at[kv, 1], "r", 2 * kv + 1)
        b.fo[kv] = (b.dv[kv, 4] + b.r[kv, 2 - c]).astype(BF)
        send(b.fo.at[kv], b.fi.at[kv], "f", kv, preceding)

    def leave_near(kv):
        arrived(b.r.at[kv, 0], "r", 2 * kv)
        arrived(b.fi.at[kv], "f", kv)
        b.go[kv] = (b.dv[kv, 2] + b.r[kv, 1 - c] + b.fi[kv].astype(F32)).astype(BF)
        send(b.go.at[kv], b.gi.at[kv], "g", kv, preceding)

    def vg_at(kv, slot, rows=slice(None)):
        lanes = slice((kv % 2) * HEAD, (kv % 2) * HEAD + HEAD)
        return b.vg.at[kv // 2, slot, rows, lanes]

    upper, lower = slice(0, 128), slice(128, 256)

    def settle(kv):
        arrived(b.gi.at[kv], "g", kv)
        total = b.dv[kv, 0] + b.r[kv, 2 * c] + b.gi[kv].astype(F32)
        b.vg[kv // 2, 0, :, (kv % 2) * HEAD : (kv % 2) * HEAD + HEAD] = total.astype(BF)
        send(vg_at(kv, 0), vg_at(kv, 2), "vg", 3 * kv, dev(fs=xup))
        send(vg_at(kv, 0), vg_at(kv, 4), "vg", 3 * kv + 1, dev(fs=xdn))
        send(vg_at(kv, 0), vg_at(kv, 1), "vd", kv // 2, sibling)

    def relay(kv):
        arrived(vg_at(kv, 2), "vg", 3 * kv)
        send(vg_at(kv, 2, upper), vg_at(kv, 6, upper), "vg", 3 * kv + 2, dev(fs=xup))
        send(vg_at(kv, 2), vg_at(kv, 3), "vd", kv // 2, sibling)
        arrived(vg_at(kv, 4), "vg", 3 * kv + 1)
        send(vg_at(kv, 4, lower), vg_at(kv, 6, lower), "vg", 3 * kv + 2, dev(fs=xdn))
        send(vg_at(kv, 4), vg_at(kv, 5), "vd", kv // 2, sibling)

    def collect(kv):
        arrived(vg_at(kv, 6), "vg", 3 * kv + 2)
        send(vg_at(kv, 6), vg_at(kv, 7), "vd", 2 + kv // 2, sibling)

    grads_far(0)
    grads_far(1)
    leave_far(0)
    grads_far(2)
    leave_far(1)
    grads_far(3)
    leave_far(2)
    grads_near(0)
    leave_far(3)
    grads_near(1)
    grads_near(2)
    leave_near(0)
    grads_near(3)
    leave_near(1)
    grads(0, 0, 1)
    grads(1, 0, 1)
    leave_near(2)
    grads(2, 0, 1)
    grads(3, 0, 1)
    leave_near(3)
    kept.wait()
    arrived(room(28 << 16), "e", 0)

    settle(0)
    settle(1)
    settle(2)
    relay(0)
    settle(3)
    relay(1)
    relay(2)

    def early(h):
        arrived(room(6 << 16), "vd", h)
        b.g[h] = jnp.dot(
            b.ex[:, :, :, 0 : 6 * TOK].reshape(512, 6 * TOK),
            b.vg[h, 0:6].reshape(6 * TOK, 256),
            preferred_element_type=F32,
        ).reshape(NY, NZ, 16, 256)

    def product(h):
        arrived(room(2 << 16), "vd", 2 + h)
        b.g[h] += jnp.dot(
            b.ex[:, :, :, 6 * TOK : 8 * TOK].reshape(512, 2 * TOK),
            b.vg[h, 6:8].reshape(2 * TOK, 256),
            preferred_element_type=F32,
        ).reshape(NY, NZ, 16, 256)
        b.g1[h] = b.g[h, yop].astype(BF)
        send(b.g1.at[h, 0:4], b.x1.at[h, 0], "x", 3 * h, dev(cp_0=yup))
        send(b.g1.at[h, 4:8], b.x1.at[h, 1], "x", 3 * h + 1, dev(cp_0=ydn))

    def across(h):
        arrived(b.x1.at[h, 0], "x", 3 * h)
        b.tx[h, 0, 0:4] = (b.g[h, yup, 0:4] + b.x1[h, 0].astype(F32)).astype(BF)
        b.tx[h, 0, 4:8] = b.g[h, yup, 4:8].astype(BF)
        send(b.tx.at[h, 0], b.x2.at[h, 0], "x", 3 * h + 2, dev(cp_0=yup))
        arrived(b.x1.at[h, 1], "x", 3 * h + 1)
        b.tx[h, 1, 0:4] = b.g[h, ydn, 0:4].astype(BF)
        b.tx[h, 1, 4:8] = (b.g[h, ydn, 4:8] + b.x1[h, 1].astype(F32)).astype(BF)
        send(b.tx.at[h, 1], b.x2.at[h, 1], "x", 3 * h + 2, dev(cp_0=ydn))

    def along(h):
        arrived(b.x2.at[h], "x", 3 * h + 2)
        b.t[h] = b.g[h, y] + b.x2[h, 0].astype(F32) + b.x2[h, 1].astype(F32)
        b.tz[h] = b.t[h].astype(BF)
        for d in (4, 3, 5, 2, 6, 1, 7):
            zt = lax.rem(z + d, NZ)
            send(b.tz.at[h, zt], b.rz.at[h, z], "z", h, dev(cp_1=zt))

    def finish(h):
        arrived(b.rz.at[h, 0:7], "z", h)
        total = b.t[h, z]
        for d in range(1, NZ):
            total = total + b.rz[h, lax.rem(z + d, NZ)].astype(F32)
        b.sum[h] = total
        made = pltpu.make_async_copy(
            b.sum.at[h], out.at[:, h * 256 : (h + 1) * 256], rcv["ld"].at[h]
        )
        made.start()
        results.append(made)

    early(0)
    collect(0)
    relay(3)
    collect(1)
    product(0)
    collect(2)
    early(1)
    collect(3)
    product(1)
    across(0)
    across(1)
    along(0)
    along(1)
    finish(0)
    finish(1)

    for made in results:
        made.wait()
    for kind, size in sent.items():
        if size:
            copy(room(size), room(size), "w1", 0, sibling, kind).wait_send()


def weight_gradient(need_ids, doc_start, embeds, queries, key_heads, cotangent, y_weight):
    any_space = pl.BlockSpec(memory_space=pl.ANY)
    vmem = pl.BlockSpec(memory_space=pltpu.VMEM)
    semaphores = [pltpu.SemaphoreType.DMA((n,)) for n in SEMAPHORES.values()]
    semaphores.append(pltpu.SemaphoreType.DMA((len(SENDERS),)))
    return pl.pallas_call(
        kernel,
        out_shape=jax.ShapeDtypeStruct((16, 512), F32),
        in_specs=[pl.BlockSpec(memory_space=pltpu.SMEM), vmem] + [any_space] * 5,
        out_specs=any_space,
        scratch_shapes=[pltpu.VMEM(shape, kind) for shape, kind in BUFFERS.values()]
        + semaphores,
        compiler_params=pltpu.CompilerParams(
            collective_id=0, has_side_effects=True, vmem_limit_bytes=58 << 20
        ),
    )(need_ids, doc_start, embeds, queries, key_heads, cotangent, y_weight)


def on_device(
    embeds,
    queries,
    key_heads,
    cotangent,
    doc_start,
    need_ids,
    y_weight,
    z_weight,
    x_weight,
    second_moment,
):
    gradient = weight_gradient(
        need_ids[0], doc_start, embeds[0], queries[0], key_heads[0], cotangent[0], y_weight
    )
    moment_next = MOMENT_DECAY * second_moment + (1.0 - MOMENT_DECAY) * gradient * gradient
    z_next = z_weight - LEARN_RATE * (
        gradient / (jnp.sqrt(moment_next) + ADAM_EPS) + WEIGHT_DECAY * y_weight.astype(jnp.float32)
    )
    x_next = (1.0 - AVERAGE_MIX) * x_weight + AVERAGE_MIX * z_next
    y_next = ((1.0 - INTERP_BETA) * z_next + INTERP_BETA * x_next).astype(jnp.bfloat16)
    return (z_next, x_next, moment_next, y_next)


def solution(mesh):
    finer = Mesh(mesh.devices.reshape(NY, NZ, 2, mesh.shape["fs"]), CP_FS)
    return jax.shard_map(
        on_device,
        mesh=finer,
        in_specs=(
            P("fs", CP, None),
            P("fs", CP, None),
            P("fs", CP, None),
            P("fs", CP, None),
            P("fs", CP),
            P("fs", CP, None),
            P(CP_FS, None),
            P(CP_FS, None),
            P(CP_FS, None),
            P(CP_FS, None),
        ),
        out_specs=(P(CP_FS, None), P(CP_FS, None), P(CP_FS, None), P(CP_FS, None)),
        check_vma=False,
    )
```

```python
import math
from types import SimpleNamespace

import jax
import jax.numpy as jnp
from jax import lax
from jax.experimental import pallas as pl
from jax.experimental.pallas import tpu as pltpu
from jax.sharding import Mesh
from jax.sharding import PartitionSpec as P

HEAD = 128
KV = 4
WIN = 4
GROUP = 4
TOK = 256
SPAN = (WIN + 1) * TOK
NY, NZ, NX = 4, 8, 4
CP = ("cp_0", "cp_1", "cp_2")
CP_FS = ("cp_0", "cp_1", "cp_2", "fs")

NORM_EPS = 0.01
MOMENT_DECAY = 0.95
LEARN_RATE = 0.005
WEIGHT_DECAY = 0.1
ADAM_EPS = 1e-08
AVERAGE_MIX = 0.25
INTERP_BETA = 0.9
EXP2_SCALE = math.log2(math.e) / math.sqrt(HEAD)
MASKED = -1e30
FAR = 1 << 30

BF = jnp.bfloat16
F32 = jnp.float32
MESH = pl.DeviceIdType.MESH

BUFFERS = {
    "emb": ((TOK, 4096), BF),
    "w": ((NY, NZ, 2, NX, 16, 512), BF),
    "q": ((TOK, 2048), BF),
    "kw": ((5, TOK, 512), BF),
    "vw": ((KV, 5, TOK, HEAD), BF),
    "cot": ((TOK, 2048), BF),
    "p": ((16, TOK, SPAN), BF),
    "s0": ((TOK, SPAN), F32),
    "s1": ((TOK, SPAN), F32),
    "bias": ((TOK, SPAN), F32),
    "att": ((16, TOK, HEAD), F32),
    "sq": ((TOK, HEAD), F32),
    "cr": ((TOK, HEAD), F32),
    "og": ((16, TOK, HEAD), BF),
    "dv": ((KV, 5, TOK, HEAD), F32),
    "r": ((KV, 3, TOK, HEAD), F32),
    "fo": ((KV, TOK, HEAD), BF),
    "fi": ((KV, TOK, HEAD), BF),
    "go": ((KV, TOK, HEAD), BF),
    "gi": ((KV, TOK, HEAD), BF),
    "vg": ((2, 8, TOK, 256), BF),
    "et": ((NY, NZ, 2, NX, 16, TOK), BF),
    "er": ((2, 2, 2, NZ, 16, TOK), BF),
    "ex": ((NY, NZ, 16, 8 * TOK), BF),
    "g": ((2, NY, NZ, 16, 256), F32),
    "g1": ((2, NZ, 16, 256), BF),
    "x1": ((2, 2, 4, 16, 256), BF),
    "tx": ((2, 2, NZ, 16, 256), BF),
    "x2": ((2, 2, NZ, 16, 256), BF),
    "t": ((2, NZ, 16, 256), F32),
    "tz": ((2, NZ, 16, 256), BF),
    "sum": ((2, 16, 256), F32),
    "rz": ((2, NZ, 16, 256), BF),
}
SEMAPHORES = {
    "ld": 8,
    "w1": 1,
    "w2": 1,
    "w3": 8,
    "wd": 1,
    "k": 5,
    "v": 12,
    "e": 2,
    "r": 8,
    "f": 4,
    "g": 4,
    "vg": 12,
    "vd": 4,
    "x": 6,
    "z": 2,
}
SENDERS = tuple(SEMAPHORES) + ("es",)


def kernel(need, doc, emb_h, q_h, k_h, cot_h, yw_h, out, *scratch):
    names = list(BUFFERS)
    b = SimpleNamespace(**dict(zip(names, scratch)))
    rest = scratch[len(names) :]
    rcv, snd = dict(zip(SEMAPHORES, rest)), rest[-1]

    y, z = lax.axis_index("cp_0"), lax.axis_index("cp_1")
    c, x = lax.axis_index("cp_2"), lax.axis_index("fs")
    o = 1 - c
    zn, yn = lax.rem(z + 1, NZ), lax.rem(y + lax.div(z + 1, NZ), NY)
    zp, yp = lax.rem(z + NZ - 1, NZ), lax.rem(y + NY - 1 + lax.div(z + NZ - 1, NZ), NY)
    yup, ydn = lax.rem(y + 1, NY), lax.rem(y + NY - 1, NY)
    xup, xdn = lax.rem(x + 1, NX), lax.rem(x + NX - 1, NX)
    yop, xop = lax.rem(y + 2, NY), lax.rem(x + 2, NX)
    block = (y * NZ + z) * 2 + c

    def dev(cp_0=y, cp_1=z, cp_2=c, fs=x):
        return {"cp_0": cp_0, "cp_1": cp_1, "cp_2": cp_2, "fs": fs}

    sibling = dev(cp_2=o)
    following, preceding = dev(cp_0=yn, cp_1=zn), dev(cp_0=yp, cp_1=zp)

    sent = dict.fromkeys(SENDERS, 0)
    results = []

    def copy(src, dst, kind, k, to, sender=None):
        return pltpu.make_async_remote_copy(
            src_ref=src,
            dst_ref=dst,
            send_sem=snd.at[SENDERS.index(sender or kind)],
            recv_sem=rcv[kind].at[k],
            device_id=to,
            device_id_type=MESH,
        )

    def prepare(src, dst, kind, k, to, sender=None):
        sent[sender or kind] += math.prod(src.shape) * jnp.dtype(src.dtype).itemsize
        return copy(src, dst, kind, k, to, sender)

    def send(*what):
        prepare(*what).start()

    def arrived(dst, kind, k):
        copy(dst, dst, kind, k, sibling).wait_recv()

    def room(size):
        n = size // (1 << 16)
        if size % (1 << 16):
            return b.w.at[0, 0 : size // (1 << 14), 0, 0]
        if n <= 8:
            return b.ex.at[0, 0:n]
        rows = next(a for a in (2, 3, 4) if n % a == 0 and n // a <= 8)
        return b.ex.at[0:rows, 0 : n // rows]

    loads = {}

    def load(name, src, dst):
        loads[name] = pltpu.make_async_copy(src, dst, rcv["ld"].at[len(loads)])
        loads[name].start()

    mine = b.w.at[y, z, c, x]
    load("w", yw_h, mine)
    load("k", k_h, b.kw.at[0])
    load("q", q_h, b.q)
    load("emb", emb_h, b.emb)
    load("cot", cot_h, b.cot)

    barrier = pltpu.get_barrier_semaphore()
    partners = [sibling, following, preceding]
    for d in range(1, NZ):
        partners.append(dev(cp_1=lax.rem(z + d, NZ)))
    for d in range(1, NY):
        partners.append(dev(cp_0=lax.rem(y + d, NY)))
    for d in range(1, NX):
        for cc in (c, o):
            partners.append(dev(fs=lax.rem(x + d, NX), cp_2=cc))
    for who in partners:
        pl.semaphore_signal(barrier, inc=1, device_id=who, device_id_type=MESH)
    pl.semaphore_wait(barrier, len(partners))

    loads["w"].wait()
    for d in range(1, NZ):
        send(mine, mine, "w1", 0, dev(cp_1=lax.rem(z + d, NZ)))

    doc_t = jnp.transpose(jnp.broadcast_to(doc[...], (TOK, TOK)))
    row = lax.broadcasted_iota(jnp.int32, (TOK, TOK), 0) + block * TOK
    col = lax.broadcasted_iota(jnp.int32, (TOK, TOK), 1)
    for d in range(WIN + 1):
        listed = need[0, 0] == block - d
        for k in range(1, WIN + 1):
            listed = jnp.logical_or(listed, need[0, k] == block - d)
        shut = jnp.where(listed, 0, FAR)
        key_pos = col + (block - d) * TOK
        seen = jnp.logical_and(key_pos >= doc_t + shut, key_pos <= row)
        b.bias[:, d * TOK : (d + 1) * TOK] = jnp.where(seen, 0.0, MASKED)
    for kv in range(KV):
        b.r[kv, 2] = jnp.zeros((TOK, HEAD), F32)
    b.sq[...] = jnp.zeros((TOK, HEAD), F32)
    b.cr[...] = jnp.zeros((TOK, HEAD), F32)

    def turn(e, carry):
        lanes = pl.ds(pl.multiple_of(e * 512, 512), 512)
        turned = jnp.transpose(b.emb[:, lanes]).reshape(4, 2, NX, 16, TOK)
        b.et[lax.div(e, 2), pl.ds(4 * lax.rem(e, 2), 4)] = turned
        return carry

    loads["emb"].wait()

    arrived(room(7 << 14), "w1", 0)
    first, second = b.w.at[y, :, c, x, :, 0:256], b.w.at[y, :, c, x, :, 256:512]
    for d in range(1, 4):
        send(first, first, "w2", 0, dev(cp_0=lax.rem(y + d, NY)))
        send(second, second, "w2", 0, dev(fs=lax.rem(x + d, NX)))

    lax.fori_loop(0, 8, turn, 0)

    arrived(room(6 << 16), "w2", 0)

    def half_a(xx):
        return b.w.at[:, :, c, xx, :, 0:256]

    def half_b(yy):
        return b.w.at[yy, :, c, :, :, 256:512]

    def relay_a(xx, s):
        return b.w.at[:, 4 * s : 4 * s + 4, c, xx, :, 0:256]

    def relay_b(yy, s):
        return b.w.at[yy, 4 * s : 4 * s + 4, c, :, :, 256:512]

    send(half_a(x), half_a(x), "w3", 0, dev(fs=xup))
    send(half_a(x), half_a(x), "w3", 1, dev(fs=xdn))
    send(half_b(y), half_b(y), "w3", 2, dev(cp_0=yup))
    send(half_b(y), half_b(y), "w3", 3, dev(cp_0=ydn))

    send(half_a(x), half_a(x), "wd", 0, sibling)
    send(half_b(y), half_b(y), "wd", 0, sibling)

    loads["k"].wait()

    def keys_at(d, s):
        return b.kw.at[d, 128 * s : 128 * s + 128]

    def pass_keys(s):
        arrived(keys_at(2, s), "k", s)
        send(keys_at(2, s), keys_at(4, s), "k", 2 + s, following)
        send(keys_at(2 * c, s), keys_at(1, s), "k", 4, sibling)

    keys_out = [prepare(keys_at(0, s), keys_at(2, s), "k", s, following) for s in range(2)]

    @pl.when(z != NZ - 1)
    def _():
        for made in keys_out:
            made.start()

    arrived(half_a(x), "w3", 0)
    send(relay_a(xdn, 0), relay_a(xdn, 0), "w3", 4, dev(fs=xup))
    arrived(half_a(x), "w3", 1)
    send(relay_a(xup, 1), relay_a(xup, 1), "w3", 5, dev(fs=xdn))
    arrived(half_b(y), "w3", 3)
    for s in range(2):
        send(relay_b(yup, s), relay_b(yup, s), "w3", 6 + s, dev(cp_0=ydn))

    @pl.when(z == NZ - 1)
    def _():
        for made in keys_out:
            made.start()

    send(half_a(xdn), half_a(xdn), "wd", 0, sibling)
    send(half_a(xup), half_a(xup), "wd", 0, sibling)
    arrived(half_b(y), "w3", 2)
    send(half_b(ydn), half_b(ydn), "wd", 0, sibling)
    send(half_b(yup), half_b(yup), "wd", 0, sibling)
    pass_keys(0)
    pass_keys(1)
    loads["q"].wait()
    for s in range(2):
        arrived(relay_a(x, s), "w3", 4 + s)
        send(relay_a(xop, s), relay_a(xop, s), "wd", 0, sibling)
    for s in range(2):
        arrived(relay_b(y, s), "w3", 6 + s)
        send(relay_b(yop, s), relay_b(yop, s), "wd", 0, sibling)
    def scores(hd, into):
        lanes = pl.ds(pl.multiple_of(hd * HEAD, HEAD), HEAD)
        key_lanes = pl.ds(pl.multiple_of(lax.div(hd, GROUP) * HEAD, HEAD), HEAD)
        keys = b.kw[:, :, key_lanes].reshape(SPAN, HEAD)
        into[...] = lax.dot_general(
            b.q[:, lanes], keys, (((1,), (1,)), ((), ())), preferred_element_type=F32
        )

    def softmax(hd, held):
        for n in range(8):
            rows = slice(n * 32, n * 32 + 32)
            score = held[rows, :] + b.bias[rows, :]
            largest = jnp.max(score, axis=-1, keepdims=True)
            weight = jnp.exp2((score - largest) * EXP2_SCALE)
            total = jnp.sum(weight, axis=-1, keepdims=True)
            b.p[hd, rows, :] = (weight * (1.0 / total)).astype(BF)

    def head_probs(pair, carry):
        scores(2 * pair + 1, b.s1)
        softmax(2 * pair, b.s0)
        scores(jnp.minimum(2 * pair + 2, 15), b.s0)
        softmax(2 * pair + 1, b.s1)
        return carry

    arrived(room(32 << 16), "wd", 0)

    def tokens_of(slot, ys=slice(None)):
        return b.ex.at[ys, :, :, slot * TOK : slot * TOK + TOK]

    kept = pltpu.make_async_copy(b.et.at[:, :, c, x], tokens_of(0), rcv["ld"].at[7])
    kept.start()
    send(b.et.at[:, :, o, x], tokens_of(1), "e", 0, sibling, "es")
    for s, xt in enumerate((xup, xdn)):
        for k, cc in enumerate((c, o)):
            part = b.et.at[2 * s : 2 * s + 2, :, cc, xop]
            send(part, b.er.at[s, k], "e", 1, dev(fs=xt))
    for s, xt in enumerate((xup, xdn)):
        for k, cc in enumerate((c, o)):
            there = tokens_of(2 + 2 * s + k)
            send(b.et.at[:, :, cc, xt], there, "e", 0, dev(fs=xt, cp_2=cc))

    def pass_embeds():
        arrived(b.er, "e", 1)
        for s, xt in enumerate((xup, xdn)):
            for k, cc in enumerate((c, o)):
                there = tokens_of(6 + k, slice(2 * s, 2 * s + 2))
                send(b.er.at[s, k], there, "e", 0, dev(fs=xt, cp_2=cc))

    made = jnp.dot(b.emb[...], b.w[...].reshape(4096, 512), preferred_element_type=F32)
    for kv in range(KV):
        b.vw[kv, 0] = made[:, kv * HEAD : (kv + 1) * HEAD].astype(BF)
        send(b.vw.at[kv, 0], b.vw.at[kv, 2], "v", kv, following)

    def pass_near(kv):
        arrived(b.vw.at[kv, 2], "v", kv)
        send(b.vw.at[kv, 2], b.vw.at[kv, 4], "v", 4 + kv, following)
        send(b.vw.at[kv, 2 * c], b.vw.at[kv, 1], "v", 8 + kv, sibling)

    def pass_far(kv):
        arrived(b.vw.at[kv, 4], "v", 4 + kv)
        send(b.vw.at[kv, 2 + 2 * c], b.vw.at[kv, 3], "v", 8 + kv, sibling)

    def attend(kv):
        arrived(b.vw.at[kv, 0:2], "v", 8 + kv)

        for hd in range(kv * GROUP, kv * GROUP + GROUP):
            values = b.vw[kv].reshape(SPAN, HEAD)
            b.att[hd] = jnp.dot(b.p[hd], values, preferred_element_type=F32)
        for hd in range(kv * GROUP, kv * GROUP + GROUP):
            lanes = slice(hd * HEAD, hd * HEAD + HEAD)
            b.sq[...] += b.att[hd] * b.att[hd]
            b.cr[...] += b.att[hd] * b.cot[:, lanes].astype(F32)

    for s in range(2):
        arrived(keys_at(4, s), "k", 2 + s)
        send(keys_at(2 + 2 * c, s), keys_at(3, s), "k", 4, sibling)

    arrived(room(8 << 16), "k", 4)
    loads["cot"].wait()
    scores(0, b.s0)
    lax.fori_loop(0, 4, head_probs, 0)
    pass_near(0)
    pass_near(1)
    lax.fori_loop(4, 5, head_probs, 0)
    pass_near(2)
    lax.fori_loop(5, 6, head_probs, 0)
    pass_near(3)
    pass_embeds()
    lax.fori_loop(6, 7, head_probs, 0)
    pass_far(0)
    lax.fori_loop(7, 8, head_probs, 0)
    pass_far(1)
    attend(0)
    pass_far(2)
    attend(1)
    pass_far(3)
    attend(2)
    attend(3)

    token_total = TOK * NY * NZ * 2 * NX

    def norm_rows(n, carry):
        rows = pl.ds(pl.multiple_of(n * 32, 32), 32)
        mean = jnp.sum(b.sq[rows, :], axis=-1, keepdims=True) / 2048.0 + NORM_EPS
        inv = 1.0 / jnp.sqrt(mean)
        inner = jnp.sum(b.cr[rows, :], axis=-1, keepdims=True) / (2048.0 * token_total) * inv
        factor = inner * inv
        for hd in range(16):
            up = b.cot[rows, hd * HEAD : (hd + 1) * HEAD].astype(F32) / token_total
            b.og[hd, rows, :] = ((up - b.att[hd, rows, :] * factor) * inv).astype(BF)
        return carry

    lax.fori_loop(0, 8, norm_rows, 0)

    def grads(kv, low, high):
        up = b.og[kv * GROUP : kv * GROUP + GROUP].reshape(GROUP * TOK, HEAD)
        for d in range(low, high):
            lanes = slice(d * TOK, d * TOK + TOK)
            part = b.p[kv * GROUP : kv * GROUP + GROUP, :, lanes].reshape(GROUP * TOK, TOK)
            b.dv[kv, d] = lax.dot_general(
                part, up, (((0,), (0,)), ((), ())), preferred_element_type=F32
            )

    def grads_far(kv):
        grads(kv, 3, 5)
        send(b.dv.at[kv, 3], b.r.at[kv, 1], "r", 2 * kv + 1, sibling)

    def grads_near(kv):
        grads(kv, 1, 3)
        send(b.dv.at[kv, 1], b.r.at[kv, 0], "r", 2 * kv, sibling)

    def leave_far(kv):
        arrived(b.r.at[kv, 1], "r", 2 * kv + 1)
        b.fo[kv] = (b.dv[kv, 4] + b.r[kv, 2 - c]).astype(BF)
        send(b.fo.at[kv], b.fi.at[kv], "f", kv, preceding)

    def leave_near(kv):
        arrived(b.r.at[kv, 0], "r", 2 * kv)
        arrived(b.fi.at[kv], "f", kv)
        b.go[kv] = (b.dv[kv, 2] + b.r[kv, 1 - c] + b.fi[kv].astype(F32)).astype(BF)
        send(b.go.at[kv], b.gi.at[kv], "g", kv, preceding)

    def vg_at(kv, slot, rows=slice(None)):
        lanes = slice((kv % 2) * HEAD, (kv % 2) * HEAD + HEAD)
        return b.vg.at[kv // 2, slot, rows, lanes]

    upper, lower = slice(0, 128), slice(128, 256)

    def settle(kv):
        arrived(b.gi.at[kv], "g", kv)
        total = b.dv[kv, 0] + b.r[kv, 2 * c] + b.gi[kv].astype(F32)
        b.vg[kv // 2, 0, :, (kv % 2) * HEAD : (kv % 2) * HEAD + HEAD] = total.astype(BF)
        send(vg_at(kv, 0), vg_at(kv, 2), "vg", 3 * kv, dev(fs=xup))
        send(vg_at(kv, 0), vg_at(kv, 4), "vg", 3 * kv + 1, dev(fs=xdn))
        send(vg_at(kv, 0), vg_at(kv, 1), "vd", kv // 2, sibling)

    def relay(kv):
        arrived(vg_at(kv, 2), "vg", 3 * kv)
        send(vg_at(kv, 2, upper), vg_at(kv, 6, upper), "vg", 3 * kv + 2, dev(fs=xup))
        send(vg_at(kv, 2), vg_at(kv, 3), "vd", kv // 2, sibling)
        arrived(vg_at(kv, 4), "vg", 3 * kv + 1)
        send(vg_at(kv, 4, lower), vg_at(kv, 6, lower), "vg", 3 * kv + 2, dev(fs=xdn))
        send(vg_at(kv, 4), vg_at(kv, 5), "vd", kv // 2, sibling)

    def collect(kv):
        arrived(vg_at(kv, 6), "vg", 3 * kv + 2)
        send(vg_at(kv, 6), vg_at(kv, 7), "vd", 2 + kv // 2, sibling)

    grads_far(0)
    grads_far(1)
    leave_far(0)
    grads_far(2)
    leave_far(1)
    grads_far(3)
    leave_far(2)
    grads_near(0)
    leave_far(3)
    grads_near(1)
    grads_near(2)
    leave_near(0)
    grads_near(3)
    leave_near(1)
    grads(0, 0, 1)
    grads(1, 0, 1)
    leave_near(2)
    grads(2, 0, 1)
    grads(3, 0, 1)
    leave_near(3)
    kept.wait()
    arrived(room(28 << 16), "e", 0)

    settle(0)
    settle(1)
    settle(2)
    relay(0)
    settle(3)
    relay(1)
    relay(2)

    def early(h):
        arrived(room(6 << 16), "vd", h)
        for ys in (slice(0, 2), slice(2, 4)):
            b.g[h, ys] = jnp.dot(
                b.ex[ys, :, :, 0 : 6 * TOK].reshape(256, 6 * TOK),
                b.vg[h, 0:6].reshape(6 * TOK, 256),
                preferred_element_type=F32,
            ).reshape(2, NZ, 16, 256)

    def product(h):
        arrived(room(2 << 16), "vd", 2 + h)
        for ys in (slice(0, 2), slice(2, 4)):
            b.g[h, ys] += jnp.dot(
                b.ex[ys, :, :, 6 * TOK : 8 * TOK].reshape(256, 2 * TOK),
                b.vg[h, 6:8].reshape(2 * TOK, 256),
                preferred_element_type=F32,
            ).reshape(2, NZ, 16, 256)
        b.g1[h] = b.g[h, yop].astype(BF)
        send(b.g1.at[h, 0:4], b.x1.at[h, 0], "x", 3 * h, dev(cp_0=yup))
        send(b.g1.at[h, 4:8], b.x1.at[h, 1], "x", 3 * h + 1, dev(cp_0=ydn))

    def across(h):
        arrived(b.x1.at[h, 0], "x", 3 * h)
        b.tx[h, 0, 0:4] = (b.g[h, yup, 0:4] + b.x1[h, 0].astype(F32)).astype(BF)
        b.tx[h, 0, 4:8] = b.g[h, yup, 4:8].astype(BF)
        send(b.tx.at[h, 0], b.x2.at[h, 0], "x", 3 * h + 2, dev(cp_0=yup))
        arrived(b.x1.at[h, 1], "x", 3 * h + 1)
        b.tx[h, 1, 0:4] = b.g[h, ydn, 0:4].astype(BF)
        b.tx[h, 1, 4:8] = (b.g[h, ydn, 4:8] + b.x1[h, 1].astype(F32)).astype(BF)
        send(b.tx.at[h, 1], b.x2.at[h, 1], "x", 3 * h + 2, dev(cp_0=ydn))

    def along(h):
        arrived(b.x2.at[h], "x", 3 * h + 2)
        b.t[h] = b.g[h, y] + b.x2[h, 0].astype(F32) + b.x2[h, 1].astype(F32)
        b.tz[h] = b.t[h].astype(BF)
        for d in (4, 3, 5, 2, 6, 1, 7):
            zt = lax.rem(z + d, NZ)
            send(b.tz.at[h, zt], b.rz.at[h, z], "z", h, dev(cp_1=zt))

    def finish(h):
        arrived(b.rz.at[h, 0:7], "z", h)
        total = b.t[h, z]
        for d in range(1, NZ):
            total = total + b.rz[h, lax.rem(z + d, NZ)].astype(F32)
        b.sum[h] = total
        made = pltpu.make_async_copy(
            b.sum.at[h], out.at[:, h * 256 : (h + 1) * 256], rcv["ld"].at[h]
        )
        made.start()
        results.append(made)

    early(0)
    collect(0)
    relay(3)
    collect(1)
    product(0)
    collect(2)
    early(1)
    collect(3)
    product(1)
    across(0)
    across(1)
    along(0)
    along(1)
    finish(0)
    finish(1)

    for made in results:
        made.wait()
    for kind, size in sent.items():
        if size:
            copy(room(size), room(size), "w1", 0, sibling, kind).wait_send()


def weight_gradient(need_ids, doc_start, embeds, queries, key_heads, cotangent, y_weight):
    any_space = pl.BlockSpec(memory_space=pl.ANY)
    vmem = pl.BlockSpec(memory_space=pltpu.VMEM)
    semaphores = [pltpu.SemaphoreType.DMA((n,)) for n in SEMAPHORES.values()]
    semaphores.append(pltpu.SemaphoreType.DMA((len(SENDERS),)))
    return pl.pallas_call(
        kernel,
        out_shape=jax.ShapeDtypeStruct((16, 512), F32),
        in_specs=[pl.BlockSpec(memory_space=pltpu.SMEM), vmem] + [any_space] * 5,
        out_specs=any_space,
        scratch_shapes=[pltpu.VMEM(shape, kind) for shape, kind in BUFFERS.values()]
        + semaphores,
        compiler_params=pltpu.CompilerParams(
            collective_id=0, has_side_effects=True, vmem_limit_bytes=58 << 20
        ),
    )(need_ids, doc_start, embeds, queries, key_heads, cotangent, y_weight)


def on_device(
    embeds,
    queries,
    key_heads,
    cotangent,
    doc_start,
    need_ids,
    y_weight,
    z_weight,
    x_weight,
    second_moment,
):
    gradient = weight_gradient(
        need_ids[0], doc_start, embeds[0], queries[0], key_heads[0], cotangent[0], y_weight
    )
    moment_next = MOMENT_DECAY * second_moment + (1.0 - MOMENT_DECAY) * gradient * gradient
    z_next = z_weight - LEARN_RATE * (
        gradient / (jnp.sqrt(moment_next) + ADAM_EPS) + WEIGHT_DECAY * y_weight.astype(jnp.float32)
    )
    x_next = (1.0 - AVERAGE_MIX) * x_weight + AVERAGE_MIX * z_next
    y_next = ((1.0 - INTERP_BETA) * z_next + INTERP_BETA * x_next).astype(jnp.bfloat16)
    return (z_next, x_next, moment_next, y_next)


def solution(mesh):
    finer = Mesh(mesh.devices.reshape(NY, NZ, 2, mesh.shape["fs"]), CP_FS)
    return jax.shard_map(
        on_device,
        mesh=finer,
        in_specs=(
            P("fs", CP, None),
            P("fs", CP, None),
            P("fs", CP, None),
            P("fs", CP, None),
            P("fs", CP),
            P("fs", CP, None),
            P(CP_FS, None),
            P(CP_FS, None),
            P(CP_FS, None),
            P(CP_FS, None),
        ),
        out_specs=(P(CP_FS, None), P(CP_FS, None), P(CP_FS, None), P(CP_FS, None)),
        check_vma=False,
    )
```

```python
import math
from types import SimpleNamespace

import jax
import jax.numpy as jnp
from jax import lax
from jax.experimental import pallas as pl
from jax.experimental.pallas import tpu as pltpu
from jax.sharding import Mesh
from jax.sharding import PartitionSpec as P

HEAD = 128
KV = 4
WIN = 4
GROUP = 4
TOK = 256
SPAN = (WIN + 1) * TOK
NY, NZ, NX = 4, 8, 4
CP = ("cp_0", "cp_1", "cp_2")
CP_FS = ("cp_0", "cp_1", "cp_2", "fs")

NORM_EPS = 0.01
MOMENT_DECAY = 0.95
LEARN_RATE = 0.005
WEIGHT_DECAY = 0.1
ADAM_EPS = 1e-08
AVERAGE_MIX = 0.25
INTERP_BETA = 0.9
EXP2_SCALE = math.log2(math.e) / math.sqrt(HEAD)
MASKED = -1e30
FAR = 1 << 30

BF = jnp.bfloat16
F32 = jnp.float32
MESH = pl.DeviceIdType.MESH

BUFFERS = {
    "emb": ((TOK, 4096), BF),
    "w": ((NY, NZ, 2, NX, 16, 512), BF),
    "q": ((TOK, 2048), BF),
    "kw": ((5, TOK, 512), BF),
    "vw": ((KV, 5, TOK, HEAD), BF),
    "cot": ((TOK, 2048), BF),
    "p": ((16, TOK, SPAN), BF),
    "s0": ((TOK, SPAN), F32),
    "s1": ((TOK, SPAN), F32),
    "bias": ((TOK, SPAN), F32),
    "att": ((16, TOK, HEAD), F32),
    "sq": ((TOK, HEAD), F32),
    "cr": ((TOK, HEAD), F32),
    "og": ((16, TOK, HEAD), BF),
    "dv": ((KV, 5, TOK, HEAD), F32),
    "r": ((KV, 3, TOK, HEAD), F32),
    "fo": ((KV, TOK, HEAD), BF),
    "fi": ((KV, TOK, HEAD), BF),
    "go": ((KV, TOK, HEAD), BF),
    "gi": ((KV, TOK, HEAD), BF),
    "vg": ((2, 8, TOK, 256), BF),
    "et": ((NY, NZ, 2, NX, 16, TOK), BF),
    "er": ((2, 2, 2, NZ, 16, TOK), BF),
    "ex": ((NY, NZ, 16, 8 * TOK), BF),
    "g": ((2, NY, NZ, 16, 256), F32),
    "g1": ((2, NZ, 16, 256), BF),
    "x1": ((2, 2, 4, 16, 256), BF),
    "tx": ((2, 2, NZ, 16, 256), BF),
    "x2": ((2, 2, NZ, 16, 256), BF),
    "t": ((2, NZ, 16, 256), F32),
    "tz": ((2, NZ, 16, 256), BF),
    "sum": ((2, 16, 256), F32),
    "rz": ((2, NZ, 16, 256), BF),
}
SEMAPHORES = {
    "ld": 8,
    "w1": 1,
    "w2": 1,
    "w3": 8,
    "wd": 1,
    "k": 5,
    "v": 12,
    "e": 2,
    "r": 8,
    "f": 4,
    "g": 4,
    "vg": 12,
    "vd": 4,
    "x": 6,
    "z": 2,
}
SENDERS = tuple(SEMAPHORES) + ("es",)


def kernel(need, doc, emb_h, q_h, k_h, cot_h, yw_h, out, *scratch):
    names = list(BUFFERS)
    b = SimpleNamespace(**dict(zip(names, scratch)))
    rest = scratch[len(names) :]
    rcv, snd = dict(zip(SEMAPHORES, rest)), rest[-1]

    y, z = lax.axis_index("cp_0"), lax.axis_index("cp_1")
    c, x = lax.axis_index("cp_2"), lax.axis_index("fs")
    o = 1 - c
    zn, yn = lax.rem(z + 1, NZ), lax.rem(y + lax.div(z + 1, NZ), NY)
    zp, yp = lax.rem(z + NZ - 1, NZ), lax.rem(y + NY - 1 + lax.div(z + NZ - 1, NZ), NY)
    yup, ydn = lax.rem(y + 1, NY), lax.rem(y + NY - 1, NY)
    xup, xdn = lax.rem(x + 1, NX), lax.rem(x + NX - 1, NX)
    yop, xop = lax.rem(y + 2, NY), lax.rem(x + 2, NX)
    block = (y * NZ + z) * 2 + c

    def dev(cp_0=y, cp_1=z, cp_2=c, fs=x):
        return {"cp_0": cp_0, "cp_1": cp_1, "cp_2": cp_2, "fs": fs}

    sibling = dev(cp_2=o)
    following, preceding = dev(cp_0=yn, cp_1=zn), dev(cp_0=yp, cp_1=zp)

    sent = dict.fromkeys(SENDERS, 0)
    results = []

    def copy(src, dst, kind, k, to, sender=None):
        return pltpu.make_async_remote_copy(
            src_ref=src,
            dst_ref=dst,
            send_sem=snd.at[SENDERS.index(sender or kind)],
            recv_sem=rcv[kind].at[k],
            device_id=to,
            device_id_type=MESH,
        )

    def prepare(src, dst, kind, k, to, sender=None):
        sent[sender or kind] += math.prod(src.shape) * jnp.dtype(src.dtype).itemsize
        return copy(src, dst, kind, k, to, sender)

    def send(*what):
        prepare(*what).start()

    def arrived(dst, kind, k):
        copy(dst, dst, kind, k, sibling).wait_recv()

    def room(size):
        n = size // (1 << 16)
        if size % (1 << 16):
            return b.w.at[0, 0 : size // (1 << 14), 0, 0]
        if n <= 8:
            return b.ex.at[0, 0:n]
        rows = next(a for a in (2, 3, 4) if n % a == 0 and n // a <= 8)
        return b.ex.at[0:rows, 0 : n // rows]

    loads = {}

    def load(name, src, dst):
        loads[name] = pltpu.make_async_copy(src, dst, rcv["ld"].at[len(loads)])
        loads[name].start()

    mine = b.w.at[y, z, c, x]
    load("w", yw_h, mine)
    load("k", k_h, b.kw.at[0])
    load("q", q_h, b.q)
    load("emb", emb_h, b.emb)
    load("cot", cot_h, b.cot)

    barrier = pltpu.get_barrier_semaphore()
    partners = [sibling, following, preceding]
    for d in range(1, NZ):
        partners.append(dev(cp_1=lax.rem(z + d, NZ)))
    for d in range(1, NY):
        partners.append(dev(cp_0=lax.rem(y + d, NY)))
    for d in range(1, NX):
        for cc in (c, o):
            partners.append(dev(fs=lax.rem(x + d, NX), cp_2=cc))
    for who in partners:
        pl.semaphore_signal(barrier, inc=1, device_id=who, device_id_type=MESH)
    pl.semaphore_wait(barrier, len(partners))

    loads["w"].wait()
    for d in range(1, NZ):
        send(mine, mine, "w1", 0, dev(cp_1=lax.rem(z + d, NZ)))

    doc_t = jnp.transpose(jnp.broadcast_to(doc[...], (TOK, TOK)))
    row = lax.broadcasted_iota(jnp.int32, (TOK, TOK), 0) + block * TOK
    col = lax.broadcasted_iota(jnp.int32, (TOK, TOK), 1)
    for d in range(WIN + 1):
        listed = need[0, 0] == block - d
        for k in range(1, WIN + 1):
            listed = jnp.logical_or(listed, need[0, k] == block - d)
        shut = jnp.where(listed, 0, FAR)
        key_pos = col + (block - d) * TOK
        seen = jnp.logical_and(key_pos >= doc_t + shut, key_pos <= row)
        b.bias[:, d * TOK : (d + 1) * TOK] = jnp.where(seen, 0.0, MASKED)
    for kv in range(KV):
        b.r[kv, 2] = jnp.zeros((TOK, HEAD), F32)
    b.sq[...] = jnp.zeros((TOK, HEAD), F32)
    b.cr[...] = jnp.zeros((TOK, HEAD), F32)

    def turn(e, carry):
        lanes = pl.ds(pl.multiple_of(e * 512, 512), 512)
        turned = jnp.transpose(b.emb[:, lanes]).reshape(4, 2, NX, 16, TOK)
        b.et[lax.div(e, 2), pl.ds(4 * lax.rem(e, 2), 4)] = turned
        return carry

    loads["emb"].wait()

    arrived(room(7 << 14), "w1", 0)
    first, second = b.w.at[y, :, c, x, :, 0:256], b.w.at[y, :, c, x, :, 256:512]
    for d in range(1, 4):
        send(first, first, "w2", 0, dev(cp_0=lax.rem(y + d, NY)))
        send(second, second, "w2", 0, dev(fs=lax.rem(x + d, NX)))

    lax.fori_loop(0, 8, turn, 0)

    arrived(room(6 << 16), "w2", 0)

    def half_a(xx):
        return b.w.at[:, :, c, xx, :, 0:256]

    def half_b(yy):
        return b.w.at[yy, :, c, :, :, 256:512]

    def relay_a(xx, s):
        return b.w.at[:, 4 * s : 4 * s + 4, c, xx, :, 0:256]

    def relay_b(yy, s):
        return b.w.at[yy, 4 * s : 4 * s + 4, c, :, :, 256:512]

    send(half_a(x), half_a(x), "w3", 0, dev(fs=xup))
    send(half_a(x), half_a(x), "w3", 1, dev(fs=xdn))
    send(half_b(y), half_b(y), "w3", 2, dev(cp_0=yup))
    send(half_b(y), half_b(y), "w3", 3, dev(cp_0=ydn))

    send(half_a(x), half_a(x), "wd", 0, sibling)
    send(half_b(y), half_b(y), "wd", 0, sibling)

    loads["k"].wait()

    def keys_at(d, s):
        return b.kw.at[d, 128 * s : 128 * s + 128]

    def pass_keys(s):
        arrived(keys_at(2, s), "k", s)
        send(keys_at(2, s), keys_at(4, s), "k", 2 + s, following)
        send(keys_at(2 * c, s), keys_at(1, s), "k", 4, sibling)

    keys_out = [prepare(keys_at(0, s), keys_at(2, s), "k", s, following) for s in range(2)]

    @pl.when(z != NZ - 1)
    def _():
        for made in keys_out:
            made.start()

    arrived(half_a(x), "w3", 0)
    send(relay_a(xdn, 0), relay_a(xdn, 0), "w3", 4, dev(fs=xup))
    arrived(half_a(x), "w3", 1)
    send(relay_a(xup, 1), relay_a(xup, 1), "w3", 5, dev(fs=xdn))
    arrived(half_b(y), "w3", 3)
    for s in range(2):
        send(relay_b(yup, s), relay_b(yup, s), "w3", 6 + s, dev(cp_0=ydn))

    @pl.when(z == NZ - 1)
    def _():
        for made in keys_out:
            made.start()

    send(half_a(xdn), half_a(xdn), "wd", 0, sibling)
    send(half_a(xup), half_a(xup), "wd", 0, sibling)
    arrived(half_b(y), "w3", 2)
    send(half_b(ydn), half_b(ydn), "wd", 0, sibling)
    send(half_b(yup), half_b(yup), "wd", 0, sibling)
    pass_keys(0)
    pass_keys(1)
    loads["q"].wait()
    for s in range(2):
        arrived(relay_a(x, s), "w3", 4 + s)
        send(relay_a(xop, s), relay_a(xop, s), "wd", 0, sibling)
    for s in range(2):
        arrived(relay_b(y, s), "w3", 6 + s)
        send(relay_b(yop, s), relay_b(yop, s), "wd", 0, sibling)
    def scores(hd, into):
        lanes = pl.ds(pl.multiple_of(hd * HEAD, HEAD), HEAD)
        key_lanes = pl.ds(pl.multiple_of(lax.div(hd, GROUP) * HEAD, HEAD), HEAD)
        keys = b.kw[:, :, key_lanes].reshape(SPAN, HEAD)
        into[...] = lax.dot_general(
            b.q[:, lanes], keys, (((1,), (1,)), ((), ())), preferred_element_type=F32
        )

    def softmax(hd, held):
        for n in range(8):
            rows = slice(n * 32, n * 32 + 32)
            score = held[rows, :] + b.bias[rows, :]
            largest = jnp.max(score, axis=-1, keepdims=True)
            weight = jnp.exp2((score - largest) * EXP2_SCALE)
            total = jnp.sum(weight, axis=-1, keepdims=True)
            b.p[hd, rows, :] = (weight * (1.0 / total)).astype(BF)

    def head_probs(pair, carry):
        scores(2 * pair + 1, b.s1)
        softmax(2 * pair, b.s0)
        scores(jnp.minimum(2 * pair + 2, 15), b.s0)
        softmax(2 * pair + 1, b.s1)
        return carry

    arrived(room(32 << 16), "wd", 0)

    def tokens_of(slot, ys=slice(None)):
        return b.ex.at[ys, :, :, slot * TOK : slot * TOK + TOK]

    kept = pltpu.make_async_copy(b.et.at[:, :, c, x], tokens_of(0), rcv["ld"].at[7])
    kept.start()
    send(b.et.at[:, :, o, x], tokens_of(1), "e", 0, sibling, "es")
    for s, xt in enumerate((xup, xdn)):
        for k, cc in enumerate((c, o)):
            part = b.et.at[2 * s : 2 * s + 2, :, cc, xop]
            send(part, b.er.at[s, k], "e", 1, dev(fs=xt))
    for s, xt in enumerate((xup, xdn)):
        for k, cc in enumerate((c, o)):
            there = tokens_of(2 + 2 * s + k)
            send(b.et.at[:, :, cc, xt], there, "e", 0, dev(fs=xt, cp_2=cc))

    def pass_embeds():
        arrived(b.er, "e", 1)
        for s, xt in enumerate((xup, xdn)):
            for k, cc in enumerate((c, o)):
                there = tokens_of(6 + k, slice(2 * s, 2 * s + 2))
                send(b.er.at[s, k], there, "e", 0, dev(fs=xt, cp_2=cc))

    made = jnp.dot(b.emb[...], b.w[...].reshape(4096, 512), preferred_element_type=F32)
    for kv in range(KV):
        b.vw[kv, 0] = made[:, kv * HEAD : (kv + 1) * HEAD].astype(BF)
        send(b.vw.at[kv, 0], b.vw.at[kv, 2], "v", kv, following)

    def pass_near(kv):
        arrived(b.vw.at[kv, 2], "v", kv)
        send(b.vw.at[kv, 2], b.vw.at[kv, 4], "v", 4 + kv, following)
        send(b.vw.at[kv, 2 * c], b.vw.at[kv, 1], "v", 8 + kv, sibling)

    def pass_far(kv):
        arrived(b.vw.at[kv, 4], "v", 4 + kv)
        send(b.vw.at[kv, 2 + 2 * c], b.vw.at[kv, 3], "v", 8 + kv, sibling)

    def attend(kv):
        arrived(b.vw.at[kv, 0:2], "v", 8 + kv)

        for hd in range(kv * GROUP, kv * GROUP + GROUP):
            values = b.vw[kv].reshape(SPAN, HEAD)
            b.att[hd] = jnp.dot(b.p[hd], values, preferred_element_type=F32)
        for hd in range(kv * GROUP, kv * GROUP + GROUP):
            lanes = slice(hd * HEAD, hd * HEAD + HEAD)
            b.sq[...] += b.att[hd] * b.att[hd]
            b.cr[...] += b.att[hd] * b.cot[:, lanes].astype(F32)

    for s in range(2):
        arrived(keys_at(4, s), "k", 2 + s)
        send(keys_at(2 + 2 * c, s), keys_at(3, s), "k", 4, sibling)

    arrived(room(8 << 16), "k", 4)
    loads["cot"].wait()
    scores(0, b.s0)
    lax.fori_loop(0, 3, head_probs, 0)
    pass_near(0)
    lax.fori_loop(3, 4, head_probs, 0)
    pass_near(1)
    lax.fori_loop(4, 5, head_probs, 0)
    pass_near(2)
    lax.fori_loop(5, 6, head_probs, 0)
    pass_near(3)
    pass_embeds()
    lax.fori_loop(6, 7, head_probs, 0)
    pass_far(0)
    lax.fori_loop(7, 8, head_probs, 0)
    pass_far(1)
    attend(0)
    pass_far(2)
    attend(1)
    pass_far(3)
    attend(2)
    attend(3)

    token_total = TOK * NY * NZ * 2 * NX
    mean = jnp.sum(b.sq[...], axis=-1, keepdims=True) * (1.0 / 2048.0) + NORM_EPS
    inv = 1.0 / jnp.sqrt(mean)
    inner = jnp.sum(b.cr[...], axis=-1, keepdims=True) * (1.0 / (2048.0 * token_total)) * inv
    b.cr[...] = jnp.broadcast_to(inner * inv, (TOK, HEAD))
    b.sq[...] = jnp.broadcast_to(inv, (TOK, HEAD))

    def norm_grads(kv):
        for hd in range(kv * GROUP, kv * GROUP + GROUP):
            up = b.cot[:, hd * HEAD : (hd + 1) * HEAD].astype(F32) * (1.0 / token_total)
            b.og[hd] = ((up - b.att[hd] * b.cr[...]) * b.sq[...]).astype(BF)

    def grads(kv, low, high):
        up = b.og[kv * GROUP : kv * GROUP + GROUP].reshape(GROUP * TOK, HEAD)
        for d in range(low, high):
            lanes = slice(d * TOK, d * TOK + TOK)
            part = b.p[kv * GROUP : kv * GROUP + GROUP, :, lanes].reshape(GROUP * TOK, TOK)
            b.dv[kv, d] = lax.dot_general(
                part, up, (((0,), (0,)), ((), ())), preferred_element_type=F32
            )

    def grads_far(kv):
        norm_grads(kv)
        grads(kv, 3, 5)
        send(b.dv.at[kv, 3], b.r.at[kv, 1], "r", 2 * kv + 1, sibling)

    def grads_near(kv):
        grads(kv, 1, 3)
        send(b.dv.at[kv, 1], b.r.at[kv, 0], "r", 2 * kv, sibling)

    def leave_far(kv):
        arrived(b.r.at[kv, 1], "r", 2 * kv + 1)
        b.fo[kv] = (b.dv[kv, 4] + b.r[kv, 2 - c]).astype(BF)
        send(b.fo.at[kv], b.fi.at[kv], "f", kv, preceding)

    def leave_near(kv):
        arrived(b.r.at[kv, 0], "r", 2 * kv)
        arrived(b.fi.at[kv], "f", kv)
        b.go[kv] = (b.dv[kv, 2] + b.r[kv, 1 - c] + b.fi[kv].astype(F32)).astype(BF)
        send(b.go.at[kv], b.gi.at[kv], "g", kv, preceding)

    def vg_at(kv, slot, rows=slice(None)):
        lanes = slice((kv % 2) * HEAD, (kv % 2) * HEAD + HEAD)
        return b.vg.at[kv // 2, slot, rows, lanes]

    upper, lower = slice(0, 128), slice(128, 256)

    def settle(kv):
        arrived(b.gi.at[kv], "g", kv)
        total = b.dv[kv, 0] + b.r[kv, 2 * c] + b.gi[kv].astype(F32)
        b.vg[kv // 2, 0, :, (kv % 2) * HEAD : (kv % 2) * HEAD + HEAD] = total.astype(BF)
        send(vg_at(kv, 0), vg_at(kv, 2), "vg", 3 * kv, dev(fs=xup))
        send(vg_at(kv, 0), vg_at(kv, 4), "vg", 3 * kv + 1, dev(fs=xdn))
        send(vg_at(kv, 0), vg_at(kv, 1), "vd", kv // 2, sibling)

    def relay(kv):
        arrived(vg_at(kv, 2), "vg", 3 * kv)
        send(vg_at(kv, 2, upper), vg_at(kv, 6, upper), "vg", 3 * kv + 2, dev(fs=xup))
        send(vg_at(kv, 2), vg_at(kv, 3), "vd", kv // 2, sibling)
        arrived(vg_at(kv, 4), "vg", 3 * kv + 1)
        send(vg_at(kv, 4, lower), vg_at(kv, 6, lower), "vg", 3 * kv + 2, dev(fs=xdn))
        send(vg_at(kv, 4), vg_at(kv, 5), "vd", kv // 2, sibling)

    def collect(kv):
        arrived(vg_at(kv, 6), "vg", 3 * kv + 2)
        send(vg_at(kv, 6), vg_at(kv, 7), "vd", 2 + kv // 2, sibling)

    grads_far(0)
    grads_far(1)
    leave_far(0)
    grads_far(2)
    leave_far(1)
    grads_far(3)
    leave_far(2)
    grads_near(0)
    leave_far(3)
    grads_near(1)
    grads_near(2)
    leave_near(0)
    grads_near(3)
    leave_near(1)
    grads(0, 0, 1)
    grads(1, 0, 1)
    leave_near(2)
    grads(2, 0, 1)
    grads(3, 0, 1)
    leave_near(3)
    kept.wait()
    arrived(room(28 << 16), "e", 0)

    for kv in range(KV):
        settle(kv)
    for kv in range(KV):
        relay(kv)

    def early(h):
        arrived(room(6 << 16), "vd", h)
        for ys in (slice(0, 2), slice(2, 4)):
            b.g[h, ys] = jnp.dot(
                b.ex[ys, :, :, 0 : 6 * TOK].reshape(256, 6 * TOK),
                b.vg[h, 0:6].reshape(6 * TOK, 256),
                preferred_element_type=F32,
            ).reshape(2, NZ, 16, 256)

    def product(h):
        arrived(room(2 << 16), "vd", 2 + h)
        for ys in (slice(0, 2), slice(2, 4)):
            b.g[h, ys] += jnp.dot(
                b.ex[ys, :, :, 6 * TOK : 8 * TOK].reshape(256, 2 * TOK),
                b.vg[h, 6:8].reshape(2 * TOK, 256),
                preferred_element_type=F32,
            ).reshape(2, NZ, 16, 256)
        b.g1[h] = b.g[h, yop].astype(BF)
        send(b.g1.at[h, 0:4], b.x1.at[h, 0], "x", 3 * h, dev(cp_0=yup))
        send(b.g1.at[h, 4:8], b.x1.at[h, 1], "x", 3 * h + 1, dev(cp_0=ydn))

    def across(h):
        arrived(b.x1.at[h, 0], "x", 3 * h)
        b.tx[h, 0, 0:4] = (b.g[h, yup, 0:4] + b.x1[h, 0].astype(F32)).astype(BF)
        b.tx[h, 0, 4:8] = b.g[h, yup, 4:8].astype(BF)
        send(b.tx.at[h, 0], b.x2.at[h, 0], "x", 3 * h + 2, dev(cp_0=yup))
        arrived(b.x1.at[h, 1], "x", 3 * h + 1)
        b.tx[h, 1, 0:4] = b.g[h, ydn, 0:4].astype(BF)
        b.tx[h, 1, 4:8] = (b.g[h, ydn, 4:8] + b.x1[h, 1].astype(F32)).astype(BF)
        send(b.tx.at[h, 1], b.x2.at[h, 1], "x", 3 * h + 2, dev(cp_0=ydn))

    def along(h):
        arrived(b.x2.at[h], "x", 3 * h + 2)
        b.t[h] = b.g[h, y] + b.x2[h, 0].astype(F32) + b.x2[h, 1].astype(F32)
        b.tz[h] = b.t[h].astype(BF)
        for d in (4, 3, 5, 2, 6, 1, 7):
            zt = lax.rem(z + d, NZ)
            send(b.tz.at[h, zt], b.rz.at[h, z], "z", h, dev(cp_1=zt))

    def finish(h):
        arrived(b.rz.at[h, 0:7], "z", h)
        total = b.t[h, z]
        for d in range(1, NZ):
            total = total + b.rz[h, lax.rem(z + d, NZ)].astype(F32)
        out[:, h * 256 : (h + 1) * 256] = total

    early(0)
    collect(0)
    collect(1)
    early(1)
    collect(2)
    product(0)
    collect(3)
    product(1)
    across(0)
    across(1)
    along(0)
    along(1)
    finish(0)
    finish(1)

    for kind, size in sent.items():
        if size:
            copy(room(size), room(size), "w1", 0, sibling, kind).wait_send()


def weight_gradient(need_ids, doc_start, embeds, queries, key_heads, cotangent, y_weight):
    any_space = pl.BlockSpec(memory_space=pl.ANY)
    vmem = pl.BlockSpec(memory_space=pltpu.VMEM)
    semaphores = [pltpu.SemaphoreType.DMA((n,)) for n in SEMAPHORES.values()]
    semaphores.append(pltpu.SemaphoreType.DMA((len(SENDERS),)))
    return pl.pallas_call(
        kernel,
        out_shape=pltpu.VMEM((16, 512), F32),
        in_specs=[pl.BlockSpec(memory_space=pltpu.SMEM), vmem] + [any_space] * 5,
        out_specs=vmem,
        scratch_shapes=[pltpu.VMEM(shape, kind) for shape, kind in BUFFERS.values()]
        + semaphores,
        compiler_params=pltpu.CompilerParams(
            collective_id=0, has_side_effects=True, vmem_limit_bytes=58 << 20
        ),
    )(need_ids, doc_start, embeds, queries, key_heads, cotangent, y_weight)


def on_device(
    embeds,
    queries,
    key_heads,
    cotangent,
    doc_start,
    need_ids,
    y_weight,
    z_weight,
    x_weight,
    second_moment,
):
    gradient = weight_gradient(
        need_ids[0], doc_start, embeds[0], queries[0], key_heads[0], cotangent[0], y_weight
    )
    moment_next = MOMENT_DECAY * second_moment + (1.0 - MOMENT_DECAY) * gradient * gradient
    z_next = z_weight - LEARN_RATE * (
        gradient / (jnp.sqrt(moment_next) + ADAM_EPS) + WEIGHT_DECAY * y_weight.astype(jnp.float32)
    )
    x_next = (1.0 - AVERAGE_MIX) * x_weight + AVERAGE_MIX * z_next
    y_next = ((1.0 - INTERP_BETA) * z_next + INTERP_BETA * x_next).astype(jnp.bfloat16)
    return (z_next, x_next, moment_next, y_next)


def solution(mesh):
    finer = Mesh(mesh.devices.reshape(NY, NZ, 2, mesh.shape["fs"]), CP_FS)
    return jax.shard_map(
        on_device,
        mesh=finer,
        in_specs=(
            P("fs", CP, None),
            P("fs", CP, None),
            P("fs", CP, None),
            P("fs", CP, None),
            P("fs", CP),
            P("fs", CP, None),
            P(CP_FS, None),
            P(CP_FS, None),
            P(CP_FS, None),
            P(CP_FS, None),
        ),
        out_specs=(P(CP_FS, None), P(CP_FS, None), P(CP_FS, None), P(CP_FS, None)),
        check_vma=False,
    )
```

```python
import math
from types import SimpleNamespace

import jax
import jax.numpy as jnp
from jax import lax
from jax.experimental import pallas as pl
from jax.experimental.pallas import tpu as pltpu
from jax.sharding import Mesh
from jax.sharding import PartitionSpec as P

HEAD = 128
KV = 4
WIN = 4
GROUP = 4
TOK = 256
SPAN = (WIN + 1) * TOK
NY, NZ, NX = 4, 8, 4
CP = ("cp_0", "cp_1", "cp_2")
CP_FS = ("cp_0", "cp_1", "cp_2", "fs")

NORM_EPS = 0.01
MOMENT_DECAY = 0.95
LEARN_RATE = 0.005
WEIGHT_DECAY = 0.1
ADAM_EPS = 1e-08
AVERAGE_MIX = 0.25
INTERP_BETA = 0.9
EXP2_SCALE = math.log2(math.e) / math.sqrt(HEAD)
MASKED = -1e30
FAR = 1 << 30

BF = jnp.bfloat16
F32 = jnp.float32
MESH = pl.DeviceIdType.MESH

BUFFERS = {
    "emb": ((TOK, 4096), BF),
    "w": ((NY, NZ, 2, NX, 16, 512), BF),
    "q": ((TOK, 2048), BF),
    "kw": ((5, TOK, 512), BF),
    "vw": ((KV, 5, TOK, HEAD), BF),
    "cot": ((TOK, 2048), BF),
    "p": ((16, TOK, SPAN), BF),
    "s0": ((TOK, SPAN), F32),
    "s1": ((TOK, SPAN), F32),
    "bias": ((TOK, SPAN), F32),
    "att": ((16, TOK, HEAD), F32),
    "sq": ((TOK, HEAD), F32),
    "cr": ((TOK, HEAD), F32),
    "og": ((16, TOK, HEAD), BF),
    "dv": ((KV, 5, TOK, HEAD), F32),
    "r": ((KV, 3, TOK, HEAD), F32),
    "fo": ((KV, TOK, HEAD), BF),
    "fi": ((KV, TOK, HEAD), BF),
    "go": ((KV, TOK, HEAD), BF),
    "gi": ((KV, TOK, HEAD), BF),
    "vg": ((2, 8, TOK, 256), BF),
    "et": ((NY, NZ, 2, NX, 16, TOK), BF),
    "er": ((2, 2, 2, NZ, 16, TOK), BF),
    "ex": ((NY, NZ, 16, 8 * TOK), BF),
    "g": ((2, NY, NZ, 16, 256), F32),
    "g1": ((2, NZ, 16, 256), BF),
    "x1": ((2, 2, 4, 16, 256), BF),
    "tx": ((2, 2, NZ, 16, 256), BF),
    "x2": ((2, 2, NZ, 16, 256), BF),
    "t": ((2, NZ, 16, 256), F32),
    "tz": ((2, NZ, 16, 256), BF),
    "sum": ((2, 16, 256), F32),
    "rz": ((2, NZ, 16, 256), BF),
}
SEMAPHORES = {
    "ld": 8,
    "w1": 1,
    "w2": 1,
    "w3": 8,
    "wd": 1,
    "k": 5,
    "v": 12,
    "e": 2,
    "r": 8,
    "f": 4,
    "g": 4,
    "vg": 12,
    "vd": 4,
    "x": 6,
    "z": 2,
}
SENDERS = tuple(SEMAPHORES) + ("es",)


def kernel(need, doc, emb_h, q_h, k_h, cot_h, yw_h, out, *scratch):
    names = list(BUFFERS)
    b = SimpleNamespace(**dict(zip(names, scratch)))
    rest = scratch[len(names) :]
    rcv, snd = dict(zip(SEMAPHORES, rest)), rest[-1]

    y, z = lax.axis_index("cp_0"), lax.axis_index("cp_1")
    c, x = lax.axis_index("cp_2"), lax.axis_index("fs")
    o = 1 - c
    zn, yn = lax.rem(z + 1, NZ), lax.rem(y + lax.div(z + 1, NZ), NY)
    zp, yp = lax.rem(z + NZ - 1, NZ), lax.rem(y + NY - 1 + lax.div(z + NZ - 1, NZ), NY)
    yup, ydn = lax.rem(y + 1, NY), lax.rem(y + NY - 1, NY)
    xup, xdn = lax.rem(x + 1, NX), lax.rem(x + NX - 1, NX)
    yop, xop = lax.rem(y + 2, NY), lax.rem(x + 2, NX)
    block = (y * NZ + z) * 2 + c

    def dev(cp_0=y, cp_1=z, cp_2=c, fs=x):
        return {"cp_0": cp_0, "cp_1": cp_1, "cp_2": cp_2, "fs": fs}

    sibling = dev(cp_2=o)
    following, preceding = dev(cp_0=yn, cp_1=zn), dev(cp_0=yp, cp_1=zp)

    sent = dict.fromkeys(SENDERS, 0)
    results = []

    def copy(src, dst, kind, k, to, sender=None):
        return pltpu.make_async_remote_copy(
            src_ref=src,
            dst_ref=dst,
            send_sem=snd.at[SENDERS.index(sender or kind)],
            recv_sem=rcv[kind].at[k],
            device_id=to,
            device_id_type=MESH,
        )

    def prepare(src, dst, kind, k, to, sender=None):
        sent[sender or kind] += math.prod(src.shape) * jnp.dtype(src.dtype).itemsize
        return copy(src, dst, kind, k, to, sender)

    def send(*what):
        prepare(*what).start()

    def arrived(dst, kind, k):
        copy(dst, dst, kind, k, sibling).wait_recv()

    def room(size):
        n = size // (1 << 16)
        if size % (1 << 16):
            return b.w.at[0, 0 : size // (1 << 14), 0, 0]
        if n <= 8:
            return b.ex.at[0, 0:n]
        rows = next(a for a in (2, 3, 4) if n % a == 0 and n // a <= 8)
        return b.ex.at[0:rows, 0 : n // rows]

    loads = {}

    def load(name, src, dst):
        loads[name] = pltpu.make_async_copy(src, dst, rcv["ld"].at[len(loads)])
        loads[name].start()

    mine = b.w.at[y, z, c, x]
    load("w", yw_h, mine)
    load("k", k_h, b.kw.at[0])
    load("q", q_h, b.q)
    load("emb", emb_h, b.emb)
    load("cot", cot_h, b.cot)

    barrier = pltpu.get_barrier_semaphore()
    partners = [sibling, following, preceding]
    for d in range(1, NZ):
        partners.append(dev(cp_1=lax.rem(z + d, NZ)))
    for d in range(1, NY):
        partners.append(dev(cp_0=lax.rem(y + d, NY)))
    for d in range(1, NX):
        for cc in (c, o):
            partners.append(dev(fs=lax.rem(x + d, NX), cp_2=cc))
    for who in partners:
        pl.semaphore_signal(barrier, inc=1, device_id=who, device_id_type=MESH)
    pl.semaphore_wait(barrier, len(partners))

    loads["w"].wait()
    for d in range(1, NZ):
        send(mine, mine, "w1", 0, dev(cp_1=lax.rem(z + d, NZ)))

    doc_t = jnp.transpose(jnp.broadcast_to(doc[...], (TOK, TOK)))
    row = lax.broadcasted_iota(jnp.int32, (TOK, TOK), 0) + block * TOK
    col = lax.broadcasted_iota(jnp.int32, (TOK, TOK), 1)
    for d in range(WIN + 1):
        listed = need[0, 0] == block - d
        for k in range(1, WIN + 1):
            listed = jnp.logical_or(listed, need[0, k] == block - d)
        shut = jnp.where(listed, 0, FAR)
        key_pos = col + (block - d) * TOK
        seen = jnp.logical_and(key_pos >= doc_t + shut, key_pos <= row)
        b.bias[:, d * TOK : (d + 1) * TOK] = jnp.where(seen, 0.0, MASKED)
    for kv in range(KV):
        b.r[kv, 2] = jnp.zeros((TOK, HEAD), F32)
    b.sq[...] = jnp.zeros((TOK, HEAD), F32)
    b.cr[...] = jnp.zeros((TOK, HEAD), F32)

    def turn(e, carry):
        lanes = pl.ds(pl.multiple_of(e * 512, 512), 512)
        turned = jnp.transpose(b.emb[:, lanes]).reshape(4, 2, NX, 16, TOK)
        b.et[lax.div(e, 2), pl.ds(4 * lax.rem(e, 2), 4)] = turned
        return carry

    loads["emb"].wait()

    arrived(room(7 << 14), "w1", 0)
    first, second = b.w.at[y, :, c, x, :, 0:256], b.w.at[y, :, c, x, :, 256:512]
    for d in range(1, 4):
        send(first, first, "w2", 0, dev(cp_0=lax.rem(y + d, NY)))
        send(second, second, "w2", 0, dev(fs=lax.rem(x + d, NX)))

    lax.fori_loop(0, 8, turn, 0)

    arrived(room(6 << 16), "w2", 0)

    def half_a(xx):
        return b.w.at[:, :, c, xx, :, 0:256]

    def half_b(yy):
        return b.w.at[yy, :, c, :, :, 256:512]

    def relay_a(xx, s):
        return b.w.at[:, 4 * s : 4 * s + 4, c, xx, :, 0:256]

    def relay_b(yy, s):
        return b.w.at[yy, 4 * s : 4 * s + 4, c, :, :, 256:512]

    send(half_a(x), half_a(x), "w3", 0, dev(fs=xup))
    send(half_a(x), half_a(x), "w3", 1, dev(fs=xdn))
    send(half_b(y), half_b(y), "w3", 2, dev(cp_0=yup))
    send(half_b(y), half_b(y), "w3", 3, dev(cp_0=ydn))

    send(half_a(x), half_a(x), "wd", 0, sibling)
    send(half_b(y), half_b(y), "wd", 0, sibling)

    loads["k"].wait()

    def keys_at(d, s):
        return b.kw.at[d, 128 * s : 128 * s + 128]

    for s in range(2):
        send(keys_at(0, s), keys_at(2, s), "k", s, following)
    keys_on = [
        (
            prepare(keys_at(2, s), keys_at(4, s), "k", 2 + s, following),
            prepare(keys_at(2 * c, s), keys_at(1, s), "k", 4, sibling),
        )
        for s in range(2)
    ]

    def pass_keys():
        for s in range(2):
            arrived(keys_at(2, s), "k", s)
            for made in keys_on[s]:
                made.start()

    arrived(half_a(x), "w3", 0)
    send(relay_a(xdn, 0), relay_a(xdn, 0), "w3", 4, dev(fs=xup))
    arrived(half_a(x), "w3", 1)
    send(relay_a(xup, 1), relay_a(xup, 1), "w3", 5, dev(fs=xdn))
    up_0 = prepare(relay_b(ydn, 0), relay_b(ydn, 0), "w3", 6, dev(cp_0=yup))
    down_0 = copy(relay_b(yup, 0), relay_b(yup, 0), "w3", 6, dev(cp_0=ydn))
    down_1 = prepare(relay_b(yup, 1), relay_b(yup, 1), "w3", 7, dev(cp_0=ydn))

    @pl.when(z != 0)
    def _():
        arrived(half_b(y), "w3", 2)
        up_0.start()
        arrived(half_b(y), "w3", 3)
        down_1.start()

    @pl.when(z == 0)
    def _():
        arrived(half_b(y), "w3", 3)
        down_0.start()
        down_1.start()

    send(half_a(xdn), half_a(xdn), "wd", 0, sibling)
    send(half_a(xup), half_a(xup), "wd", 0, sibling)
    send(half_b(yup), half_b(yup), "wd", 0, sibling)

    @pl.when(z != NZ - 1)
    def _():
        pass_keys()

    @pl.when(z == 0)
    def _():
        arrived(half_b(y), "w3", 2)

    send(half_b(ydn), half_b(ydn), "wd", 0, sibling)
    loads["q"].wait()
    for s in range(2):
        arrived(relay_a(x, s), "w3", 4 + s)
        send(relay_a(xop, s), relay_a(xop, s), "wd", 0, sibling)

    @pl.when(z == NZ - 1)
    def _():
        pass_keys()

    for s in range(2):
        arrived(relay_b(y, s), "w3", 6 + s)
        send(relay_b(yop, s), relay_b(yop, s), "wd", 0, sibling)

    def scores(hd, into):
        lanes = pl.ds(pl.multiple_of(hd * HEAD, HEAD), HEAD)
        key_lanes = pl.ds(pl.multiple_of(lax.div(hd, GROUP) * HEAD, HEAD), HEAD)
        keys = b.kw[:, :, key_lanes].reshape(SPAN, HEAD)
        into[...] = lax.dot_general(
            b.q[:, lanes], keys, (((1,), (1,)), ((), ())), preferred_element_type=F32
        )

    def softmax(hd, held):
        for n in range(8):
            rows = slice(n * 32, n * 32 + 32)
            score = held[rows, :] + b.bias[rows, :]
            largest = jnp.max(score, axis=-1, keepdims=True)
            weight = jnp.exp2((score - largest) * EXP2_SCALE)
            total = jnp.sum(weight, axis=-1, keepdims=True)
            b.p[hd, rows, :] = (weight * (1.0 / total)).astype(BF)

    def head_probs(pair, carry):
        scores(2 * pair + 1, b.s1)
        softmax(2 * pair, b.s0)
        scores(jnp.minimum(2 * pair + 2, 15), b.s0)
        softmax(2 * pair + 1, b.s1)
        return carry

    arrived(room(32 << 16), "wd", 0)

    def tokens_of(slot, ys=slice(None)):
        return b.ex.at[ys, :, :, slot * TOK : slot * TOK + TOK]

    kept = pltpu.make_async_copy(b.et.at[:, :, c, x], tokens_of(0), rcv["ld"].at[7])
    kept.start()
    send(b.et.at[:, :, o, x], tokens_of(1), "e", 0, sibling, "es")
    for s, xt in enumerate((xup, xdn)):
        for k, cc in enumerate((c, o)):
            part = b.et.at[2 * s : 2 * s + 2, :, cc, xop]
            send(part, b.er.at[s, k], "e", 1, dev(fs=xt))
    for s, xt in enumerate((xup, xdn)):
        for k, cc in enumerate((c, o)):
            there = tokens_of(2 + 2 * s + k)
            send(b.et.at[:, :, cc, xt], there, "e", 0, dev(fs=xt, cp_2=cc))

    def pass_embeds():
        arrived(b.er, "e", 1)
        for s, xt in enumerate((xup, xdn)):
            for k, cc in enumerate((c, o)):
                there = tokens_of(6 + k, slice(2 * s, 2 * s + 2))
                send(b.er.at[s, k], there, "e", 0, dev(fs=xt, cp_2=cc))

    made = jnp.dot(b.emb[...], b.w[...].reshape(4096, 512), preferred_element_type=F32)
    for kv in range(KV):
        b.vw[kv, 0] = made[:, kv * HEAD : (kv + 1) * HEAD].astype(BF)
        send(b.vw.at[kv, 0], b.vw.at[kv, 2], "v", kv, following)

    def pass_near(kv):
        arrived(b.vw.at[kv, 2], "v", kv)
        send(b.vw.at[kv, 2], b.vw.at[kv, 4], "v", 4 + kv, following)
        send(b.vw.at[kv, 2 * c], b.vw.at[kv, 1], "v", 8 + kv, sibling)

    def pass_far(kv):
        arrived(b.vw.at[kv, 4], "v", 4 + kv)
        send(b.vw.at[kv, 2 + 2 * c], b.vw.at[kv, 3], "v", 8 + kv, sibling)

    def attend(kv):
        arrived(b.vw.at[kv, 0:2], "v", 8 + kv)

        for hd in range(kv * GROUP, kv * GROUP + GROUP):
            values = b.vw[kv].reshape(SPAN, HEAD)
            b.att[hd] = jnp.dot(b.p[hd], values, preferred_element_type=F32)
        for hd in range(kv * GROUP, kv * GROUP + GROUP):
            lanes = slice(hd * HEAD, hd * HEAD + HEAD)
            b.sq[...] += b.att[hd] * b.att[hd]
            b.cr[...] += b.att[hd] * b.cot[:, lanes].astype(F32)

    for s in range(2):
        arrived(keys_at(4, s), "k", 2 + s)
        send(keys_at(2 + 2 * c, s), keys_at(3, s), "k", 4, sibling)

    arrived(room(8 << 16), "k", 4)
    loads["cot"].wait()
    scores(0, b.s0)
    lax.fori_loop(0, 3, head_probs, 0)
    pass_near(0)
    lax.fori_loop(3, 4, head_probs, 0)
    pass_near(1)
    lax.fori_loop(4, 5, head_probs, 0)
    pass_near(2)
    lax.fori_loop(5, 6, head_probs, 0)
    pass_near(3)
    pass_embeds()
    lax.fori_loop(6, 7, head_probs, 0)
    pass_far(0)
    lax.fori_loop(7, 8, head_probs, 0)
    pass_far(1)
    attend(0)
    pass_far(2)
    attend(1)
    pass_far(3)
    attend(2)
    attend(3)

    token_total = TOK * NY * NZ * 2 * NX
    mean = jnp.sum(b.sq[...], axis=-1, keepdims=True) * (1.0 / 2048.0) + NORM_EPS
    inv = 1.0 / jnp.sqrt(mean)
    inner = jnp.sum(b.cr[...], axis=-1, keepdims=True) * (1.0 / (2048.0 * token_total)) * inv
    b.cr[...] = jnp.broadcast_to(inner * inv, (TOK, HEAD))
    b.sq[...] = jnp.broadcast_to(inv, (TOK, HEAD))

    def norm_grads(kv):
        for hd in range(kv * GROUP, kv * GROUP + GROUP):
            up = b.cot[:, hd * HEAD : (hd + 1) * HEAD].astype(F32) * (1.0 / token_total)
            b.og[hd] = ((up - b.att[hd] * b.cr[...]) * b.sq[...]).astype(BF)

    def grads(kv, low, high):
        up = b.og[kv * GROUP : kv * GROUP + GROUP].reshape(GROUP * TOK, HEAD)
        for d in range(low, high):
            lanes = slice(d * TOK, d * TOK + TOK)
            part = b.p[kv * GROUP : kv * GROUP + GROUP, :, lanes].reshape(GROUP * TOK, TOK)
            b.dv[kv, d] = lax.dot_general(
                part, up, (((0,), (0,)), ((), ())), preferred_element_type=F32
            )

    def grads_far(kv):
        norm_grads(kv)
        grads(kv, 3, 5)
        send(b.dv.at[kv, 3], b.r.at[kv, 1], "r", 2 * kv + 1, sibling)

    def grads_near(kv):
        grads(kv, 1, 3)
        send(b.dv.at[kv, 1], b.r.at[kv, 0], "r", 2 * kv, sibling)

    def leave_far(kv):
        arrived(b.r.at[kv, 1], "r", 2 * kv + 1)
        b.fo[kv] = (b.dv[kv, 4] + b.r[kv, 2 - c]).astype(BF)
        send(b.fo.at[kv], b.fi.at[kv], "f", kv, preceding)

    def leave_near(kv):
        arrived(b.r.at[kv, 0], "r", 2 * kv)
        arrived(b.fi.at[kv], "f", kv)
        b.go[kv] = (b.dv[kv, 2] + b.r[kv, 1 - c] + b.fi[kv].astype(F32)).astype(BF)
        send(b.go.at[kv], b.gi.at[kv], "g", kv, preceding)

    def vg_at(kv, slot, rows=slice(None)):
        lanes = slice((kv % 2) * HEAD, (kv % 2) * HEAD + HEAD)
        return b.vg.at[kv // 2, slot, rows, lanes]

    upper, lower = slice(0, 128), slice(128, 256)

    def settle(kv):
        arrived(b.gi.at[kv], "g", kv)
        total = b.dv[kv, 0] + b.r[kv, 2 * c] + b.gi[kv].astype(F32)
        b.vg[kv // 2, 0, :, (kv % 2) * HEAD : (kv % 2) * HEAD + HEAD] = total.astype(BF)
        send(vg_at(kv, 0), vg_at(kv, 2), "vg", 3 * kv, dev(fs=xup))
        send(vg_at(kv, 0), vg_at(kv, 4), "vg", 3 * kv + 1, dev(fs=xdn))
        send(vg_at(kv, 0), vg_at(kv, 1), "vd", kv // 2, sibling)

    def relay(kv):
        arrived(vg_at(kv, 2), "vg", 3 * kv)
        send(vg_at(kv, 2, upper), vg_at(kv, 6, upper), "vg", 3 * kv + 2, dev(fs=xup))
        send(vg_at(kv, 2), vg_at(kv, 3), "vd", kv // 2, sibling)
        arrived(vg_at(kv, 4), "vg", 3 * kv + 1)
        send(vg_at(kv, 4, lower), vg_at(kv, 6, lower), "vg", 3 * kv + 2, dev(fs=xdn))
        send(vg_at(kv, 4), vg_at(kv, 5), "vd", kv // 2, sibling)

    def collect(kv):
        arrived(vg_at(kv, 6), "vg", 3 * kv + 2)
        send(vg_at(kv, 6), vg_at(kv, 7), "vd", 2 + kv // 2, sibling)

    grads_far(0)
    grads_far(1)
    leave_far(0)
    grads_far(2)
    leave_far(1)
    grads_far(3)
    leave_far(2)
    grads_near(0)
    leave_far(3)
    grads_near(1)
    grads_near(2)
    leave_near(0)
    grads_near(3)
    leave_near(1)
    grads(0, 0, 1)
    grads(1, 0, 1)
    leave_near(2)
    grads(2, 0, 1)
    grads(3, 0, 1)
    leave_near(3)
    kept.wait()
    arrived(room(28 << 16), "e", 0)

    for kv in range(KV):
        settle(kv)
    for kv in range(KV):
        relay(kv)

    def early(h):
        arrived(room(6 << 16), "vd", h)
        for ys in (slice(0, 2), slice(2, 4)):
            b.g[h, ys] = jnp.dot(
                b.ex[ys, :, :, 0 : 6 * TOK].reshape(256, 6 * TOK),
                b.vg[h, 0:6].reshape(6 * TOK, 256),
                preferred_element_type=F32,
            ).reshape(2, NZ, 16, 256)

    def product(h):
        arrived(room(2 << 16), "vd", 2 + h)
        for ys in (slice(0, 2), slice(2, 4)):
            b.g[h, ys] += jnp.dot(
                b.ex[ys, :, :, 6 * TOK : 8 * TOK].reshape(256, 2 * TOK),
                b.vg[h, 6:8].reshape(2 * TOK, 256),
                preferred_element_type=F32,
            ).reshape(2, NZ, 16, 256)
        b.g1[h] = b.g[h, yop].astype(BF)
        send(b.g1.at[h, 0:4], b.x1.at[h, 0], "x", 3 * h, dev(cp_0=yup))
        send(b.g1.at[h, 4:8], b.x1.at[h, 1], "x", 3 * h + 1, dev(cp_0=ydn))

    def across(h):
        arrived(b.x1.at[h, 0], "x", 3 * h)
        b.tx[h, 0, 0:4] = (b.g[h, yup, 0:4] + b.x1[h, 0].astype(F32)).astype(BF)
        b.tx[h, 0, 4:8] = b.g[h, yup, 4:8].astype(BF)
        send(b.tx.at[h, 0], b.x2.at[h, 0], "x", 3 * h + 2, dev(cp_0=yup))
        arrived(b.x1.at[h, 1], "x", 3 * h + 1)
        b.tx[h, 1, 0:4] = b.g[h, ydn, 0:4].astype(BF)
        b.tx[h, 1, 4:8] = (b.g[h, ydn, 4:8] + b.x1[h, 1].astype(F32)).astype(BF)
        send(b.tx.at[h, 1], b.x2.at[h, 1], "x", 3 * h + 2, dev(cp_0=ydn))

    def along(h):
        arrived(b.x2.at[h], "x", 3 * h + 2)
        b.t[h] = b.g[h, y] + b.x2[h, 0].astype(F32) + b.x2[h, 1].astype(F32)
        b.tz[h] = b.t[h].astype(BF)
        for d in (4, 3, 5, 2, 6, 1, 7):
            zt = lax.rem(z + d, NZ)
            send(b.tz.at[h, zt], b.rz.at[h, z], "z", h, dev(cp_1=zt))

    def finish(h):
        arrived(b.rz.at[h, 0:7], "z", h)
        total = b.t[h, z]
        for d in range(1, NZ):
            total = total + b.rz[h, lax.rem(z + d, NZ)].astype(F32)
        out[:, h * 256 : (h + 1) * 256] = total

    early(0)
    collect(0)
    collect(1)
    early(1)
    collect(2)
    product(0)
    collect(3)
    product(1)
    across(0)
    across(1)
    along(0)
    along(1)
    finish(0)
    finish(1)

    for kind, size in sent.items():
        if size:
            copy(room(size), room(size), "w1", 0, sibling, kind).wait_send()


def weight_gradient(need_ids, doc_start, embeds, queries, key_heads, cotangent, y_weight):
    any_space = pl.BlockSpec(memory_space=pl.ANY)
    vmem = pl.BlockSpec(memory_space=pltpu.VMEM)
    semaphores = [pltpu.SemaphoreType.DMA((n,)) for n in SEMAPHORES.values()]
    semaphores.append(pltpu.SemaphoreType.DMA((len(SENDERS),)))
    return pl.pallas_call(
        kernel,
        out_shape=pltpu.VMEM((16, 512), F32),
        in_specs=[pl.BlockSpec(memory_space=pltpu.SMEM), vmem] + [any_space] * 5,
        out_specs=vmem,
        scratch_shapes=[pltpu.VMEM(shape, kind) for shape, kind in BUFFERS.values()]
        + semaphores,
        compiler_params=pltpu.CompilerParams(
            collective_id=0, has_side_effects=True, vmem_limit_bytes=58 << 20
        ),
    )(need_ids, doc_start, embeds, queries, key_heads, cotangent, y_weight)


def on_device(
    embeds,
    queries,
    key_heads,
    cotangent,
    doc_start,
    need_ids,
    y_weight,
    z_weight,
    x_weight,
    second_moment,
):
    gradient = weight_gradient(
        need_ids[0], doc_start, embeds[0], queries[0], key_heads[0], cotangent[0], y_weight
    )
    moment_next = MOMENT_DECAY * second_moment + (1.0 - MOMENT_DECAY) * gradient * gradient
    z_next = z_weight - LEARN_RATE * (
        gradient / (jnp.sqrt(moment_next) + ADAM_EPS) + WEIGHT_DECAY * y_weight.astype(jnp.float32)
    )
    x_next = (1.0 - AVERAGE_MIX) * x_weight + AVERAGE_MIX * z_next
    y_next = ((1.0 - INTERP_BETA) * z_next + INTERP_BETA * x_next).astype(jnp.bfloat16)
    return (z_next, x_next, moment_next, y_next)


def solution(mesh):
    finer = Mesh(mesh.devices.reshape(NY, NZ, 2, mesh.shape["fs"]), CP_FS)
    return jax.shard_map(
        on_device,
        mesh=finer,
        in_specs=(
            P("fs", CP, None),
            P("fs", CP, None),
            P("fs", CP, None),
            P("fs", CP, None),
            P("fs", CP),
            P("fs", CP, None),
            P(CP_FS, None),
            P(CP_FS, None),
            P(CP_FS, None),
            P(CP_FS, None),
        ),
        out_specs=(P(CP_FS, None), P(CP_FS, None), P(CP_FS, None), P(CP_FS, None)),
        check_vma=False,
    )
```

```python
import math
from types import SimpleNamespace

import jax
import jax.numpy as jnp
from jax import lax
from jax.experimental import pallas as pl
from jax.experimental.pallas import tpu as pltpu
from jax.sharding import Mesh
from jax.sharding import PartitionSpec as P

HEAD = 128
KV = 4
WIN = 4
GROUP = 4
TOK = 256
SPAN = (WIN + 1) * TOK
NY, NZ, NX = 4, 8, 4
CP = ("cp_0", "cp_1", "cp_2")
CP_FS = ("cp_0", "cp_1", "cp_2", "fs")

NORM_EPS = 0.01
MOMENT_DECAY = 0.95
LEARN_RATE = 0.005
WEIGHT_DECAY = 0.1
ADAM_EPS = 1e-08
AVERAGE_MIX = 0.25
INTERP_BETA = 0.9
EXP2_SCALE = math.log2(math.e) / math.sqrt(HEAD)
MASKED = -1e30
FAR = 1 << 30

BF = jnp.bfloat16
F32 = jnp.float32
MESH = pl.DeviceIdType.MESH

BUFFERS = {
    "emb": ((TOK, 4096), BF),
    "w": ((NY, NZ, 2, NX, 16, 512), BF),
    "q": ((TOK, 2048), BF),
    "kw": ((5, TOK, 512), BF),
    "vw": ((KV, 5, TOK, HEAD), BF),
    "cot": ((TOK, 2048), BF),
    "p": ((16, TOK, SPAN), BF),
    "s0": ((TOK, SPAN), F32),
    "s1": ((TOK, SPAN), F32),
    "bias": ((TOK, SPAN), F32),
    "att": ((16, TOK, HEAD), F32),
    "sq": ((TOK, HEAD), F32),
    "cr": ((TOK, HEAD), F32),
    "og": ((16, TOK, HEAD), BF),
    "dv": ((KV, 5, TOK, HEAD), F32),
    "r": ((KV, 3, TOK, HEAD), F32),
    "fo": ((KV, TOK, HEAD), BF),
    "fi": ((KV, TOK, HEAD), BF),
    "go": ((KV, TOK, HEAD), BF),
    "gi": ((KV, TOK, HEAD), BF),
    "vg": ((2, 8, TOK, 256), BF),
    "et": ((NY, NZ, 2, NX, 16, TOK), BF),
    "er": ((2, 2, 2, NZ, 16, TOK), BF),
    "ex": ((NY, NZ, 16, 8 * TOK), BF),
    "g": ((2, NY, NZ, 16, 256), F32),
    "g1": ((2, NZ, 16, 256), BF),
    "x1": ((2, 2, 4, 16, 256), BF),
    "tx": ((2, 2, NZ, 16, 256), BF),
    "x2": ((2, 2, NZ, 16, 256), BF),
    "t": ((2, NZ, 16, 256), F32),
    "tz": ((2, NZ, 16, 256), BF),
    "sum": ((2, 16, 256), F32),
    "rz": ((2, NZ, 16, 256), BF),
}
SEMAPHORES = {
    "ld": 8,
    "w1": 1,
    "w2": 1,
    "w3": 8,
    "wd": 1,
    "k": 5,
    "v": 12,
    "e": 2,
    "r": 8,
    "f": 4,
    "g": 4,
    "vg": 12,
    "vd": 4,
    "x": 6,
    "z": 2,
}
SENDERS = tuple(SEMAPHORES) + ("es",)


def kernel(need, doc, emb_h, q_h, k_h, cot_h, yw_h, out, *scratch):
    names = list(BUFFERS)
    b = SimpleNamespace(**dict(zip(names, scratch)))
    rest = scratch[len(names) :]
    rcv, snd = dict(zip(SEMAPHORES, rest)), rest[-1]

    y, z = lax.axis_index("cp_0"), lax.axis_index("cp_1")
    c, x = lax.axis_index("cp_2"), lax.axis_index("fs")
    o = 1 - c
    zn, yn = lax.rem(z + 1, NZ), lax.rem(y + lax.div(z + 1, NZ), NY)
    zp, yp = lax.rem(z + NZ - 1, NZ), lax.rem(y + NY - 1 + lax.div(z + NZ - 1, NZ), NY)
    yup, ydn = lax.rem(y + 1, NY), lax.rem(y + NY - 1, NY)
    xup, xdn = lax.rem(x + 1, NX), lax.rem(x + NX - 1, NX)
    yop, xop = lax.rem(y + 2, NY), lax.rem(x + 2, NX)
    block = (y * NZ + z) * 2 + c

    def dev(cp_0=y, cp_1=z, cp_2=c, fs=x):
        return {"cp_0": cp_0, "cp_1": cp_1, "cp_2": cp_2, "fs": fs}

    sibling = dev(cp_2=o)
    following, preceding = dev(cp_0=yn, cp_1=zn), dev(cp_0=yp, cp_1=zp)

    sent = dict.fromkeys(SENDERS, 0)
    results = []

    def copy(src, dst, kind, k, to, sender=None):
        return pltpu.make_async_remote_copy(
            src_ref=src,
            dst_ref=dst,
            send_sem=snd.at[SENDERS.index(sender or kind)],
            recv_sem=rcv[kind].at[k],
            device_id=to,
            device_id_type=MESH,
        )

    def prepare(src, dst, kind, k, to, sender=None):
        sent[sender or kind] += math.prod(src.shape) * jnp.dtype(src.dtype).itemsize
        return copy(src, dst, kind, k, to, sender)

    def send(*what):
        prepare(*what).start()

    def arrived(dst, kind, k):
        copy(dst, dst, kind, k, sibling).wait_recv()

    def room(size):
        n = size // (1 << 16)
        if size % (1 << 16):
            return b.w.at[0, 0 : size // (1 << 14), 0, 0]
        if n <= 8:
            return b.ex.at[0, 0:n]
        rows = next(a for a in (2, 3, 4) if n % a == 0 and n // a <= 8)
        return b.ex.at[0:rows, 0 : n // rows]

    loads = {}

    def load(name, src, dst):
        loads[name] = pltpu.make_async_copy(src, dst, rcv["ld"].at[len(loads)])
        loads[name].start()

    mine = b.w.at[y, z, c, x]
    load("w", yw_h, mine)
    load("k", k_h, b.kw.at[0])
    load("q", q_h, b.q)
    load("emb", emb_h, b.emb)
    load("cot", cot_h, b.cot)

    barrier = pltpu.get_barrier_semaphore()
    partners = [sibling, following, preceding]
    for d in range(1, NZ):
        partners.append(dev(cp_1=lax.rem(z + d, NZ)))
    for d in range(1, NY):
        partners.append(dev(cp_0=lax.rem(y + d, NY)))
    for d in range(1, NX):
        for cc in (c, o):
            partners.append(dev(fs=lax.rem(x + d, NX), cp_2=cc))
    for who in partners:
        pl.semaphore_signal(barrier, inc=1, device_id=who, device_id_type=MESH)
    pl.semaphore_wait(barrier, len(partners))

    loads["w"].wait()
    for d in range(1, NZ):
        send(mine, mine, "w1", 0, dev(cp_1=lax.rem(z + d, NZ)))

    doc_t = jnp.transpose(jnp.broadcast_to(doc[...], (TOK, TOK)))
    row = lax.broadcasted_iota(jnp.int32, (TOK, TOK), 0) + block * TOK
    col = lax.broadcasted_iota(jnp.int32, (TOK, TOK), 1)
    for d in range(WIN + 1):
        listed = need[0, 0] == block - d
        for k in range(1, WIN + 1):
            listed = jnp.logical_or(listed, need[0, k] == block - d)
        shut = jnp.where(listed, 0, FAR)
        key_pos = col + (block - d) * TOK
        seen = jnp.logical_and(key_pos >= doc_t + shut, key_pos <= row)
        b.bias[:, d * TOK : (d + 1) * TOK] = jnp.where(seen, 0.0, MASKED)
    for kv in range(KV):
        b.r[kv, 2] = jnp.zeros((TOK, HEAD), F32)
    b.sq[...] = jnp.zeros((TOK, HEAD), F32)
    b.cr[...] = jnp.zeros((TOK, HEAD), F32)

    def turn(e, carry):
        lanes = pl.ds(pl.multiple_of(e * 512, 512), 512)
        turned = jnp.transpose(b.emb[:, lanes]).reshape(4, 2, NX, 16, TOK)
        b.et[lax.div(e, 2), pl.ds(4 * lax.rem(e, 2), 4)] = turned
        return carry

    loads["emb"].wait()

    arrived(room(7 << 14), "w1", 0)
    first, second = b.w.at[y, :, c, x, :, 0:256], b.w.at[y, :, c, x, :, 256:512]
    for d in range(1, 4):
        send(first, first, "w2", 0, dev(cp_0=lax.rem(y + d, NY)))
        send(second, second, "w2", 0, dev(fs=lax.rem(x + d, NX)))

    lax.fori_loop(0, 8, turn, 0)

    arrived(room(6 << 16), "w2", 0)

    def half_a(xx):
        return b.w.at[:, :, c, xx, :, 0:256]

    def half_b(yy):
        return b.w.at[yy, :, c, :, :, 256:512]

    def relay_a(xx, s):
        return b.w.at[:, 4 * s : 4 * s + 4, c, xx, :, 0:256]

    def relay_b(yy, s):
        return b.w.at[yy, 4 * s : 4 * s + 4, c, :, :, 256:512]

    send(half_a(x), half_a(x), "w3", 0, dev(fs=xup))
    send(half_a(x), half_a(x), "w3", 1, dev(fs=xdn))
    send(half_b(y), half_b(y), "w3", 2, dev(cp_0=yup))
    send(half_b(y), half_b(y), "w3", 3, dev(cp_0=ydn))

    send(half_a(x), half_a(x), "wd", 0, sibling)
    send(half_b(y), half_b(y), "wd", 0, sibling)

    loads["k"].wait()

    def keys_at(d, s):
        return b.kw.at[d, 128 * s : 128 * s + 128]

    for s in range(2):
        send(keys_at(0, s), keys_at(2, s), "k", s, following)
    keys_on = [
        (
            prepare(keys_at(2, s), keys_at(4, s), "k", 2 + s, following),
            prepare(keys_at(2 * c, s), keys_at(1, s), "k", 4, sibling),
        )
        for s in range(2)
    ]

    def pass_keys():
        for s in range(2):
            arrived(keys_at(2, s), "k", s)
            for made in keys_on[s]:
                made.start()

    arrived(half_a(x), "w3", 0)
    send(relay_a(xdn, 0), relay_a(xdn, 0), "w3", 4, dev(fs=xup))
    arrived(half_a(x), "w3", 1)
    send(relay_a(xup, 1), relay_a(xup, 1), "w3", 5, dev(fs=xdn))
    up_0 = prepare(relay_b(ydn, 0), relay_b(ydn, 0), "w3", 6, dev(cp_0=yup))
    down_0 = copy(relay_b(yup, 0), relay_b(yup, 0), "w3", 6, dev(cp_0=ydn))
    down_1 = prepare(relay_b(yup, 1), relay_b(yup, 1), "w3", 7, dev(cp_0=ydn))

    @pl.when(z != 0)
    def _():
        arrived(half_b(y), "w3", 2)
        up_0.start()
        arrived(half_b(y), "w3", 3)
        down_1.start()

    @pl.when(z == 0)
    def _():
        arrived(half_b(y), "w3", 3)
        down_0.start()
        down_1.start()

    send(half_a(xdn), half_a(xdn), "wd", 0, sibling)
    send(half_a(xup), half_a(xup), "wd", 0, sibling)
    send(half_b(yup), half_b(yup), "wd", 0, sibling)

    behind = prepare(half_b(ydn), half_b(ydn), "wd", 0, sibling)

    @pl.when(z != 0)
    def _():
        behind.start()

    @pl.when(z != NZ - 1)
    def _():
        pass_keys()

    loads["q"].wait()
    for s in range(2):
        arrived(relay_a(x, s), "w3", 4 + s)
        send(relay_a(xop, s), relay_a(xop, s), "wd", 0, sibling)

    @pl.when(z == NZ - 1)
    def _():
        pass_keys()

    for s in range(2):
        arrived(relay_b(y, s), "w3", 6 + s)
        send(relay_b(yop, s), relay_b(yop, s), "wd", 0, sibling)

    @pl.when(z == 0)
    def _():
        arrived(half_b(y), "w3", 2)
        behind.start()

    def scores(hd, into):
        lanes = pl.ds(pl.multiple_of(hd * HEAD, HEAD), HEAD)
        key_lanes = pl.ds(pl.multiple_of(lax.div(hd, GROUP) * HEAD, HEAD), HEAD)
        keys = b.kw[:, :, key_lanes].reshape(SPAN, HEAD)
        into[...] = lax.dot_general(
            b.q[:, lanes], keys, (((1,), (1,)), ((), ())), preferred_element_type=F32
        )

    def softmax(hd, held):
        for n in range(8):
            rows = slice(n * 32, n * 32 + 32)
            score = held[rows, :] + b.bias[rows, :]
            largest = jnp.max(score, axis=-1, keepdims=True)
            weight = jnp.exp2((score - largest) * EXP2_SCALE)
            total = jnp.sum(weight, axis=-1, keepdims=True)
            b.p[hd, rows, :] = (weight * (1.0 / total)).astype(BF)

    def head_probs(pair, carry):
        scores(2 * pair + 1, b.s1)
        softmax(2 * pair, b.s0)
        scores(jnp.minimum(2 * pair + 2, 15), b.s0)
        softmax(2 * pair + 1, b.s1)
        return carry

    arrived(room(32 << 16), "wd", 0)

    def tokens_of(slot, ys=slice(None)):
        return b.ex.at[ys, :, :, slot * TOK : slot * TOK + TOK]

    kept = pltpu.make_async_copy(b.et.at[:, :, c, x], tokens_of(0), rcv["ld"].at[7])
    kept.start()
    send(b.et.at[:, :, o, x], tokens_of(1), "e", 0, sibling, "es")
    for s, xt in enumerate((xup, xdn)):
        for k, cc in enumerate((c, o)):
            part = b.et.at[2 * s : 2 * s + 2, :, cc, xop]
            send(part, b.er.at[s, k], "e", 1, dev(fs=xt))
    for s, xt in enumerate((xup, xdn)):
        for k, cc in enumerate((c, o)):
            there = tokens_of(2 + 2 * s + k)
            send(b.et.at[:, :, cc, xt], there, "e", 0, dev(fs=xt, cp_2=cc))

    def pass_embeds():
        arrived(b.er, "e", 1)
        for s, xt in enumerate((xup, xdn)):
            for k, cc in enumerate((c, o)):
                there = tokens_of(6 + k, slice(2 * s, 2 * s + 2))
                send(b.er.at[s, k], there, "e", 0, dev(fs=xt, cp_2=cc))

    made = jnp.dot(b.emb[...], b.w[...].reshape(4096, 512), preferred_element_type=F32)
    for kv in range(KV):
        b.vw[kv, 0] = made[:, kv * HEAD : (kv + 1) * HEAD].astype(BF)
        send(b.vw.at[kv, 0], b.vw.at[kv, 2], "v", kv, following)

    def pass_near(kv):
        arrived(b.vw.at[kv, 2], "v", kv)
        send(b.vw.at[kv, 2], b.vw.at[kv, 4], "v", 4 + kv, following)
        send(b.vw.at[kv, 2 * c], b.vw.at[kv, 1], "v", 8 + kv, sibling)

    def pass_far(kv):
        arrived(b.vw.at[kv, 4], "v", 4 + kv)
        send(b.vw.at[kv, 2 + 2 * c], b.vw.at[kv, 3], "v", 8 + kv, sibling)

    def attend(kv):
        arrived(b.vw.at[kv, 0:2], "v", 8 + kv)

        for hd in range(kv * GROUP, kv * GROUP + GROUP):
            values = b.vw[kv].reshape(SPAN, HEAD)
            b.att[hd] = jnp.dot(b.p[hd], values, preferred_element_type=F32)
        for hd in range(kv * GROUP, kv * GROUP + GROUP):
            lanes = slice(hd * HEAD, hd * HEAD + HEAD)
            b.sq[...] += b.att[hd] * b.att[hd]
            b.cr[...] += b.att[hd] * b.cot[:, lanes].astype(F32)

    for s in range(2):
        arrived(keys_at(4, s), "k", 2 + s)
        send(keys_at(2 + 2 * c, s), keys_at(3, s), "k", 4, sibling)

    arrived(room(8 << 16), "k", 4)
    loads["cot"].wait()
    scores(0, b.s0)
    lax.fori_loop(0, 3, head_probs, 0)
    pass_near(0)
    lax.fori_loop(3, 4, head_probs, 0)
    pass_near(1)
    lax.fori_loop(4, 5, head_probs, 0)
    pass_near(2)
    lax.fori_loop(5, 6, head_probs, 0)
    pass_near(3)
    pass_embeds()
    lax.fori_loop(6, 7, head_probs, 0)
    pass_far(0)
    lax.fori_loop(7, 8, head_probs, 0)
    pass_far(1)
    attend(0)
    pass_far(2)
    attend(1)
    pass_far(3)
    attend(2)
    attend(3)

    token_total = TOK * NY * NZ * 2 * NX
    mean = jnp.sum(b.sq[...], axis=-1, keepdims=True) * (1.0 / 2048.0) + NORM_EPS
    inv = 1.0 / jnp.sqrt(mean)
    inner = jnp.sum(b.cr[...], axis=-1, keepdims=True) * (1.0 / (2048.0 * token_total)) * inv
    b.cr[...] = jnp.broadcast_to(inner * inv, (TOK, HEAD))
    b.sq[...] = jnp.broadcast_to(inv, (TOK, HEAD))

    def norm_grads(kv):
        for hd in range(kv * GROUP, kv * GROUP + GROUP):
            up = b.cot[:, hd * HEAD : (hd + 1) * HEAD].astype(F32) * (1.0 / token_total)
            b.og[hd] = ((up - b.att[hd] * b.cr[...]) * b.sq[...]).astype(BF)

    def grads(kv, low, high):
        up = b.og[kv * GROUP : kv * GROUP + GROUP].reshape(GROUP * TOK, HEAD)
        for d in range(low, high):
            lanes = slice(d * TOK, d * TOK + TOK)
            part = b.p[kv * GROUP : kv * GROUP + GROUP, :, lanes].reshape(GROUP * TOK, TOK)
            b.dv[kv, d] = lax.dot_general(
                part, up, (((0,), (0,)), ((), ())), preferred_element_type=F32
            )

    def grads_far(kv):
        norm_grads(kv)
        grads(kv, 3, 5)
        send(b.dv.at[kv, 3], b.r.at[kv, 1], "r", 2 * kv + 1, sibling)

    def grads_near(kv):
        grads(kv, 1, 3)
        send(b.dv.at[kv, 1], b.r.at[kv, 0], "r", 2 * kv, sibling)

    def leave_far(kv):
        arrived(b.r.at[kv, 1], "r", 2 * kv + 1)
        b.fo[kv] = (b.dv[kv, 4] + b.r[kv, 2 - c]).astype(BF)
        send(b.fo.at[kv], b.fi.at[kv], "f", kv, preceding)

    def leave_near(kv):
        arrived(b.r.at[kv, 0], "r", 2 * kv)
        arrived(b.fi.at[kv], "f", kv)
        b.go[kv] = (b.dv[kv, 2] + b.r[kv, 1 - c] + b.fi[kv].astype(F32)).astype(BF)
        send(b.go.at[kv], b.gi.at[kv], "g", kv, preceding)

    def vg_at(kv, slot, rows=slice(None)):
        lanes = slice((kv % 2) * HEAD, (kv % 2) * HEAD + HEAD)
        return b.vg.at[kv // 2, slot, rows, lanes]

    upper, lower = slice(0, 128), slice(128, 256)

    def settle(kv):
        arrived(b.gi.at[kv], "g", kv)
        total = b.dv[kv, 0] + b.r[kv, 2 * c] + b.gi[kv].astype(F32)
        b.vg[kv // 2, 0, :, (kv % 2) * HEAD : (kv % 2) * HEAD + HEAD] = total.astype(BF)
        send(vg_at(kv, 0), vg_at(kv, 2), "vg", 3 * kv, dev(fs=xup))
        send(vg_at(kv, 0), vg_at(kv, 4), "vg", 3 * kv + 1, dev(fs=xdn))
        send(vg_at(kv, 0), vg_at(kv, 1), "vd", kv // 2, sibling)

    def relay(kv):
        arrived(vg_at(kv, 2), "vg", 3 * kv)
        send(vg_at(kv, 2, upper), vg_at(kv, 6, upper), "vg", 3 * kv + 2, dev(fs=xup))
        send(vg_at(kv, 2), vg_at(kv, 3), "vd", kv // 2, sibling)
        arrived(vg_at(kv, 4), "vg", 3 * kv + 1)
        send(vg_at(kv, 4, lower), vg_at(kv, 6, lower), "vg", 3 * kv + 2, dev(fs=xdn))
        send(vg_at(kv, 4), vg_at(kv, 5), "vd", kv // 2, sibling)

    def collect(kv):
        arrived(vg_at(kv, 6), "vg", 3 * kv + 2)
        send(vg_at(kv, 6), vg_at(kv, 7), "vd", 2 + kv // 2, sibling)

    grads_far(0)
    grads_far(1)
    leave_far(0)
    grads_far(2)
    leave_far(1)
    grads_far(3)
    leave_far(2)
    grads_near(0)
    leave_far(3)
    grads_near(1)
    grads_near(2)
    leave_near(0)
    grads_near(3)
    leave_near(1)
    grads(0, 0, 1)
    grads(1, 0, 1)
    leave_near(2)
    grads(2, 0, 1)
    grads(3, 0, 1)
    leave_near(3)
    kept.wait()
    arrived(room(28 << 16), "e", 0)

    for kv in range(KV):
        settle(kv)
    for kv in range(KV):
        relay(kv)

    def early(h):
        arrived(room(6 << 16), "vd", h)
        for ys in (slice(0, 2), slice(2, 4)):
            b.g[h, ys] = jnp.dot(
                b.ex[ys, :, :, 0 : 6 * TOK].reshape(256, 6 * TOK),
                b.vg[h, 0:6].reshape(6 * TOK, 256),
                preferred_element_type=F32,
            ).reshape(2, NZ, 16, 256)

    def product(h):
        arrived(room(2 << 16), "vd", 2 + h)
        for ys in (slice(0, 2), slice(2, 4)):
            b.g[h, ys] += jnp.dot(
                b.ex[ys, :, :, 6 * TOK : 8 * TOK].reshape(256, 2 * TOK),
                b.vg[h, 6:8].reshape(2 * TOK, 256),
                preferred_element_type=F32,
            ).reshape(2, NZ, 16, 256)
        b.g1[h] = b.g[h, yop].astype(BF)
        send(b.g1.at[h, 0:4], b.x1.at[h, 0], "x", 3 * h, dev(cp_0=yup))
        send(b.g1.at[h, 4:8], b.x1.at[h, 1], "x", 3 * h + 1, dev(cp_0=ydn))

    def across(h):
        arrived(b.x1.at[h, 0], "x", 3 * h)
        b.tx[h, 0, 0:4] = (b.g[h, yup, 0:4] + b.x1[h, 0].astype(F32)).astype(BF)
        b.tx[h, 0, 4:8] = b.g[h, yup, 4:8].astype(BF)
        send(b.tx.at[h, 0], b.x2.at[h, 0], "x", 3 * h + 2, dev(cp_0=yup))
        arrived(b.x1.at[h, 1], "x", 3 * h + 1)
        b.tx[h, 1, 0:4] = b.g[h, ydn, 0:4].astype(BF)
        b.tx[h, 1, 4:8] = (b.g[h, ydn, 4:8] + b.x1[h, 1].astype(F32)).astype(BF)
        send(b.tx.at[h, 1], b.x2.at[h, 1], "x", 3 * h + 2, dev(cp_0=ydn))

    def along(h):
        arrived(b.x2.at[h], "x", 3 * h + 2)
        b.t[h] = b.g[h, y] + b.x2[h, 0].astype(F32) + b.x2[h, 1].astype(F32)
        b.tz[h] = b.t[h].astype(BF)
        for d in (4, 3, 5, 2, 6, 1, 7):
            zt = lax.rem(z + d, NZ)
            send(b.tz.at[h, zt], b.rz.at[h, z], "z", h, dev(cp_1=zt))

    def finish(h):
        arrived(b.rz.at[h, 0:7], "z", h)
        total = b.t[h, z]
        for d in range(1, NZ):
            total = total + b.rz[h, lax.rem(z + d, NZ)].astype(F32)
        out[:, h * 256 : (h + 1) * 256] = total

    early(0)
    collect(0)
    collect(1)
    early(1)
    collect(2)
    product(0)
    collect(3)
    product(1)
    across(0)
    across(1)
    along(0)
    along(1)
    finish(0)
    finish(1)

    for kind, size in sent.items():
        if size:
            copy(room(size), room(size), "w1", 0, sibling, kind).wait_send()


def weight_gradient(need_ids, doc_start, embeds, queries, key_heads, cotangent, y_weight):
    any_space = pl.BlockSpec(memory_space=pl.ANY)
    vmem = pl.BlockSpec(memory_space=pltpu.VMEM)
    semaphores = [pltpu.SemaphoreType.DMA((n,)) for n in SEMAPHORES.values()]
    semaphores.append(pltpu.SemaphoreType.DMA((len(SENDERS),)))
    return pl.pallas_call(
        kernel,
        out_shape=pltpu.VMEM((16, 512), F32),
        in_specs=[pl.BlockSpec(memory_space=pltpu.SMEM), vmem] + [any_space] * 5,
        out_specs=vmem,
        scratch_shapes=[pltpu.VMEM(shape, kind) for shape, kind in BUFFERS.values()]
        + semaphores,
        compiler_params=pltpu.CompilerParams(
            collective_id=0, has_side_effects=True, vmem_limit_bytes=58 << 20
        ),
    )(need_ids, doc_start, embeds, queries, key_heads, cotangent, y_weight)


def on_device(
    embeds,
    queries,
    key_heads,
    cotangent,
    doc_start,
    need_ids,
    y_weight,
    z_weight,
    x_weight,
    second_moment,
):
    gradient = weight_gradient(
        need_ids[0], doc_start, embeds[0], queries[0], key_heads[0], cotangent[0], y_weight
    )
    moment_next = MOMENT_DECAY * second_moment + (1.0 - MOMENT_DECAY) * gradient * gradient
    z_next = z_weight - LEARN_RATE * (
        gradient / (jnp.sqrt(moment_next) + ADAM_EPS) + WEIGHT_DECAY * y_weight.astype(jnp.float32)
    )
    x_next = (1.0 - AVERAGE_MIX) * x_weight + AVERAGE_MIX * z_next
    y_next = ((1.0 - INTERP_BETA) * z_next + INTERP_BETA * x_next).astype(jnp.bfloat16)
    return (z_next, x_next, moment_next, y_next)


def solution(mesh):
    finer = Mesh(mesh.devices.reshape(NY, NZ, 2, mesh.shape["fs"]), CP_FS)
    return jax.shard_map(
        on_device,
        mesh=finer,
        in_specs=(
            P("fs", CP, None),
            P("fs", CP, None),
            P("fs", CP, None),
            P("fs", CP, None),
            P("fs", CP),
            P("fs", CP, None),
            P(CP_FS, None),
            P(CP_FS, None),
            P(CP_FS, None),
            P(CP_FS, None),
        ),
        out_specs=(P(CP_FS, None), P(CP_FS, None), P(CP_FS, None), P(CP_FS, None)),
        check_vma=False,
    )
```

```python
import math
from types import SimpleNamespace

import jax
import jax.numpy as jnp
from jax import lax
from jax.experimental import pallas as pl
from jax.experimental.pallas import tpu as pltpu
from jax.sharding import Mesh
from jax.sharding import PartitionSpec as P

HEAD = 128
KV = 4
WIN = 4
GROUP = 4
TOK = 256
SPAN = (WIN + 1) * TOK
NY, NZ, NX = 4, 8, 4
CP = ("cp_0", "cp_1", "cp_2")
CP_FS = ("cp_0", "cp_1", "cp_2", "fs")

NORM_EPS = 0.01
MOMENT_DECAY = 0.95
LEARN_RATE = 0.005
WEIGHT_DECAY = 0.1
ADAM_EPS = 1e-08
AVERAGE_MIX = 0.25
INTERP_BETA = 0.9
EXP2_SCALE = math.log2(math.e) / math.sqrt(HEAD)
MASKED = -1e30
FAR = 1 << 30

BF = jnp.bfloat16
F32 = jnp.float32
MESH = pl.DeviceIdType.MESH

BUFFERS = {
    "emb": ((TOK, 4096), BF),
    "w": ((NY, NZ, 2, NX, 16, 512), BF),
    "q": ((TOK, 2048), BF),
    "kw": ((5, TOK, 512), BF),
    "vw": ((KV, 5, TOK, HEAD), BF),
    "cot": ((TOK, 2048), BF),
    "p": ((16, TOK, SPAN), BF),
    "s0": ((TOK, SPAN), F32),
    "s1": ((TOK, SPAN), F32),
    "bias": ((TOK, SPAN), F32),
    "att": ((16, TOK, HEAD), F32),
    "sq": ((TOK, HEAD), F32),
    "cr": ((TOK, HEAD), F32),
    "og": ((16, TOK, HEAD), BF),
    "dv": ((KV, 5, TOK, HEAD), F32),
    "r": ((KV, 3, TOK, HEAD), F32),
    "fo": ((KV, TOK, HEAD), BF),
    "fi": ((KV, TOK, HEAD), BF),
    "go": ((KV, TOK, HEAD), BF),
    "gi": ((KV, TOK, HEAD), BF),
    "vg": ((2, 8, TOK, 256), BF),
    "et": ((NY, NZ, 2, NX, 16, TOK), BF),
    "er": ((2, 2, 2, NZ, 16, TOK), BF),
    "ex": ((NY, NZ, 16, 8 * TOK), BF),
    "g": ((2, NY, NZ, 16, 256), F32),
    "g1": ((2, NZ, 16, 256), BF),
    "x1": ((2, 2, 4, 16, 256), BF),
    "tx": ((2, 2, NZ, 16, 256), BF),
    "x2": ((2, 2, NZ, 16, 256), BF),
    "t": ((2, NZ, 16, 256), F32),
    "tz": ((2, NZ, 16, 256), BF),
    "sum": ((2, 16, 256), F32),
    "rz": ((2, NZ, 16, 256), BF),
}
SEMAPHORES = {
    "ld": 8,
    "w1": 1,
    "w2": 1,
    "w3": 8,
    "wd": 1,
    "k": 5,
    "v": 12,
    "e": 2,
    "r": 8,
    "f": 4,
    "g": 4,
    "vg": 12,
    "vd": 4,
    "x": 6,
    "z": 2,
}
SENDERS = tuple(SEMAPHORES) + ("es",)


def kernel(need, doc, emb_h, q_h, k_h, cot_h, yw_h, out, *scratch):
    names = list(BUFFERS)
    b = SimpleNamespace(**dict(zip(names, scratch)))
    rest = scratch[len(names) :]
    rcv, snd = dict(zip(SEMAPHORES, rest)), rest[-1]

    y, z = lax.axis_index("cp_0"), lax.axis_index("cp_1")
    c, x = lax.axis_index("cp_2"), lax.axis_index("fs")
    o = 1 - c
    zn, yn = lax.rem(z + 1, NZ), lax.rem(y + lax.div(z + 1, NZ), NY)
    zp, yp = lax.rem(z + NZ - 1, NZ), lax.rem(y + NY - 1 + lax.div(z + NZ - 1, NZ), NY)
    yup, ydn = lax.rem(y + 1, NY), lax.rem(y + NY - 1, NY)
    xup, xdn = lax.rem(x + 1, NX), lax.rem(x + NX - 1, NX)
    yop, xop = lax.rem(y + 2, NY), lax.rem(x + 2, NX)
    block = (y * NZ + z) * 2 + c

    def dev(cp_0=y, cp_1=z, cp_2=c, fs=x):
        return {"cp_0": cp_0, "cp_1": cp_1, "cp_2": cp_2, "fs": fs}

    sibling = dev(cp_2=o)
    following, preceding = dev(cp_0=yn, cp_1=zn), dev(cp_0=yp, cp_1=zp)

    sent = dict.fromkeys(SENDERS, 0)
    results = []

    def copy(src, dst, kind, k, to, sender=None):
        return pltpu.make_async_remote_copy(
            src_ref=src,
            dst_ref=dst,
            send_sem=snd.at[SENDERS.index(sender or kind)],
            recv_sem=rcv[kind].at[k],
            device_id=to,
            device_id_type=MESH,
        )

    def prepare(src, dst, kind, k, to, sender=None):
        sent[sender or kind] += math.prod(src.shape) * jnp.dtype(src.dtype).itemsize
        return copy(src, dst, kind, k, to, sender)

    def send(*what):
        prepare(*what).start()

    def arrived(dst, kind, k):
        copy(dst, dst, kind, k, sibling).wait_recv()

    def room(size):
        n = size // (1 << 16)
        if size % (1 << 16):
            return b.w.at[0, 0 : size // (1 << 14), 0, 0]
        if n <= 8:
            return b.ex.at[0, 0:n]
        rows = next(a for a in (2, 3, 4) if n % a == 0 and n // a <= 8)
        return b.ex.at[0:rows, 0 : n // rows]

    loads = {}

    def load(name, src, dst):
        loads[name] = pltpu.make_async_copy(src, dst, rcv["ld"].at[len(loads)])
        loads[name].start()

    mine = b.w.at[y, z, c, x]
    load("w", yw_h, mine)
    load("k", k_h, b.kw.at[0])
    load("q", q_h, b.q)
    load("emb", emb_h, b.emb)
    load("cot", cot_h, b.cot)

    barrier = pltpu.get_barrier_semaphore()
    partners = [sibling, following, preceding]
    for d in range(1, NZ):
        partners.append(dev(cp_1=lax.rem(z + d, NZ)))
    for d in range(1, NY):
        partners.append(dev(cp_0=lax.rem(y + d, NY)))
    for d in range(1, NX):
        for cc in (c, o):
            partners.append(dev(fs=lax.rem(x + d, NX), cp_2=cc))
    for who in partners:
        pl.semaphore_signal(barrier, inc=1, device_id=who, device_id_type=MESH)
    pl.semaphore_wait(barrier, len(partners))

    loads["w"].wait()
    for d in range(1, NZ):
        send(mine, mine, "w1", 0, dev(cp_1=lax.rem(z + d, NZ)))

    doc_t = jnp.transpose(jnp.broadcast_to(doc[...], (TOK, TOK)))
    row = lax.broadcasted_iota(jnp.int32, (TOK, TOK), 0) + block * TOK
    col = lax.broadcasted_iota(jnp.int32, (TOK, TOK), 1)
    for d in range(WIN + 1):
        listed = need[0, 0] == block - d
        for k in range(1, WIN + 1):
            listed = jnp.logical_or(listed, need[0, k] == block - d)
        shut = jnp.where(listed, 0, FAR)
        key_pos = col + (block - d) * TOK
        seen = jnp.logical_and(key_pos >= doc_t + shut, key_pos <= row)
        b.bias[:, d * TOK : (d + 1) * TOK] = jnp.where(seen, 0.0, MASKED)
    for kv in range(KV):
        b.r[kv, 2] = jnp.zeros((TOK, HEAD), F32)
    b.sq[...] = jnp.zeros((TOK, HEAD), F32)
    b.cr[...] = jnp.zeros((TOK, HEAD), F32)

    def turn(e, carry):
        lanes = pl.ds(pl.multiple_of(e * 512, 512), 512)
        turned = jnp.transpose(b.emb[:, lanes]).reshape(4, 2, NX, 16, TOK)
        b.et[lax.div(e, 2), pl.ds(4 * lax.rem(e, 2), 4)] = turned
        return carry

    loads["emb"].wait()

    arrived(room(7 << 14), "w1", 0)
    first, second = b.w.at[y, :, c, x, :, 0:256], b.w.at[y, :, c, x, :, 256:512]
    for d in range(1, 4):
        send(first, first, "w2", 0, dev(cp_0=lax.rem(y + d, NY)))
        send(second, second, "w2", 0, dev(fs=lax.rem(x + d, NX)))

    lax.fori_loop(0, 8, turn, 0)

    arrived(room(6 << 16), "w2", 0)

    def half_a(xx):
        return b.w.at[:, :, c, xx, :, 0:256]

    def half_b(yy):
        return b.w.at[yy, :, c, :, :, 256:512]

    def relay_a(xx, s):
        return b.w.at[:, 4 * s : 4 * s + 4, c, xx, :, 0:256]

    def relay_b(yy, s):
        return b.w.at[yy, 4 * s : 4 * s + 4, c, :, :, 256:512]

    send(half_a(x), half_a(x), "w3", 0, dev(fs=xup))
    send(half_a(x), half_a(x), "w3", 1, dev(fs=xdn))
    send(half_b(y), half_b(y), "w3", 2, dev(cp_0=yup))
    send(half_b(y), half_b(y), "w3", 3, dev(cp_0=ydn))

    send(half_a(x), half_a(x), "wd", 0, sibling)
    send(half_b(y), half_b(y), "wd", 0, sibling)

    loads["k"].wait()

    def keys_at(d, s):
        return b.kw.at[d, 128 * s : 128 * s + 128]

    for s in range(2):
        send(keys_at(0, s), keys_at(2, s), "k", s, following)
    keys_on = [
        (
            prepare(keys_at(2, s), keys_at(4, s), "k", 2 + s, following),
            prepare(keys_at(2 * c, s), keys_at(1, s), "k", 4, sibling),
        )
        for s in range(2)
    ]

    def pass_keys():
        for s in range(2):
            arrived(keys_at(2, s), "k", s)
            for made in keys_on[s]:
                made.start()

    arrived(half_a(x), "w3", 0)
    send(relay_a(xdn, 0), relay_a(xdn, 0), "w3", 4, dev(fs=xup))
    arrived(half_a(x), "w3", 1)
    send(relay_a(xup, 1), relay_a(xup, 1), "w3", 5, dev(fs=xdn))
    up_0 = prepare(relay_b(ydn, 0), relay_b(ydn, 0), "w3", 6, dev(cp_0=yup))
    down_0 = copy(relay_b(yup, 0), relay_b(yup, 0), "w3", 6, dev(cp_0=ydn))
    down_1 = prepare(relay_b(yup, 1), relay_b(yup, 1), "w3", 7, dev(cp_0=ydn))

    @pl.when(z != 0)
    def _():
        arrived(half_b(y), "w3", 2)
        up_0.start()
        arrived(half_b(y), "w3", 3)
        down_1.start()

    @pl.when(z == 0)
    def _():
        arrived(half_b(y), "w3", 3)
        down_0.start()
        down_1.start()

    send(half_a(xdn), half_a(xdn), "wd", 0, sibling)
    send(half_a(xup), half_a(xup), "wd", 0, sibling)
    send(half_b(yup), half_b(yup), "wd", 0, sibling)

    behind = prepare(half_b(ydn), half_b(ydn), "wd", 0, sibling)

    @pl.when(z != 0)
    def _():
        behind.start()

    @pl.when(z != NZ - 1)
    def _():
        pass_keys()

    loads["q"].wait()
    for s in range(2):
        arrived(relay_a(x, s), "w3", 4 + s)
        send(relay_a(xop, s), relay_a(xop, s), "wd", 0, sibling)

    @pl.when(z == NZ - 1)
    def _():
        pass_keys()

    for s in range(2):
        arrived(relay_b(y, s), "w3", 6 + s)
        send(relay_b(yop, s), relay_b(yop, s), "wd", 0, sibling)

    @pl.when(z == 0)
    def _():
        arrived(half_b(y), "w3", 2)
        behind.start()

    def scores(hd, into):
        lanes = pl.ds(pl.multiple_of(hd * HEAD, HEAD), HEAD)
        key_lanes = pl.ds(pl.multiple_of(lax.div(hd, GROUP) * HEAD, HEAD), HEAD)
        keys = b.kw[:, :, key_lanes].reshape(SPAN, HEAD)
        into[...] = lax.dot_general(
            b.q[:, lanes], keys, (((1,), (1,)), ((), ())), preferred_element_type=F32
        )

    def softmax(hd, held):
        for n in range(8):
            rows = slice(n * 32, n * 32 + 32)
            score = held[rows, :] + b.bias[rows, :]
            largest = jnp.max(score, axis=-1, keepdims=True)
            weight = jnp.exp2((score - largest) * EXP2_SCALE)
            total = jnp.sum(weight, axis=-1, keepdims=True)
            b.p[hd, rows, :] = (weight * (1.0 / total)).astype(BF)

    def head_probs(pair, carry):
        scores(2 * pair + 1, b.s1)
        softmax(2 * pair, b.s0)
        scores(jnp.minimum(2 * pair + 2, 15), b.s0)
        softmax(2 * pair + 1, b.s1)
        return carry

    arrived(room(32 << 16), "wd", 0)

    def tokens_of(slot, ys=slice(None)):
        return b.ex.at[ys, :, :, slot * TOK : slot * TOK + TOK]

    kept = pltpu.make_async_copy(b.et.at[:, :, c, x], tokens_of(0), rcv["ld"].at[7])
    kept.start()
    send(b.et.at[:, :, o, x], tokens_of(1), "e", 0, sibling, "es")
    for s, xt in enumerate((xup, xdn)):
        for k, cc in enumerate((c, o)):
            part = b.et.at[2 * s : 2 * s + 2, :, cc, xop]
            send(part, b.er.at[s, k], "e", 1, dev(fs=xt))
    for s, xt in enumerate((xup, xdn)):
        for k, cc in enumerate((c, o)):
            there = tokens_of(2 + 2 * s + k)
            send(b.et.at[:, :, cc, xt], there, "e", 0, dev(fs=xt, cp_2=cc))

    def pass_embeds():
        arrived(b.er, "e", 1)
        for s, xt in enumerate((xup, xdn)):
            for k, cc in enumerate((c, o)):
                there = tokens_of(6 + k, slice(2 * s, 2 * s + 2))
                send(b.er.at[s, k], there, "e", 0, dev(fs=xt, cp_2=cc))

    made = jnp.dot(b.emb[...], b.w[...].reshape(4096, 512), preferred_element_type=F32)
    for kv in range(KV):
        b.vw[kv, 0] = made[:, kv * HEAD : (kv + 1) * HEAD].astype(BF)
        send(b.vw.at[kv, 0], b.vw.at[kv, 2], "v", kv, following)

    def pass_near(kv):
        arrived(b.vw.at[kv, 2], "v", kv)
        send(b.vw.at[kv, 2], b.vw.at[kv, 4], "v", 4 + kv, following)
        send(b.vw.at[kv, 2 * c], b.vw.at[kv, 1], "v", 8 + kv, sibling)

    def pass_far(kv):
        arrived(b.vw.at[kv, 4], "v", 4 + kv)
        send(b.vw.at[kv, 2 + 2 * c], b.vw.at[kv, 3], "v", 8 + kv, sibling)

    def attend(kv):
        arrived(b.vw.at[kv, 0:2], "v", 8 + kv)

        for hd in range(kv * GROUP, kv * GROUP + GROUP):
            values = b.vw[kv].reshape(SPAN, HEAD)
            b.att[hd] = jnp.dot(b.p[hd], values, preferred_element_type=F32)
        for hd in range(kv * GROUP, kv * GROUP + GROUP):
            lanes = slice(hd * HEAD, hd * HEAD + HEAD)
            b.sq[...] += b.att[hd] * b.att[hd]
            b.cr[...] += b.att[hd] * b.cot[:, lanes].astype(F32)

    for s in range(2):
        arrived(keys_at(4, s), "k", 2 + s)
        send(keys_at(2 + 2 * c, s), keys_at(3, s), "k", 4, sibling)

    arrived(room(8 << 16), "k", 4)
    loads["cot"].wait()
    scores(0, b.s0)
    lax.fori_loop(0, 3, head_probs, 0)
    pass_near(0)
    lax.fori_loop(3, 4, head_probs, 0)
    pass_near(1)
    lax.fori_loop(4, 5, head_probs, 0)
    pass_near(2)
    lax.fori_loop(5, 6, head_probs, 0)
    pass_near(3)
    pass_embeds()
    lax.fori_loop(6, 7, head_probs, 0)
    pass_far(0)
    lax.fori_loop(7, 8, head_probs, 0)
    pass_far(1)
    attend(0)
    pass_far(2)
    attend(1)
    pass_far(3)
    attend(2)
    attend(3)

    token_total = TOK * NY * NZ * 2 * NX
    mean = jnp.sum(b.sq[...], axis=-1, keepdims=True) * (1.0 / 2048.0) + NORM_EPS
    inv = 1.0 / jnp.sqrt(mean)
    inner = jnp.sum(b.cr[...], axis=-1, keepdims=True) * (1.0 / (2048.0 * token_total)) * inv
    b.cr[...] = jnp.broadcast_to(inner * inv, (TOK, HEAD))
    b.sq[...] = jnp.broadcast_to(inv, (TOK, HEAD))

    def norm_grads(kv):
        for hd in range(kv * GROUP, kv * GROUP + GROUP):
            up = b.cot[:, hd * HEAD : (hd + 1) * HEAD].astype(F32) * (1.0 / token_total)
            b.og[hd] = ((up - b.att[hd] * b.cr[...]) * b.sq[...]).astype(BF)

    def grads(kv, low, high):
        up = b.og[kv * GROUP : kv * GROUP + GROUP].reshape(GROUP * TOK, HEAD)
        for d in range(low, high):
            lanes = slice(d * TOK, d * TOK + TOK)
            part = b.p[kv * GROUP : kv * GROUP + GROUP, :, lanes].reshape(GROUP * TOK, TOK)
            b.dv[kv, d] = lax.dot_general(
                part, up, (((0,), (0,)), ((), ())), preferred_element_type=F32
            )

    def grads_far(kv):
        norm_grads(kv)
        grads(kv, 3, 5)
        send(b.dv.at[kv, 3], b.r.at[kv, 1], "r", 2 * kv + 1, sibling)

    def grads_near(kv):
        grads(kv, 1, 3)
        send(b.dv.at[kv, 1], b.r.at[kv, 0], "r", 2 * kv, sibling)

    def leave_far(kv):
        arrived(b.r.at[kv, 1], "r", 2 * kv + 1)
        b.fo[kv] = (b.dv[kv, 4] + b.r[kv, 2 - c]).astype(BF)
        send(b.fo.at[kv], b.fi.at[kv], "f", kv, preceding)

    def leave_near(kv):
        arrived(b.r.at[kv, 0], "r", 2 * kv)
        arrived(b.fi.at[kv], "f", kv)
        b.go[kv] = (b.dv[kv, 2] + b.r[kv, 1 - c] + b.fi[kv].astype(F32)).astype(BF)
        send(b.go.at[kv], b.gi.at[kv], "g", kv, preceding)

    def vg_at(kv, slot, rows=slice(None)):
        lanes = slice((kv % 2) * HEAD, (kv % 2) * HEAD + HEAD)
        return b.vg.at[kv // 2, slot, rows, lanes]

    upper, lower = slice(0, 128), slice(128, 256)

    def settle(kv):
        arrived(b.gi.at[kv], "g", kv)
        total = b.dv[kv, 0] + b.r[kv, 2 * c] + b.gi[kv].astype(F32)
        b.vg[kv // 2, 0, :, (kv % 2) * HEAD : (kv % 2) * HEAD + HEAD] = total.astype(BF)
        send(vg_at(kv, 0), vg_at(kv, 2), "vg", 3 * kv, dev(fs=xup))
        send(vg_at(kv, 0), vg_at(kv, 4), "vg", 3 * kv + 1, dev(fs=xdn))
        send(vg_at(kv, 0), vg_at(kv, 1), "vd", kv // 2, sibling)

    def relay(kv):
        arrived(vg_at(kv, 2), "vg", 3 * kv)
        send(vg_at(kv, 2, upper), vg_at(kv, 6, upper), "vg", 3 * kv + 2, dev(fs=xup))
        send(vg_at(kv, 2), vg_at(kv, 3), "vd", kv // 2, sibling)
        arrived(vg_at(kv, 4), "vg", 3 * kv + 1)
        send(vg_at(kv, 4, lower), vg_at(kv, 6, lower), "vg", 3 * kv + 2, dev(fs=xdn))
        send(vg_at(kv, 4), vg_at(kv, 5), "vd", kv // 2, sibling)

    def collect(kv):
        arrived(vg_at(kv, 6), "vg", 3 * kv + 2)
        send(vg_at(kv, 6), vg_at(kv, 7), "vd", 2 + kv // 2, sibling)

    grads_far(0)
    grads_far(1)
    leave_far(0)
    grads_far(2)
    leave_far(1)
    grads_far(3)
    leave_far(2)
    grads_near(0)
    leave_far(3)
    grads_near(1)
    grads_near(2)
    leave_near(0)
    grads_near(3)
    leave_near(1)
    grads(0, 0, 1)
    grads(1, 0, 1)
    leave_near(2)
    grads(2, 0, 1)
    grads(3, 0, 1)
    leave_near(3)
    kept.wait()
    arrived(room(28 << 16), "e", 0)

    for kv in range(KV):
        settle(kv)
    for kv in range(KV):
        relay(kv)

    def early(h):
        arrived(room(6 << 16), "vd", h)
        for ys in (slice(0, 2), slice(2, 4)):
            b.g[h, ys] = jnp.dot(
                b.ex[ys, :, :, 0 : 6 * TOK].reshape(256, 6 * TOK),
                b.vg[h, 0:6].reshape(6 * TOK, 256),
                preferred_element_type=F32,
            ).reshape(2, NZ, 16, 256)

    def product(h):
        arrived(room(2 << 16), "vd", 2 + h)
        for ys in (slice(0, 2), slice(2, 4)):
            b.g[h, ys] += jnp.dot(
                b.ex[ys, :, :, 6 * TOK : 8 * TOK].reshape(256, 2 * TOK),
                b.vg[h, 6:8].reshape(2 * TOK, 256),
                preferred_element_type=F32,
            ).reshape(2, NZ, 16, 256)
        b.g1[h] = b.g[h, yop].astype(BF)
        send(b.g1.at[h, 0:4], b.x1.at[h, 0], "x", 3 * h, dev(cp_0=yup))
        send(b.g1.at[h, 4:8], b.x1.at[h, 1], "x", 3 * h + 1, dev(cp_0=ydn))

    def across(h):
        arrived(b.x1.at[h, 0], "x", 3 * h)
        b.tx[h, 0, 0:4] = (b.g[h, yup, 0:4] + b.x1[h, 0].astype(F32)).astype(BF)
        b.tx[h, 0, 4:8] = b.g[h, yup, 4:8].astype(BF)
        send(b.tx.at[h, 0], b.x2.at[h, 0], "x", 3 * h + 2, dev(cp_0=yup))
        arrived(b.x1.at[h, 1], "x", 3 * h + 1)
        b.tx[h, 1, 0:4] = b.g[h, ydn, 0:4].astype(BF)
        b.tx[h, 1, 4:8] = (b.g[h, ydn, 4:8] + b.x1[h, 1].astype(F32)).astype(BF)
        send(b.tx.at[h, 1], b.x2.at[h, 1], "x", 3 * h + 2, dev(cp_0=ydn))

    def along(h):
        arrived(b.x2.at[h], "x", 3 * h + 2)
        b.t[h] = b.g[h, y] + b.x2[h, 0].astype(F32) + b.x2[h, 1].astype(F32)
        b.tz[h] = b.t[h].astype(BF)
        for d in (4, 3, 5, 2, 6, 1, 7):
            zt = lax.rem(z + d, NZ)
            send(b.tz.at[h, zt], b.rz.at[h, z], "z", h, dev(cp_1=zt))

    def finish(h):
        arrived(b.rz.at[h, 0:7], "z", h)
        total = b.t[h, z]
        for d in range(1, NZ):
            total = total + b.rz[h, lax.rem(z + d, NZ)].astype(F32)
        out[:, h * 256 : (h + 1) * 256] = total

    collect(0)
    collect(1)
    early(0)
    collect(2)
    early(1)
    collect(3)
    product(0)
    product(1)
    across(0)
    across(1)
    along(0)
    along(1)
    finish(0)
    finish(1)

    for kind, size in sent.items():
        if size:
            copy(room(size), room(size), "w1", 0, sibling, kind).wait_send()


def weight_gradient(need_ids, doc_start, embeds, queries, key_heads, cotangent, y_weight):
    any_space = pl.BlockSpec(memory_space=pl.ANY)
    vmem = pl.BlockSpec(memory_space=pltpu.VMEM)
    semaphores = [pltpu.SemaphoreType.DMA((n,)) for n in SEMAPHORES.values()]
    semaphores.append(pltpu.SemaphoreType.DMA((len(SENDERS),)))
    return pl.pallas_call(
        kernel,
        out_shape=pltpu.VMEM((16, 512), F32),
        in_specs=[pl.BlockSpec(memory_space=pltpu.SMEM), vmem] + [any_space] * 5,
        out_specs=vmem,
        scratch_shapes=[pltpu.VMEM(shape, kind) for shape, kind in BUFFERS.values()]
        + semaphores,
        compiler_params=pltpu.CompilerParams(
            collective_id=0, has_side_effects=True, vmem_limit_bytes=58 << 20
        ),
    )(need_ids, doc_start, embeds, queries, key_heads, cotangent, y_weight)


def on_device(
    embeds,
    queries,
    key_heads,
    cotangent,
    doc_start,
    need_ids,
    y_weight,
    z_weight,
    x_weight,
    second_moment,
):
    gradient = weight_gradient(
        need_ids[0], doc_start, embeds[0], queries[0], key_heads[0], cotangent[0], y_weight
    )
    moment_next = MOMENT_DECAY * second_moment + (1.0 - MOMENT_DECAY) * gradient * gradient
    z_next = z_weight - LEARN_RATE * (
        gradient / (jnp.sqrt(moment_next) + ADAM_EPS) + WEIGHT_DECAY * y_weight.astype(jnp.float32)
    )
    x_next = (1.0 - AVERAGE_MIX) * x_weight + AVERAGE_MIX * z_next
    y_next = ((1.0 - INTERP_BETA) * z_next + INTERP_BETA * x_next).astype(jnp.bfloat16)
    return (z_next, x_next, moment_next, y_next)


def solution(mesh):
    finer = Mesh(mesh.devices.reshape(NY, NZ, 2, mesh.shape["fs"]), CP_FS)
    return jax.shard_map(
        on_device,
        mesh=finer,
        in_specs=(
            P("fs", CP, None),
            P("fs", CP, None),
            P("fs", CP, None),
            P("fs", CP, None),
            P("fs", CP),
            P("fs", CP, None),
            P(CP_FS, None),
            P(CP_FS, None),
            P(CP_FS, None),
            P(CP_FS, None),
        ),
        out_specs=(P(CP_FS, None), P(CP_FS, None), P(CP_FS, None), P(CP_FS, None)),
        check_vma=False,
    )
```
